32 devices in a mesh: gx: 8 (over z, x), gy: 4 (over y, core).
Axes of the slice: x: 2, y: 2, z: 4, core: 2. Of those that a mesh axis runs over, the one named last changes fastest.
Arguments:
- map_codes: int32 [1024, 2048], P('gy', 'gx'), may hold values from 0 to 63
- reward_table: float32 [4, 64], replicated, may hold values from -1 to 1
- start_cell: int32 [65536], P(('gx', 'gy')), may hold values from 0 to 65535, as said below
- agent_task: int32 [65536], P(('gx', 'gy')), may hold values from 0 to 3
- actions: int32 [16, 65536], P(None, ('gx', 'gy')), may hold values from 0 to 4, as said below
Outputs:
- values: float32 [4, 1024, 2048], P(None, 'gy', 'gx')
- agent_value: float32 [65536], P(('gx', 'gy'))
The draws below stay inside these ranges and needn't reach their ends.
Inputs may be any that keep to these rules, and one draw needn't show every extreme that they name: `start_cell`: each agent starts inside the tile of its block. `actions`: 0 stays, 1 and 2 move one row up and down, 3 and 4 one column left and right. After its moves every agent stands in its starting tile or in one of the eight tiles around it (diagonal ones included); at most 128 agents of one block stand in any one of those eight tiles, and for every block exactly 128 stand in one of them.
All inputs are finite; a program needn't handle non-finite values.
Results may differ from the reference program's by a relative error of at most 0.00026.
Values sent between devices are 32-bit elements; how exact they have to be, the bound alone decides.
No kernel may reach another device: no remote copies, remote signals or barrier semaphores. Data moves between devices by JAX's collectives and lax.ppermute only.
A program may use at most 64 MiB of HBM per device.

```python
import jax
import jax.numpy as jnp
from jax import lax

CR = 256
CC = 256
TASKS = 4
AG_DEV = 2048
CAP = 128
STEPS = 16
SWEEPS = 16
CODES = 64
TERMINAL = 2
NR = 1024
NC = 2048
AGENTS = 65536
N_GY = 4


DIRECTION_ROWS = (-1, -1, -1, 0, 0, 1, 1, 1, 0)


DIRECTION_COLS = (-1, 0, 1, -1, 1, -1, 0, 1, 0)


def component(key_list, heading, crossing, extent, reach):
    layout = heading.shape
    inward = jax.random.randint(key_list[0], layout, 0, reach, dtype=jnp.int32)
    second = jax.random.randint(key_list[1], layout, 0, reach, dtype=jnp.int32)
    spread = jax.random.randint(key_list[2], layout, 0, 2 * reach + 1, dtype=jnp.int32)
    middle = jax.random.randint(key_list[3], layout, 0, extent - 4 * reach, dtype=jnp.int32)
    across = inward + 1 + second
    anchor_plus = extent - 1 - inward
    offset_plus = jnp.where(crossing, across, -reach + spread % (inward + reach + 1))
    anchor_minus = inward
    offset_minus = jnp.where(crossing, -across, reach - spread % (inward + reach + 1))
    anchor_zero = 2 * reach + middle
    offset_zero = -reach + spread
    anchor = jnp.where(heading > 0, anchor_plus, jnp.where(heading < 0, anchor_minus, anchor_zero))
    offset = jnp.where(heading > 0, offset_plus, jnp.where(heading < 0, offset_minus, offset_zero))
    return (anchor, offset)


def plan_agents(key):
    block_count = AGENTS // AG_DEV
    reach = STEPS // 4
    key_list = jax.random.split(jax.random.fold_in(key, 31), 16)
    scores = jax.random.randint(key_list[0], (block_count, AG_DEV), 0, (1 << 30) // AG_DEV, dtype=jnp.int32) * AG_DEV + jnp.arange(AG_DEV, dtype=jnp.int32)[None, :]
    roles = jnp.argsort(jnp.argsort(scores, axis=1), axis=1).astype(jnp.int32)
    direction = jnp.where(roles < 8 * CAP, roles // CAP, 8)
    favoured = jax.random.randint(key_list[1], (block_count, 1), 0, 8, dtype=jnp.int32)
    tossed = jax.random.randint(key_list[2], (block_count, AG_DEV), 0, 2, dtype=jnp.int32)
    crossing = (direction < 8) & ((direction == favoured) | (tossed == 1))
    row_heading = jnp.array(DIRECTION_ROWS, jnp.int32)[direction]
    col_heading = jnp.array(DIRECTION_COLS, jnp.int32)[direction]
    row_anchor, row_offset = component(key_list[3:7], row_heading, crossing, CR, reach)
    col_anchor, col_offset = component(key_list[7:11], col_heading, crossing, CC, reach)
    start_cell = (row_anchor * CC + col_anchor).reshape(-1).astype(jnp.int32)
    row_count = jnp.abs(row_offset)
    col_count = jnp.abs(col_offset)
    leftover = STEPS - row_count - col_count
    pairs_count = jax.random.randint(key_list[11], row_count.shape, 0, 1 << 20, dtype=jnp.int32) % (leftover // 2 + 1)
    vertical = jax.random.randint(key_list[12], row_count.shape, 0, 2, dtype=jnp.int32)
    moment = jnp.arange(STEPS, dtype=jnp.int32)[:, None, None]
    chosen = jnp.where(moment < row_count, jnp.where(row_offset > 0, 2, 1), jnp.where(moment < row_count + col_count, jnp.where(col_offset > 0, 4, 3), jnp.where(moment < row_count + col_count + pairs_count, jnp.where(vertical == 1, 1, 3), jnp.where(moment < row_count + col_count + 2 * pairs_count, jnp.where(vertical == 1, 2, 4), 0)))).astype(jnp.int32)
    shuffle = jax.random.randint(key_list[13], chosen.shape, 0, (1 << 30) // STEPS, dtype=jnp.int32) * STEPS + moment
    ordering = jnp.argsort(shuffle, axis=0)
    actions = jnp.take_along_axis(chosen, ordering, axis=0).reshape(STEPS, -1).astype(jnp.int32)
    return (start_cell, actions)


def draw_start_cell(key, part):
    return plan_agents(key)[0]


def draw_actions(key, part):
    return plan_agents(key)[1]


def with_ends(values, own_key, smallest, largest):
    place = [jax.random.randint(jax.random.fold_in(own_key, axis), (), 0, length) for axis, length in enumerate(values.shape)]
    widest = values.shape.index(max(values.shape))
    neighbour = place[:widest] + [(place[widest] + 1) % values.shape[widest]] + place[widest + 1:]
    return values.at[tuple(place)].set(smallest).at[tuple(neighbour)].set(largest)


def setup_inputs(seed: int = 0) -> dict:
    seeds = jax.random.split(jax.random.key(seed), 6)
    map_codes = with_ends(jax.random.randint(seeds[0], (NR, NC), 0, CODES), jax.random.fold_in(seeds[0], 1), 0, CODES - 1).astype(jnp.int32)
    reward_table = jnp.clip(jax.random.uniform(seeds[1], (TASKS, CODES), jnp.float32, -1.0, 1.0), -1.0, 1.0)
    start_cell = draw_start_cell(jax.random.fold_in(seeds[5], 71), 0)
    agent_task = with_ends(jax.random.randint(seeds[3], (AGENTS,), 0, TASKS), jax.random.fold_in(seeds[3], 1), 0, TASKS - 1).astype(jnp.int32)
    actions = draw_actions(jax.random.fold_in(seeds[5], 71), 0)
    return dict(map_codes=map_codes, reward_table=reward_table, start_cell=start_cell, agent_task=agent_task, actions=actions)


GAMMA = 0.95
PENALTY = 0.5


def sweep_cells(reward, living, padded):
    from_above = padded[..., :-2, 1:-1]
    from_below = padded[..., 2:, 1:-1]
    from_left = padded[..., 1:-1, :-2]
    from_right = padded[..., 1:-1, 2:]
    highest = jnp.maximum(jnp.maximum(from_above, from_below), jnp.maximum(from_left, from_right))
    return reward + GAMMA * living * highest


def reference(map_codes, reward_table, start_cell, agent_task, actions):
    row_moves = jnp.sum((actions == 2).astype(jnp.int32) - (actions == 1).astype(jnp.int32), axis=0)
    col_moves = jnp.sum((actions == 4).astype(jnp.int32) - (actions == 3).astype(jnp.int32), axis=0)
    slot_index = jnp.arange(AGENTS, dtype=jnp.int32)
    block_index = slot_index // AG_DEV
    tile_column = block_index // N_GY
    tile_row = block_index % N_GY
    final_row = (tile_row * CR + start_cell // CC + row_moves) % NR
    final_col = (tile_column * CC + start_cell % CC + col_moves) % NC
    final_cell = (final_row * NC + final_col).astype(jnp.int32)
    crowding = jnp.zeros((NR * NC,), jnp.float32).at[final_cell].add(1.0).reshape(NR, NC)
    living = (map_codes < CODES - TERMINAL).astype(jnp.float32)

    def solve_task(table_row):
        reward = table_row[map_codes] - PENALTY * crowding

        def one_sweep(sweep_index, current):
            padded = jnp.pad(current, ((1, 1), (1, 1)), mode="wrap")
            return sweep_cells(reward, living, padded)

        return lax.fori_loop(0, SWEEPS, one_sweep, reward)

    values = lax.map(solve_task, reward_table)
    flat_values = values.reshape(TASKS, NR * NC)
    agent_value = flat_values[agent_task, final_cell]
    return values, agent_value
```

```python
import jax
import jax.numpy as jnp
from jax import lax
from jax.experimental import pallas as pl
from jax.experimental.pallas import tpu as pltpu
from jax.sharding import PartitionSpec as P


SWEEPS = 16
TERMINAL = 2
GAMMA = 0.95
PENALTY = 0.5
LANES = 128
SUB = 8


class Plan:
    def __init__(self, rows, cols, agents, steps, tasks, codes):
        self.rows, self.cols, self.agents = rows, cols, agents
        self.steps, self.tasks, self.codes = steps, tasks, codes
        self.near = steps
        self.wide = steps + SWEEPS
        self.ring = rows + 2 * self.wide
        self.tiles = cols // LANES + 1
        self.span = self.ring // SUB
        self.step = LANES - 2 * SWEEPS
        self.sweep_tiles = -(-(cols + 2 * self.near) // self.step)
        self.code_bits = (codes - 1).bit_length()
        self.across_rows = rows + 2 * self.near
        self.band = self.wide + self.near
        self.down_rows = self.tiles * self.band + (self.tiles - 1) * self.wide
        assert cols % LANES == 0 and rows % SUB == 0 and agents % LANES == 0
        assert 4 * self.wide <= LANES and self.near % SUB == 0 and self.wide % SUB == 0
        assert self.ring % SUB == 0 and codes <= LANES
        self.magic = -(-(1 << 16) // self.span)
        assert all((r * self.magic) >> 16 == r // self.span for r in range(self.ring))

    def start(self, j):
        return j * self.step - self.wide


def lane_of(shape):
    return lax.broadcasted_iota(jnp.int32, shape, len(shape) - 1)


def split_cell(cell, cols):
    if cols & (cols - 1) == 0:
        return cell >> (cols.bit_length() - 1), cell & (cols - 1)
    return lax.div(cell, cols), lax.rem(cell, cols)


def count_kernel(plan, act, start, task, code, hist, right, left, address, lane_out, row_hot, col_hot):
    p = plan
    ring_cols = p.tiles * LANES
    row_id = lax.broadcasted_iota(jnp.int32, (p.ring, LANES), 0)
    col_id = lax.broadcasted_iota(jnp.int32, (ring_cols, LANES), 0)
    for i in range(p.agents // LANES):
        here = slice(i * LANES, (i + 1) * LANES)
        a = act[:, here]
        one = lambda c: jnp.where(a == c, 1, 0)
        row_moves = jnp.sum(one(2) - one(1), axis=0, keepdims=True)
        col_moves = jnp.sum(one(4) - one(3), axis=0, keepdims=True)
        row, col = split_cell(start[i : i + 1, :], p.cols)
        row = row + row_moves
        col = col + col_moves
        ring_row = jnp.where(row < 0, row + p.ring, row)
        ring_col = jnp.where(col < 0, col + ring_cols, col)
        row_hot[:, here] = jnp.where(row_id == ring_row, 1.0, 0.0).astype(jnp.bfloat16)
        col_hot[:, here] = jnp.where(col_id == ring_col, 1.0, 0.0).astype(jnp.bfloat16)
        inner = col + p.near
        j = jnp.zeros_like(inner)
        for edge in range(1, p.sweep_tiles):
            j = j + jnp.where(inner >= edge * p.step, 1, 0)
        lane_out[i : i + 1, :] = inner - j * p.step + (p.wide - p.near)
        sub = (ring_row * p.magic) >> 16
        address[i : i + 1, :] = (
            (j * p.tasks + task[i : i + 1, :]) * p.ring + (ring_row - sub * p.span) * SUB + sub
        )
    counts = lax.dot_general(
        row_hot[...], col_hot[...], (((1,), (1,)), ((), ())), preferred_element_type=jnp.float32
    )
    for t in range(p.tiles):
        hist[t] = counts[:, t * LANES : (t + 1) * LANES]
    last = p.tiles - 1
    for dst, src, n in ((0, 0, p.rows), (p.rows, p.rows, p.near), (p.rows + p.near, p.ring - p.near, p.near)):
        lane = lane_of((n, LANES))
        at = pl.ds(src, n)
        to_right = jnp.where(lane < p.near, hist[last, at, :], hist[last - 1, at, :])
        to_left = jnp.where(lane < p.wide, hist[0, at, :], hist[last, at, :])
        if src == 0:
            low = code[:, :LANES].astype(jnp.float32)
            high = code[:, (last - 1) * LANES :].astype(jnp.float32)
            inside = (lane >= LANES - 2 * p.wide) & (lane < LANES - p.wide)
            to_right = jnp.where(inside, pltpu.roll(high, LANES - p.wide, 1), to_right)
            inside = (lane >= p.wide) & (lane < 2 * p.wide)
            to_left = jnp.where(inside, pltpu.roll(low, p.wide, 1), to_left)
        right[pl.ds(dst, n), :] = to_right
        left[pl.ds(dst, n), :] = to_left


def across_kernel(plan, hist, code, from_left, from_right, key, first, second, cnt, cds):
    p = plan
    last = p.tiles - 1
    for dst, src, n in ((0, 0, p.rows + p.near), (p.ring - p.near, p.rows + p.near, p.near)):
        lane = lane_of((n, LANES))
        at = pl.ds(dst, n)
        l = from_left[pl.ds(src, n), :]
        r = from_right[pl.ds(src, n), :]
        for t in range(p.tiles):
            h = hist[t, at, :]
            if t == 0:
                h = h + jnp.where(lane < p.near, l, 0.0)
            if t == last - 1:
                h = h + jnp.where(lane >= LANES - p.near, r, 0.0)
            if t == last:
                h = h + jnp.where(lane >= LANES - p.wide, l, jnp.where(lane < p.wide, r, 0.0))
            cnt[t, at, :] = h
    own = pl.ds(0, p.rows)
    lane = lane_of((p.rows, LANES))
    l = pltpu.roll(from_left[own, :], p.wide, 1)
    r = pltpu.roll(from_right[own, :], LANES - p.wide, 1)
    for t in range(last):
        cds[t] = code[:, t * LANES : (t + 1) * LANES].astype(jnp.float32)
    cds[last] = jnp.where(lane >= LANES - p.wide, l, jnp.where(lane < p.wide, r, 0.0))
    for t in range(p.tiles):
        key[t, own, :] = (cnt[t, own, :].astype(jnp.int32) << p.code_bits) + cds[t].astype(jnp.int32)
        for lo, n in ((p.rows, p.near), (p.ring - p.near, p.near)):
            at = pl.ds(lo, n)
            key[t, at, :] = cnt[t, at, :].astype(jnp.int32) << p.code_bits

    def write(down, up):
        lane = lane_of((p.wide, LANES))
        inside = (lane >= p.wide) & (lane < LANES - p.wide)
        for t in range(p.tiles):
            base = t * p.band
            down[pl.ds(base, p.band), :] = cnt[t, pl.ds(p.rows - p.wide, p.band), :]
            up[pl.ds(base, p.near), :] = cnt[t, pl.ds(p.ring - p.near, p.near), :]
            up[pl.ds(base + p.near, p.wide), :] = cnt[t, pl.ds(0, p.wide), :]
            low = cds[t, pl.ds(0, p.wide), :]
            high = cds[t, pl.ds(p.rows - p.wide, p.wide), :]
            if t < last:
                base = p.tiles * p.band + t * p.wide
                down[pl.ds(base, p.wide), :] = high
                up[pl.ds(base, p.wide), :] = low
            else:
                half = LANES // 2
                at = pl.ds(base, p.wide)
                down[at, :] = jnp.where(inside, pltpu.roll(high, half, 1), down[at, :])
                at = pl.ds(base + p.near, p.wide)
                up[at, :] = jnp.where(inside, pltpu.roll(low, half, 1), up[at, :])

    odd = lax.axis_index("gy") % 2 == 1

    @pl.when(odd)
    def _():
        write(second, first)

    @pl.when(jnp.logical_not(odd))
    def _():
        write(first, second)


def sweep_kernel(plan, table, key, first, second, address, lane_in, values, answers,
                 ring, tiles, reward, gain, value, natural, rows_of, sems):
    p = plan
    last = p.tiles - 1
    odd = lax.axis_index("gy") % 2 == 1
    half = LANES // 2

    def above(at, n):
        at = pl.ds(at, n)
        return jnp.where(odd, first[at, :], second[at, :]).astype(jnp.int32)

    def below(at, n):
        at = pl.ds(at, n)
        return jnp.where(odd, second[at, :], first[at, :]).astype(jnp.int32)

    w, s, bits = p.wide, p.near, p.code_bits
    for t in range(p.tiles):
        base = t * p.band
        code_base = p.tiles * p.band + t * w
        up_cnt = above(base, p.band) << bits
        low_cnt = below(base, p.band) << bits
        if t < last:
            up_code = above(code_base, w)
            low_code = below(code_base, w)
        else:
            up_code = pltpu.roll(above(base, w), half, 1)
            low_code = pltpu.roll(below(base + s, w), half, 1)
        own = lambda lo, n: key[t, pl.ds(lo, n), :]

        def put(lo, n, x):
            ring[t, pl.ds(lo, n), :] = x

        put(0, s, own(0, s) + up_cnt[w:])
        put(s, p.rows - 2 * s, own(s, p.rows - 2 * s))
        put(p.rows - s, s, own(p.rows - s, s) + low_cnt[:s])
        put(p.rows, s, own(p.rows, s) + low_cnt[s : 2 * s] + low_code[:s])
        put(p.rows + s, w - s, low_cnt[2 * s :] + low_code[s:])
        put(p.ring - w, w - s, up_cnt[: w - s] + up_code[: w - s])
        put(p.ring - s, s, own(p.ring - s, s) + up_cnt[w - s : w] + up_code[w - s :])

    lane = lane_of((p.ring, LANES))
    for j in range(p.sweep_tiles):
        at = p.start(j) % (p.tiles * LANES)
        a, off = at // LANES, at % LANES
        x = ring[a]
        if off:
            x = pltpu.roll(jnp.where(lane >= off, x, ring[(a + 1) % p.tiles]), LANES - off, 1)
        tiles[j] = x

    looks = [jnp.broadcast_to(table[t : t + 1, :], (SUB, LANES)) for t in range(p.tasks)]
    for j in range(p.sweep_tiles):
        for k in range(p.span):
            x = tiles[j, pl.ds(k, SUB, stride=p.span), :]
            code = x & ((1 << bits) - 1)
            crowd = PENALTY * (x >> bits).astype(jnp.float32)
            at = pl.ds(k * SUB, SUB)
            gain[j, at, :] = jnp.where(code < p.codes - TERMINAL, GAMMA, 0.0)
            for t in range(p.tasks):
                r = jnp.take_along_axis(looks[t], code, axis=1, mode="promise_in_bounds") - crowd
                reward[j * p.tasks + t, at, :] = r
                value[pl.ds((j * p.tasks + t) * p.ring + k * SUB, SUB), :] = r

    def sweep(_, carry):
        for j in range(p.sweep_tiles):
            base = [(j * p.tasks + t) * p.ring for t in range(p.tasks)]
            load = lambda t, k: value[pl.ds(base[t] + k * SUB, SUB), :]
            first_row = [load(t, 0) for t in range(p.tasks)]
            before = [pltpu.roll(load(t, p.span - 1), 1, 0) for t in range(p.tasks)]
            now = list(first_row)
            for k in range(p.span):
                g = gain[j, pl.ds(k * SUB, SUB), :]
                for t in range(p.tasks):
                    after = load(t, k + 1) if k + 1 < p.span else pltpu.roll(first_row[t], SUB - 1, 0)
                    side = jnp.maximum(pltpu.roll(now[t], 1, 1), pltpu.roll(now[t], LANES - 1, 1))
                    best = jnp.maximum(jnp.maximum(before[t], after), side)
                    new = reward[j * p.tasks + t, pl.ds(k * SUB, SUB), :] + g * best
                    value[pl.ds(base[t] + k * SUB, SUB), :] = new
                    before[t], now[t] = now[t], after
        return carry

    lax.fori_loop(0, SWEEPS, sweep, 0)

    lane = lane_of((SUB, LANES))
    copies = []
    for t in range(p.tasks):
        for c in range(last):
            for k in range(p.span):
                out = None
                for j in range(p.sweep_tiles):
                    lo = p.start(j) + SWEEPS - c * LANES
                    hi = lo + p.step
                    if hi <= 0 or lo >= LANES:
                        continue
                    x = value[pl.ds((j * p.tasks + t) * p.ring + k * SUB, SUB), :]
                    x = pltpu.roll(x, (p.start(j) - c * LANES) % LANES, 1)
                    out = x if out is None else jnp.where(lane >= lo, x, out)
                natural[t * last + c, pl.ds(k, SUB, stride=p.span), :] = out
            copy = pltpu.make_async_copy(
                natural.at[t * last + c, pl.ds(0, p.rows), :],
                values.at[t, :, pl.ds(c * LANES, LANES)],
                sems.at[t * last + c],
            )
            copy.start()
            copies.append(copy)

    def fetch(i, carry):
        for l in range(LANES):
            rows_of[pl.ds(i * LANES + l, 1), :] = value[pl.ds(address[i, l], 1), :]
        return carry

    lax.fori_loop(0, p.agents // LANES, fetch, 0)
    lane_id = lax.broadcasted_iota(jnp.int32, (LANES, LANES), 0)
    for i in range(p.agents // LANES):
        turned = jnp.transpose(rows_of[pl.ds(i * LANES, LANES), :])
        picked = jnp.where(lane_id == lane_in[i : i + 1, :], turned, 0.0)
        answers[i : i + 1, :] = jnp.sum(picked, axis=0, keepdims=True)
    for copy in copies:
        copy.wait()


def shift(value, axis, steps):
    count = lax.axis_size(axis)
    return lax.ppermute(value, axis, [(i, (i + steps) % count) for i in range(count)])


def swap(value, axis, parity):
    count = lax.axis_size(axis)
    assert count % 2 == 0
    return lax.ppermute(
        value, axis, [(i, (i + (1 if i % 2 == parity else -1)) % count) for i in range(count)]
    )


def on_device(map_codes, reward_table, start_cell, agent_task, actions):
    rows, cols = map_codes.shape
    tasks, codes = reward_table.shape
    steps, agents = actions.shape
    p = Plan(rows, cols, agents, steps, tasks, codes)
    vmem = pl.BlockSpec(memory_space=pltpu.VMEM)
    smem = pl.BlockSpec(memory_space=pltpu.SMEM)
    f32, i32 = jnp.float32, jnp.int32
    shape = jax.ShapeDtypeStruct
    by_lane = (agents // LANES, LANES)

    def bind(kernel):
        def body(*refs):
            kernel(p, *refs)

        return body

    table = jnp.pad(reward_table, ((0, 0), (0, LANES - codes)))
    hist, to_right, to_left, address, lane = pl.pallas_call(
        bind(count_kernel),
        in_specs=[vmem] * 4,
        out_specs=[vmem] * 5,
        out_shape=[
            shape((p.tiles, p.ring, LANES), f32),
            shape((p.across_rows, LANES), f32),
            shape((p.across_rows, LANES), f32),
            shape(by_lane, i32),
            shape(by_lane, i32),
        ],
        scratch_shapes=[
            pltpu.VMEM((p.ring, agents), jnp.bfloat16),
            pltpu.VMEM((p.tiles * LANES, agents), jnp.bfloat16),
        ],
        name="count",
    )(actions, start_cell.reshape(by_lane), agent_task.reshape(by_lane), map_codes)
    from_left = shift(to_right, "gx", 1)
    from_right = shift(to_left, "gx", -1)
    key, first, second = pl.pallas_call(
        bind(across_kernel),
        in_specs=[vmem] * 4,
        out_specs=[vmem] * 3,
        out_shape=[
            shape((p.tiles, p.ring, LANES), i32),
            shape((p.down_rows, LANES), f32),
            shape((p.down_rows, LANES), f32),
        ],
        scratch_shapes=[
            pltpu.VMEM((p.tiles, p.ring, LANES), f32),
            pltpu.VMEM((p.tiles, p.rows, LANES), f32),
        ],
        name="across",
    )(hist, map_codes, from_left, from_right)
    first = swap(first, "gy", 0)
    second = swap(second, "gy", 1)
    blocks = p.sweep_tiles * tasks
    outs = tasks * (p.tiles - 1)
    values, answers = pl.pallas_call(
        bind(sweep_kernel),
        in_specs=[vmem, vmem, vmem, vmem, smem, vmem],
        out_specs=[pl.BlockSpec(memory_space=pl.ANY), vmem],
        out_shape=[shape((tasks, rows, cols), f32), shape(by_lane, f32)],
        scratch_shapes=[
            pltpu.VMEM((p.tiles, p.ring, LANES), i32),
            pltpu.VMEM((p.sweep_tiles, p.ring, LANES), i32),
            pltpu.VMEM((blocks, p.ring, LANES), f32),
            pltpu.VMEM((p.sweep_tiles, p.ring, LANES), f32),
            pltpu.VMEM((blocks * p.ring, LANES), f32),
            pltpu.VMEM((outs, p.ring, LANES), f32),
            pltpu.VMEM((agents, LANES), f32),
            pltpu.SemaphoreType.DMA((outs,)),
        ],
        name="sweep",
    )(table, key, first, second, address, lane)
    return values, answers.reshape(agents)


def solution(mesh):
    placed = (P("gy", "gx"), P(), P(("gx", "gy")), P(("gx", "gy")), P(None, ("gx", "gy")))
    return jax.shard_map(
        on_device,
        mesh=mesh,
        in_specs=placed,
        out_specs=(P(None, "gy", "gx"), P(("gx", "gy"))),
        check_vma=False,
    )
```

```python
import jax
import jax.numpy as jnp
from jax import lax
from jax.experimental import pallas as pl
from jax.experimental.pallas import tpu as pltpu
from jax.sharding import PartitionSpec as P


SWEEPS = 16
TERMINAL = 2
GAMMA = 0.95
PENALTY = 0.5
LANES = 128
SUB = 8


class Plan:
    def __init__(self, rows, cols, agents, steps, tasks, codes):
        self.rows, self.cols, self.agents = rows, cols, agents
        self.steps, self.tasks, self.codes = steps, tasks, codes
        self.near = steps
        self.wide = steps + SWEEPS
        self.ring = rows + 2 * self.wide
        self.tiles = cols // LANES + 1
        self.span = self.ring // SUB
        self.step = LANES - 2 * SWEEPS
        self.sweep_tiles = -(-(cols + 2 * self.near) // self.step)
        self.code_bits = (codes - 1).bit_length()
        self.across_rows = rows + 2 * self.near
        self.band = self.wide + self.near
        self.down_rows = self.tiles * self.band + (self.tiles - 1) * self.wide
        assert cols % LANES == 0 and rows % SUB == 0 and agents % LANES == 0
        assert 4 * self.wide <= LANES and self.near % SUB == 0 and self.wide % SUB == 0
        assert self.ring % SUB == 0 and codes <= LANES
        self.magic = -(-(1 << 16) // self.span)
        assert all((r * self.magic) >> 16 == r // self.span for r in range(self.ring))

    def start(self, j):
        return j * self.step - self.wide


def lane_of(shape):
    return lax.broadcasted_iota(jnp.int32, shape, len(shape) - 1)


def split_cell(cell, cols):
    if cols & (cols - 1) == 0:
        return cell >> (cols.bit_length() - 1), cell & (cols - 1)
    return lax.div(cell, cols), lax.rem(cell, cols)


def count_kernel(plan, act, start, task, code, hist, right, left, address, lane_out, row_hot, col_hot):
    p = plan
    ring_cols = p.tiles * LANES
    row_id = lax.broadcasted_iota(jnp.int32, (p.ring, LANES), 0)
    col_id = lax.broadcasted_iota(jnp.int32, (ring_cols, LANES), 0)
    for i in range(p.agents // LANES):
        here = slice(i * LANES, (i + 1) * LANES)
        a = act[:, here]
        one = lambda c: jnp.where(a == c, 1, 0)
        row_moves = jnp.sum(one(2) - one(1), axis=0, keepdims=True)
        col_moves = jnp.sum(one(4) - one(3), axis=0, keepdims=True)
        row, col = split_cell(start[i : i + 1, :], p.cols)
        row = row + row_moves
        col = col + col_moves
        ring_row = jnp.where(row < 0, row + p.ring, row)
        ring_col = jnp.where(col < 0, col + ring_cols, col)
        row_hot[:, here] = jnp.where(row_id == ring_row, 1.0, 0.0).astype(jnp.bfloat16)
        col_hot[:, here] = jnp.where(col_id == ring_col, 1.0, 0.0).astype(jnp.bfloat16)
        inner = col + p.near
        j = jnp.zeros_like(inner)
        for edge in range(1, p.sweep_tiles):
            j = j + jnp.where(inner >= edge * p.step, 1, 0)
        lane_out[i : i + 1, :] = inner - j * p.step + (p.wide - p.near)
        sub = (ring_row * p.magic) >> 16
        address[i : i + 1, :] = (
            (j * p.tasks + task[i : i + 1, :]) * p.ring + (ring_row - sub * p.span) * SUB + sub
        )
    counts = lax.dot_general(
        row_hot[...], col_hot[...], (((1,), (1,)), ((), ())), preferred_element_type=jnp.float32
    )
    for t in range(p.tiles):
        hist[t] = counts[:, t * LANES : (t + 1) * LANES]
    last = p.tiles - 1
    for dst, src, n in ((0, 0, p.rows), (p.rows, p.rows, p.near), (p.rows + p.near, p.ring - p.near, p.near)):
        lane = lane_of((n, LANES))
        at = pl.ds(src, n)
        to_right = jnp.where(lane < p.near, hist[last, at, :], hist[last - 1, at, :])
        to_left = jnp.where(lane < p.wide, hist[0, at, :], hist[last, at, :])
        if src == 0:
            low = code[:, :LANES].astype(jnp.float32)
            high = code[:, (last - 1) * LANES :].astype(jnp.float32)
            inside = (lane >= LANES - 2 * p.wide) & (lane < LANES - p.wide)
            to_right = jnp.where(inside, pltpu.roll(high, LANES - p.wide, 1), to_right)
            inside = (lane >= p.wide) & (lane < 2 * p.wide)
            to_left = jnp.where(inside, pltpu.roll(low, p.wide, 1), to_left)
        right[pl.ds(dst, n), :] = to_right
        left[pl.ds(dst, n), :] = to_left


def across_kernel(plan, hist, code, from_left, from_right, key, first, second, cnt, cds):
    p = plan
    last = p.tiles - 1
    for dst, src, n in ((0, 0, p.rows + p.near), (p.ring - p.near, p.rows + p.near, p.near)):
        lane = lane_of((n, LANES))
        at = pl.ds(dst, n)
        l = from_left[pl.ds(src, n), :]
        r = from_right[pl.ds(src, n), :]
        for t in range(p.tiles):
            h = hist[t, at, :]
            if t == 0:
                h = h + jnp.where(lane < p.near, l, 0.0)
            if t == last - 1:
                h = h + jnp.where(lane >= LANES - p.near, r, 0.0)
            if t == last:
                h = h + jnp.where(lane >= LANES - p.wide, l, jnp.where(lane < p.wide, r, 0.0))
            cnt[t, at, :] = h
    own = pl.ds(0, p.rows)
    lane = lane_of((p.rows, LANES))
    l = pltpu.roll(from_left[own, :], p.wide, 1)
    r = pltpu.roll(from_right[own, :], LANES - p.wide, 1)
    for t in range(last):
        cds[t] = code[:, t * LANES : (t + 1) * LANES].astype(jnp.float32)
    cds[last] = jnp.where(lane >= LANES - p.wide, l, jnp.where(lane < p.wide, r, 0.0))
    for t in range(p.tiles):
        key[t, own, :] = (cnt[t, own, :].astype(jnp.int32) << p.code_bits) + cds[t].astype(jnp.int32)
        for lo, n in ((p.rows, p.near), (p.ring - p.near, p.near)):
            at = pl.ds(lo, n)
            key[t, at, :] = cnt[t, at, :].astype(jnp.int32) << p.code_bits

    def write(down, up):
        lane = lane_of((p.wide, LANES))
        inside = (lane >= p.wide) & (lane < LANES - p.wide)
        for t in range(p.tiles):
            base = t * p.band
            down[pl.ds(base, p.band), :] = cnt[t, pl.ds(p.rows - p.wide, p.band), :]
            up[pl.ds(base, p.near), :] = cnt[t, pl.ds(p.ring - p.near, p.near), :]
            up[pl.ds(base + p.near, p.wide), :] = cnt[t, pl.ds(0, p.wide), :]
            low = cds[t, pl.ds(0, p.wide), :]
            high = cds[t, pl.ds(p.rows - p.wide, p.wide), :]
            if t < last:
                base = p.tiles * p.band + t * p.wide
                down[pl.ds(base, p.wide), :] = high
                up[pl.ds(base, p.wide), :] = low
            else:
                half = LANES // 2
                at = pl.ds(base, p.wide)
                down[at, :] = jnp.where(inside, pltpu.roll(high, half, 1), down[at, :])
                at = pl.ds(base + p.near, p.wide)
                up[at, :] = jnp.where(inside, pltpu.roll(low, half, 1), up[at, :])

    odd = lax.axis_index("gy") % 2 == 1

    @pl.when(odd)
    def _():
        write(second, first)

    @pl.when(jnp.logical_not(odd))
    def _():
        write(first, second)


def sweep_kernel(plan, table, key, first, second, address, lane_in, values, answers,
                 looked, ring, tiles, reward, gain, value, natural, rows_of, sems):
    p = plan
    last = p.tiles - 1
    odd = lax.axis_index("gy") % 2 == 1
    half = LANES // 2

    def above(at, n):
        at = pl.ds(at, n)
        return jnp.where(odd, first[at, :], second[at, :]).astype(jnp.int32)

    def below(at, n):
        at = pl.ds(at, n)
        return jnp.where(odd, second[at, :], first[at, :]).astype(jnp.int32)

    w, s, bits = p.wide, p.near, p.code_bits
    for t in range(p.tiles):
        base = t * p.band
        code_base = p.tiles * p.band + t * w
        up_cnt = above(base, p.band) << bits
        low_cnt = below(base, p.band) << bits
        if t < last:
            up_code = above(code_base, w)
            low_code = below(code_base, w)
        else:
            up_code = pltpu.roll(above(base, w), half, 1)
            low_code = pltpu.roll(below(base + s, w), half, 1)
        own = lambda lo, n: key[t, pl.ds(lo, n), :]

        def put(lo, n, x):
            ring[t, pl.ds(lo, n), :] = x

        put(0, s, own(0, s) + up_cnt[w:])
        put(s, p.rows - 2 * s, own(s, p.rows - 2 * s))
        put(p.rows - s, s, own(p.rows - s, s) + low_cnt[:s])
        put(p.rows, s, own(p.rows, s) + low_cnt[s : 2 * s] + low_code[:s])
        put(p.rows + s, w - s, low_cnt[2 * s :] + low_code[s:])
        put(p.ring - w, w - s, up_cnt[: w - s] + up_code[: w - s])
        put(p.ring - s, s, own(p.ring - s, s) + up_cnt[w - s : w] + up_code[w - s :])

    lane = lane_of((p.ring, LANES))
    for j in range(p.sweep_tiles):
        at = p.start(j) % (p.tiles * LANES)
        a, off = at // LANES, at % LANES
        x = ring[a]
        if off:
            x = pltpu.roll(jnp.where(lane >= off, x, ring[(a + 1) % p.tiles]), LANES - off, 1)
        tiles[j] = x

    looked[pl.ds(0, p.tasks), pl.ds(0, p.codes)] = table[...]
    looks = [jnp.broadcast_to(looked[t : t + 1, :], (SUB, LANES)) for t in range(p.tasks)]
    for j in range(p.sweep_tiles):
        for k in range(p.span):
            x = tiles[j, pl.ds(k, SUB, stride=p.span), :]
            code = x & ((1 << bits) - 1)
            crowd = PENALTY * (x >> bits).astype(jnp.float32)
            at = pl.ds(k * SUB, SUB)
            gain[j, at, :] = jnp.where(code < p.codes - TERMINAL, GAMMA, 0.0)
            for t in range(p.tasks):
                r = jnp.take_along_axis(looks[t], code, axis=1, mode="promise_in_bounds") - crowd
                reward[j * p.tasks + t, at, :] = r
                value[pl.ds((j * p.tasks + t) * p.ring + k * SUB, SUB), :] = r

    def sweep(_, carry):
        for j in range(p.sweep_tiles):
            base = [(j * p.tasks + t) * p.ring for t in range(p.tasks)]
            load = lambda t, k: value[pl.ds(base[t] + k * SUB, SUB), :]
            first_row = [load(t, 0) for t in range(p.tasks)]
            before = [pltpu.roll(load(t, p.span - 1), 1, 0) for t in range(p.tasks)]
            now = list(first_row)
            for k in range(p.span):
                g = gain[j, pl.ds(k * SUB, SUB), :]
                for t in range(p.tasks):
                    after = load(t, k + 1) if k + 1 < p.span else pltpu.roll(first_row[t], SUB - 1, 0)
                    side = jnp.maximum(pltpu.roll(now[t], 1, 1), pltpu.roll(now[t], LANES - 1, 1))
                    best = jnp.maximum(jnp.maximum(before[t], after), side)
                    new = reward[j * p.tasks + t, pl.ds(k * SUB, SUB), :] + g * best
                    value[pl.ds(base[t] + k * SUB, SUB), :] = new
                    before[t], now[t] = now[t], after
        return carry

    lax.fori_loop(0, SWEEPS, sweep, 0)

    lane = lane_of((SUB, LANES))
    copies = []
    for t in range(p.tasks):
        for c in range(last):
            for k in range(p.span):
                out = None
                for j in range(p.sweep_tiles):
                    lo = p.start(j) + SWEEPS - c * LANES
                    hi = lo + p.step
                    if hi <= 0 or lo >= LANES:
                        continue
                    x = value[pl.ds((j * p.tasks + t) * p.ring + k * SUB, SUB), :]
                    x = pltpu.roll(x, (p.start(j) - c * LANES) % LANES, 1)
                    out = x if out is None else jnp.where(lane >= lo, x, out)
                natural[t * last + c, pl.ds(k, SUB, stride=p.span), :] = out
            copy = pltpu.make_async_copy(
                natural.at[t * last + c, pl.ds(0, p.rows), :],
                values.at[t, :, pl.ds(c * LANES, LANES)],
                sems.at[t * last + c],
            )
            copy.start()
            copies.append(copy)

    def fetch(i, carry):
        for l in range(LANES):
            rows_of[pl.ds(i * LANES + l, 1), :] = value[pl.ds(address[i, l], 1), :]
        return carry

    lax.fori_loop(0, p.agents // LANES, fetch, 0)
    lane_id = lax.broadcasted_iota(jnp.int32, (LANES, LANES), 0)
    for i in range(p.agents // LANES):
        turned = jnp.transpose(rows_of[pl.ds(i * LANES, LANES), :])
        picked = jnp.where(lane_id == lane_in[i : i + 1, :], turned, 0.0)
        answers[i : i + 1, :] = jnp.sum(picked, axis=0, keepdims=True)
    for copy in copies:
        copy.wait()


def shift(value, axis, steps):
    count = lax.axis_size(axis)
    return lax.ppermute(value, axis, [(i, (i + steps) % count) for i in range(count)])


def swap(value, axis, parity):
    count = lax.axis_size(axis)
    assert count % 2 == 0
    return lax.ppermute(
        value, axis, [(i, (i + (1 if i % 2 == parity else -1)) % count) for i in range(count)]
    )


def on_device(map_codes, reward_table, start_cell, agent_task, actions):
    rows, cols = map_codes.shape
    tasks, codes = reward_table.shape
    steps, agents = actions.shape
    p = Plan(rows, cols, agents, steps, tasks, codes)
    vmem = pl.BlockSpec(memory_space=pltpu.VMEM)
    smem = pl.BlockSpec(memory_space=pltpu.SMEM)
    f32, i32 = jnp.float32, jnp.int32
    shape = jax.ShapeDtypeStruct
    fast = lambda dims, dtype: pltpu.VMEM(dims, dtype)
    near = lambda x: pltpu.with_memory_space_constraint(x, pltpu.VMEM)
    by_lane = (agents // LANES, LANES)

    def bind(kernel):
        def body(*refs):
            kernel(p, *refs)

        return body

    hist, to_right, to_left, address, lane = pl.pallas_call(
        bind(count_kernel),
        in_specs=[vmem] * 4,
        out_specs=[vmem] * 5,
        out_shape=[
            fast((p.tiles, p.ring, LANES), f32),
            fast((p.across_rows, LANES), f32),
            fast((p.across_rows, LANES), f32),
            shape(by_lane, i32),
            fast(by_lane, i32),
        ],
        scratch_shapes=[
            pltpu.VMEM((p.ring, agents), jnp.bfloat16),
            pltpu.VMEM((p.tiles * LANES, agents), jnp.bfloat16),
        ],
        name="count",
    )(actions, start_cell.reshape(by_lane), agent_task.reshape(by_lane), map_codes)
    from_left = shift(to_right, "gx", 1)
    from_right = shift(to_left, "gx", -1)
    key, first, second = pl.pallas_call(
        bind(across_kernel),
        in_specs=[vmem] * 4,
        out_specs=[vmem] * 3,
        out_shape=[
            fast((p.tiles, p.ring, LANES), i32),
            fast((p.down_rows, LANES), f32),
            fast((p.down_rows, LANES), f32),
        ],
        scratch_shapes=[
            pltpu.VMEM((p.tiles, p.ring, LANES), f32),
            pltpu.VMEM((p.tiles, p.rows, LANES), f32),
        ],
        name="across",
    )(near(hist), map_codes, near(from_left), near(from_right))
    first = swap(first, "gy", 0)
    second = swap(second, "gy", 1)
    blocks = p.sweep_tiles * tasks
    outs = tasks * (p.tiles - 1)
    values, answers = pl.pallas_call(
        bind(sweep_kernel),
        in_specs=[vmem, vmem, vmem, vmem, smem, vmem],
        out_specs=[pl.BlockSpec(memory_space=pl.ANY), vmem],
        out_shape=[shape((tasks, rows, cols), f32), shape(by_lane, f32)],
        scratch_shapes=[
            pltpu.VMEM((tasks, LANES), f32),
            pltpu.VMEM((p.tiles, p.ring, LANES), i32),
            pltpu.VMEM((p.sweep_tiles, p.ring, LANES), i32),
            pltpu.VMEM((blocks, p.ring, LANES), f32),
            pltpu.VMEM((p.sweep_tiles, p.ring, LANES), f32),
            pltpu.VMEM((blocks * p.ring, LANES), f32),
            pltpu.VMEM((outs, p.ring, LANES), f32),
            pltpu.VMEM((agents, LANES), f32),
            pltpu.SemaphoreType.DMA((outs,)),
        ],
        name="sweep",
    )(reward_table, near(key), near(first), near(second), address, near(lane))
    return values, answers.reshape(agents)


def solution(mesh):
    placed = (P("gy", "gx"), P(), P(("gx", "gy")), P(("gx", "gy")), P(None, ("gx", "gy")))
    return jax.shard_map(
        on_device,
        mesh=mesh,
        in_specs=placed,
        out_specs=(P(None, "gy", "gx"), P(("gx", "gy"))),
        check_vma=False,
    )
```

```python
import jax
import jax.numpy as jnp
from jax import lax
from jax.experimental import pallas as pl
from jax.experimental.pallas import tpu as pltpu
from jax.sharding import PartitionSpec as P


SWEEPS = 16
TERMINAL = 2
GAMMA = 0.95
PENALTY = 0.5
LANES = 128
SUB = 8
PACK = 2
UNROLL = 3


class Plan:
    def __init__(self, rows, cols, agents, steps, tasks, codes):
        self.rows, self.cols, self.agents = rows, cols, agents
        self.steps, self.tasks, self.codes = steps, tasks, codes
        self.near = steps
        self.wide = steps + SWEEPS
        self.ring = rows + 2 * self.wide
        self.tiles = cols // LANES + 1
        self.lines = cols + 2 * self.wide
        self.span = self.lines // SUB
        self.blocks = LANES // PACK
        self.deep = self.ring // self.blocks
        self.groups = tasks // PACK
        self.planes = self.groups * self.deep
        self.code_bits = (codes - 1).bit_length()
        self.across_rows = rows + 2 * self.near
        self.band = self.wide + self.near
        self.down_rows = self.tiles * self.band + (self.tiles - 1) * self.wide
        assert cols % LANES == 0 and rows % SUB == 0 and agents % LANES == 0
        assert 4 * self.wide <= LANES and self.near % SUB == 0 and self.wide % SUB == 0
        assert self.ring % self.blocks == 0 and self.lines % SUB == 0
        assert tasks % PACK == 0 and codes <= LANES
        self.magic = -(-(1 << 16) // self.deep)
        assert all((r * self.magic) >> 16 == r // self.deep for r in range(self.ring))


def lane_of(shape):
    return lax.broadcasted_iota(jnp.int32, shape, len(shape) - 1)


def split_cell(cell, cols):
    if cols & (cols - 1) == 0:
        return cell >> (cols.bit_length() - 1), cell & (cols - 1)
    return lax.div(cell, cols), lax.rem(cell, cols)


def count_kernel(plan, act, start, task, code, hist, right, left, address, lane_out, row_hot, col_hot):
    p = plan
    ring_cols = p.tiles * LANES
    row_id = lax.broadcasted_iota(jnp.int32, (p.ring, LANES), 0)
    col_id = lax.broadcasted_iota(jnp.int32, (ring_cols, LANES), 0)
    for i in range(p.agents // LANES):
        here = slice(i * LANES, (i + 1) * LANES)
        a = act[:, here]
        one = lambda c: jnp.where(a == c, 1, 0)
        row_moves = jnp.sum(one(2) - one(1), axis=0, keepdims=True)
        col_moves = jnp.sum(one(4) - one(3), axis=0, keepdims=True)
        row, col = split_cell(start[i : i + 1, :], p.cols)
        row = row + row_moves
        col = col + col_moves
        ring_row = jnp.where(row < 0, row + p.ring, row)
        ring_col = jnp.where(col < 0, col + ring_cols, col)
        row_hot[:, here] = jnp.where(row_id == ring_row, 1.0, 0.0).astype(jnp.bfloat16)
        col_hot[:, here] = jnp.where(col_id == ring_col, 1.0, 0.0).astype(jnp.bfloat16)
        t = task[i : i + 1, :]
        u = t // PACK
        block = ((row + p.wide) * p.magic) >> 16
        lane_out[i : i + 1, :] = (t - u * PACK) * p.blocks + block
        plane = u * p.deep + row + p.wide - block * p.deep
        address[i : i + 1, :] = plane * p.lines + col + p.wide
    counts = lax.dot_general(
        row_hot[...], col_hot[...], (((1,), (1,)), ((), ())), preferred_element_type=jnp.float32
    )
    for t in range(p.tiles):
        hist[t] = counts[:, t * LANES : (t + 1) * LANES]
    last = p.tiles - 1
    for dst, src, n in ((0, 0, p.rows), (p.rows, p.rows, p.near), (p.rows + p.near, p.ring - p.near, p.near)):
        lane = lane_of((n, LANES))
        at = pl.ds(src, n)
        to_right = jnp.where(lane < p.near, hist[last, at, :], hist[last - 1, at, :])
        to_left = jnp.where(lane < p.wide, hist[0, at, :], hist[last, at, :])
        if src == 0:
            low = code[:, :LANES].astype(jnp.float32)
            high = code[:, (last - 1) * LANES :].astype(jnp.float32)
            inside = (lane >= LANES - 2 * p.wide) & (lane < LANES - p.wide)
            to_right = jnp.where(inside, pltpu.roll(high, LANES - p.wide, 1), to_right)
            inside = (lane >= p.wide) & (lane < 2 * p.wide)
            to_left = jnp.where(inside, pltpu.roll(low, p.wide, 1), to_left)
        right[pl.ds(dst, n), :] = to_right
        left[pl.ds(dst, n), :] = to_left


def across_kernel(plan, hist, code, from_left, from_right, key, first, second, cnt, cds):
    p = plan
    last = p.tiles - 1
    for dst, src, n in ((0, 0, p.rows + p.near), (p.ring - p.near, p.rows + p.near, p.near)):
        lane = lane_of((n, LANES))
        at = pl.ds(dst, n)
        l = from_left[pl.ds(src, n), :]
        r = from_right[pl.ds(src, n), :]
        for t in range(p.tiles):
            h = hist[t, at, :]
            if t == 0:
                h = h + jnp.where(lane < p.near, l, 0.0)
            if t == last - 1:
                h = h + jnp.where(lane >= LANES - p.near, r, 0.0)
            if t == last:
                h = h + jnp.where(lane >= LANES - p.wide, l, jnp.where(lane < p.wide, r, 0.0))
            cnt[t, at, :] = h
    own = pl.ds(0, p.rows)
    lane = lane_of((p.rows, LANES))
    l = pltpu.roll(from_left[own, :], p.wide, 1)
    r = pltpu.roll(from_right[own, :], LANES - p.wide, 1)
    for t in range(last):
        cds[t] = code[:, t * LANES : (t + 1) * LANES].astype(jnp.float32)
    cds[last] = jnp.where(lane >= LANES - p.wide, l, jnp.where(lane < p.wide, r, 0.0))
    for t in range(p.tiles):
        key[t, own, :] = (cnt[t, own, :].astype(jnp.int32) << p.code_bits) + cds[t].astype(jnp.int32)
        for lo, n in ((p.rows, p.near), (p.ring - p.near, p.near)):
            at = pl.ds(lo, n)
            key[t, at, :] = cnt[t, at, :].astype(jnp.int32) << p.code_bits

    def write(down, up):
        lane = lane_of((p.wide, LANES))
        inside = (lane >= p.wide) & (lane < LANES - p.wide)
        for t in range(p.tiles):
            base = t * p.band
            down[pl.ds(base, p.band), :] = cnt[t, pl.ds(p.rows - p.wide, p.band), :]
            up[pl.ds(base, p.near), :] = cnt[t, pl.ds(p.ring - p.near, p.near), :]
            up[pl.ds(base + p.near, p.wide), :] = cnt[t, pl.ds(0, p.wide), :]
            low = cds[t, pl.ds(0, p.wide), :]
            high = cds[t, pl.ds(p.rows - p.wide, p.wide), :]
            if t < last:
                base = p.tiles * p.band + t * p.wide
                down[pl.ds(base, p.wide), :] = high
                up[pl.ds(base, p.wide), :] = low
            else:
                half = LANES // 2
                at = pl.ds(base, p.wide)
                down[at, :] = jnp.where(inside, pltpu.roll(high, half, 1), down[at, :])
                at = pl.ds(base + p.near, p.wide)
                up[at, :] = jnp.where(inside, pltpu.roll(low, half, 1), up[at, :])

    odd = lax.axis_index("gy") % 2 == 1

    @pl.when(odd)
    def _():
        write(second, first)

    @pl.when(jnp.logical_not(odd))
    def _():
        write(first, second)


def sweep_kernel(plan, table, key, first, second, address, lane_in, values, answers,
                 looked, ring, flat, turned, reward, gain, value, edge, final, natural, rows_of, sems):
    p = plan
    last = p.tiles - 1
    odd = lax.axis_index("gy") % 2 == 1
    half = LANES // 2

    def above(at, n):
        at = pl.ds(at, n)
        return jnp.where(odd, first[at, :], second[at, :]).astype(jnp.int32)

    def below(at, n):
        at = pl.ds(at, n)
        return jnp.where(odd, second[at, :], first[at, :]).astype(jnp.int32)

    w, s, bits = p.wide, p.near, p.code_bits
    for t in range(p.tiles):
        base = t * p.band
        code_base = p.tiles * p.band + t * w
        up_cnt = above(base, p.band) << bits
        low_cnt = below(base, p.band) << bits
        if t < last:
            up_code = above(code_base, w)
            low_code = below(code_base, w)
        else:
            up_code = pltpu.roll(above(base, w), half, 1)
            low_code = pltpu.roll(below(base + s, w), half, 1)
        own = lambda lo, n: key[t, pl.ds(lo, n), :]

        def put(lo, n, x):
            ring[t, pl.ds(lo + w, n), :] = x

        put(0, s, own(0, s) + up_cnt[w:])
        put(s, p.rows - 2 * s, own(s, p.rows - 2 * s))
        put(p.rows - s, s, own(p.rows - s, s) + low_cnt[:s])
        put(p.rows, s, own(p.rows, s) + low_cnt[s : 2 * s] + low_code[:s])
        put(p.rows + s, w - s, low_cnt[2 * s :] + low_code[s:])
        put(-w, w - s, up_cnt[: w - s] + up_code[: w - s])
        put(-s, s, own(p.ring - s, s) + up_cnt[w - s : w] + up_code[w - s :])

    looked[pl.ds(0, p.tasks), pl.ds(0, p.codes)] = table[...]
    looks = [jnp.broadcast_to(looked[t : t + 1, :], (SUB, LANES)) for t in range(p.tasks)]
    for c in range(p.tiles):
        for k in range(p.ring // SUB):
            at = pl.ds(k * SUB, SUB)
            x = ring[c, at, :]
            code = x & ((1 << bits) - 1)
            crowd = PENALTY * (x >> bits).astype(jnp.float32)
            flat[p.tasks * p.tiles + c, at, :] = jnp.where(code < p.codes - TERMINAL, GAMMA, 0.0)
            for t in range(p.tasks):
                found = jnp.take_along_axis(looks[t], code, axis=1, mode="promise_in_bounds")
                flat[t * p.tiles + c, at, :] = found - crowd

    for u in range(p.groups + 1):
        for i in range(p.deep):
            for c in range(p.tiles):
                parts = []
                for h in range(PACK):
                    t = u * PACK + h if u < p.groups else p.tasks
                    parts.append(flat[t * p.tiles + c, pl.ds(i, p.blocks, stride=p.deep), :])
                x = jnp.transpose(jnp.concatenate(parts, axis=0))
                if c < last:
                    turned[u * p.deep + i, pl.ds(w + c * LANES, LANES), :] = x
                else:
                    turned[u * p.deep + i, pl.ds(w + p.cols, w), :] = x[:w]
                    turned[u * p.deep + i, pl.ds(0, w), :] = x[LANES - w :]

    for q in range(p.span):
        for n in range(p.planes + p.deep):
            x = turned[n, pl.ds(q, SUB, stride=p.span), :]
            if n < p.planes:
                at = pl.ds((q * p.planes + n) * SUB, SUB)
                reward[at, :] = x
                value[at, :] = x
            else:
                gain[pl.ds((q * p.deep + n - p.planes) * SUB, SUB), :] = x

    def sweep(put):
        load = lambda q: [value[pl.ds((q * p.planes + n) * SUB, SUB), :] for n in range(p.planes)]
        now = load(0)
        before = [pltpu.roll(x, 1, 0) for x in load(p.span - 1)]
        for n in range(p.planes):
            edge[pl.ds(n * SUB, SUB), :] = pltpu.roll(now[n], SUB - 1, 0)
        for q in range(p.span):
            if q + 1 < p.span:
                after = load(q + 1)
            else:
                after = [edge[pl.ds(n * SUB, SUB), :] for n in range(p.planes)]
            for i in range(p.deep):
                g = gain[pl.ds((q * p.deep + i) * SUB, SUB), :]
                for u in range(p.groups):
                    n = u * p.deep + i
                    up = now[n - 1] if i > 0 else pltpu.roll(now[n + p.deep - 1], 1, 1)
                    down = now[n + 1] if i + 1 < p.deep else pltpu.roll(now[n + 1 - p.deep], LANES - 1, 1)
                    best = jnp.maximum(jnp.maximum(up, down), jnp.maximum(before[n], after[n]))
                    put(q, n, reward[pl.ds((q * p.planes + n) * SUB, SUB), :] + g * best)
            before, now = now, after

    def put_value(q, n, x):
        value[pl.ds((q * p.planes + n) * SUB, SUB), :] = x

    def put_final(q, n, x):
        final[pl.ds(n * p.lines + q, SUB, stride=p.span), :] = x

    def sweeps(_, carry):
        for _ in range(UNROLL):
            sweep(put_value)
        return carry

    assert (SWEEPS - 1) % UNROLL == 0
    lax.fori_loop(0, (SWEEPS - 1) // UNROLL, sweeps, 0)
    sweep(put_final)

    copies = []
    for u in range(p.groups):
        for c in range(last):
            for i in range(p.deep):
                lines = pl.ds((u * p.deep + i) * p.lines + w + c * LANES, LANES)
                x = jnp.transpose(final[lines, :])
                for h in range(PACK):
                    at = pl.ds(i, p.blocks, stride=p.deep)
                    natural[(u * PACK + h) * last + c, at, :] = x[h * p.blocks : (h + 1) * p.blocks]
            for h in range(PACK):
                t = u * PACK + h
                copy = pltpu.make_async_copy(
                    natural.at[t * last + c, pl.ds(w, p.rows), :],
                    values.at[t, :, pl.ds(c * LANES, LANES)],
                    sems.at[t * last + c],
                )
                copy.start()
                copies.append(copy)

    def fetch(i, carry):
        for l in range(LANES):
            rows_of[pl.ds(i * LANES + l, 1), :] = final[pl.ds(address[i, l], 1), :]
        return carry

    lax.fori_loop(0, p.agents // LANES, fetch, 0)
    lane_id = lax.broadcasted_iota(jnp.int32, (LANES, LANES), 0)
    for i in range(p.agents // LANES):
        x = jnp.transpose(rows_of[pl.ds(i * LANES, LANES), :])
        picked = jnp.where(lane_id == lane_in[i : i + 1, :], x, 0.0)
        answers[i : i + 1, :] = jnp.sum(picked, axis=0, keepdims=True)
    for copy in copies:
        copy.wait()


def shift(value, axis, steps):
    count = lax.axis_size(axis)
    return lax.ppermute(value, axis, [(i, (i + steps) % count) for i in range(count)])


def swap(value, axis, parity):
    count = lax.axis_size(axis)
    assert count % 2 == 0
    return lax.ppermute(
        value, axis, [(i, (i + (1 if i % 2 == parity else -1)) % count) for i in range(count)]
    )


def on_device(map_codes, reward_table, start_cell, agent_task, actions):
    rows, cols = map_codes.shape
    tasks, codes = reward_table.shape
    steps, agents = actions.shape
    p = Plan(rows, cols, agents, steps, tasks, codes)
    vmem = pl.BlockSpec(memory_space=pltpu.VMEM)
    smem = pl.BlockSpec(memory_space=pltpu.SMEM)
    f32, i32 = jnp.float32, jnp.int32
    shape = jax.ShapeDtypeStruct
    fast = lambda dims, dtype: pltpu.VMEM(dims, dtype)
    near = lambda x: pltpu.with_memory_space_constraint(x, pltpu.VMEM)
    by_lane = (agents // LANES, LANES)

    def bind(kernel):
        def body(*refs):
            kernel(p, *refs)

        return body

    hist, to_right, to_left, address, lane = pl.pallas_call(
        bind(count_kernel),
        in_specs=[vmem] * 4,
        out_specs=[vmem] * 5,
        out_shape=[
            fast((p.tiles, p.ring, LANES), f32),
            fast((p.across_rows, LANES), f32),
            fast((p.across_rows, LANES), f32),
            shape(by_lane, i32),
            fast(by_lane, i32),
        ],
        scratch_shapes=[
            pltpu.VMEM((p.ring, agents), jnp.bfloat16),
            pltpu.VMEM((p.tiles * LANES, agents), jnp.bfloat16),
        ],
        name="count",
    )(actions, start_cell.reshape(by_lane), agent_task.reshape(by_lane), map_codes)
    from_left = shift(to_right, "gx", 1)
    from_right = shift(to_left, "gx", -1)
    key, first, second = pl.pallas_call(
        bind(across_kernel),
        in_specs=[vmem] * 4,
        out_specs=[vmem] * 3,
        out_shape=[
            fast((p.tiles, p.ring, LANES), i32),
            fast((p.down_rows, LANES), f32),
            fast((p.down_rows, LANES), f32),
        ],
        scratch_shapes=[
            pltpu.VMEM((p.tiles, p.ring, LANES), f32),
            pltpu.VMEM((p.tiles, p.rows, LANES), f32),
        ],
        name="across",
    )(near(hist), map_codes, near(from_left), near(from_right))
    first = swap(first, "gy", 0)
    second = swap(second, "gy", 1)
    outs = tasks * (p.tiles - 1)
    values, answers = pl.pallas_call(
        bind(sweep_kernel),
        in_specs=[vmem, vmem, vmem, vmem, smem, vmem],
        out_specs=[pl.BlockSpec(memory_space=pl.ANY), vmem],
        out_shape=[shape((tasks, rows, cols), f32), shape(by_lane, f32)],
        scratch_shapes=[
            pltpu.VMEM((tasks, LANES), f32),
            pltpu.VMEM((p.tiles, p.ring, LANES), i32),
            pltpu.VMEM(((tasks + 1) * p.tiles, p.ring, LANES), f32),
            pltpu.VMEM((p.planes + p.deep, p.lines, LANES), f32),
            pltpu.VMEM((p.planes * p.lines, LANES), f32),
            pltpu.VMEM((p.deep * p.lines, LANES), f32),
            pltpu.VMEM((p.planes * p.lines, LANES), f32),
            pltpu.VMEM((p.planes * SUB, LANES), f32),
            pltpu.VMEM((p.planes * p.lines, LANES), f32),
            pltpu.VMEM((outs, p.ring, LANES), f32),
            pltpu.VMEM((agents, LANES), f32),
            pltpu.SemaphoreType.DMA((outs,)),
        ],
        name="sweep",
    )(reward_table, near(key), near(first), near(second), address, near(lane))
    return values, answers.reshape(agents)


def solution(mesh):
    placed = (P("gy", "gx"), P(), P(("gx", "gy")), P(("gx", "gy")), P(None, ("gx", "gy")))
    return jax.shard_map(
        on_device,
        mesh=mesh,
        in_specs=placed,
        out_specs=(P(None, "gy", "gx"), P(("gx", "gy"))),
        check_vma=False,
    )
```

```python
import jax
import jax.numpy as jnp
from jax import lax
from jax.experimental import pallas as pl
from jax.experimental.pallas import tpu as pltpu
from jax.sharding import PartitionSpec as P


SWEEPS = 16
TERMINAL = 2
GAMMA = 0.95
PENALTY = 0.5
LANES = 128
SUB = 8
PACK = 2
UNROLL = 2


class Plan:
    def __init__(self, rows, cols, agents, steps, tasks, codes):
        self.rows, self.cols, self.agents = rows, cols, agents
        self.steps, self.tasks, self.codes = steps, tasks, codes
        self.near = steps
        self.wide = steps + SWEEPS
        self.ring = rows + 2 * self.wide
        self.tiles = cols // LANES + 1
        self.lines = cols + 2 * self.wide
        self.span = self.lines // SUB
        self.blocks = LANES // PACK
        self.deep = self.ring // self.blocks
        self.groups = tasks // PACK
        self.planes = self.groups * self.deep
        self.code_bits = (codes - 1).bit_length()
        self.message = rows + 2 * self.near
        self.half = self.message // 2
        self.band = self.wide + self.near
        self.pack = -(-(rows - self.half) // (LANES // self.wide * SUB)) * SUB
        self.across_rows = self.half + self.pack
        self.down_rows = self.tiles * self.band + (self.tiles - 1) * self.wide
        assert cols % LANES == 0 and rows % SUB == 0 and agents % LANES == 0
        assert 4 * self.wide <= LANES and self.near % SUB == 0 and self.wide % SUB == 0
        assert self.half % SUB == 0 and LANES % self.wide == 0 and self.near % 16 == 0
        assert self.band + self.wide + self.band <= LANES
        assert self.ring % self.blocks == 0 and self.lines % SUB == 0
        assert tasks % PACK == 0 and codes <= LANES
        self.magic = -(-(1 << 16) // self.deep)
        assert all((r * self.magic) >> 16 == r // self.deep for r in range(self.ring))


def lane_of(shape):
    return lax.broadcasted_iota(jnp.int32, shape, len(shape) - 1)


def split_cell(cell, cols):
    if cols & (cols - 1) == 0:
        return cell >> (cols.bit_length() - 1), cell & (cols - 1)
    return lax.div(cell, cols), lax.rem(cell, cols)


def one_hot(ids, positions):
    return jnp.where(ids == positions, 1.0, 0.0).astype(jnp.bfloat16)


def counted(row_hot, col_hot):
    return lax.dot_general(
        row_hot[...], col_hot[...], (((1,), (1,)), ((), ())), preferred_element_type=jnp.float32
    )


def right_roll(p, piece):
    return {"second": p.band, "code": LANES - p.wide}.get(piece, None if isinstance(piece, str) else (piece + 1) * p.wide % LANES)


def left_roll(p, piece):
    return {"second": LANES - p.band, "code": p.wide}.get(piece, None if isinstance(piece, str) else piece * p.wide)


def roll(x, amount):
    amount %= LANES
    return x if amount == 0 else pltpu.roll(x, amount, 1)


def bands_kernel(plan, act, start, code, right, left, ring_row, ring_col, row_hot, col_hot):
    p = plan
    last = p.tiles - 1
    ring_cols = p.tiles * LANES
    row_id = lax.broadcasted_iota(jnp.int32, (p.message, LANES), 0)
    row_id = jnp.where(row_id >= p.rows + p.near, row_id + p.ring - p.message, row_id)
    lines = (
        (0, p.near, last * LANES),
        (LANES - p.wide, p.wide, (last - 1) * LANES + LANES - p.wide),
        (LANES, p.wide, 0),
        (2 * LANES - p.near, p.near, ring_cols - p.near),
    )
    blank = 0
    for at, n, _ in lines + ((2 * LANES, 0, 0),):
        if at > blank:
            col_hot[blank:at, :] = jnp.zeros((at - blank, p.agents), jnp.bfloat16)
        blank = at + n
    for i in range(p.agents // LANES):
        here = slice(i * LANES, (i + 1) * LANES)
        a = act[:, here]
        one = lambda c: jnp.where(a == c, 1, 0)
        row, col = split_cell(start[i : i + 1, :], p.cols)
        row = row + jnp.sum(one(2) - one(1), axis=0, keepdims=True)
        col = col + jnp.sum(one(4) - one(3), axis=0, keepdims=True)
        row = jnp.where(row < 0, row + p.ring, row)
        col = jnp.where(col < 0, col + ring_cols, col)
        ring_row[i : i + 1, :] = row
        ring_col[i : i + 1, :] = col
        row_hot[:, here] = one_hot(row_id, row)
        for at, n, first in lines:
            ids = first + lax.broadcasted_iota(jnp.int32, (n, LANES), 0)
            col_hot[at : at + n, here] = one_hot(ids, col)
    counts = counted(row_hot, col_hot)
    lane = lane_of((p.half, LANES))
    for out, side, spare, shift, band in (
        (right, 0, p.near, right_roll, code[:, (last - 1) * LANES :]),
        (left, 1, LANES - p.near - p.band, left_roll, code[:, :LANES]),
    ):
        own = counts[:, side * LANES : (side + 1) * LANES]
        band = band.astype(jnp.float32)
        x = own[: p.half]
        x = jnp.where((lane >= spare) & (lane < spare + p.band), roll(own[p.half :], shift(p, "second")), x)
        lo = LANES - 2 * p.wide if side == 0 else p.wide
        x = jnp.where((lane >= lo) & (lane < lo + p.wide), roll(band[: p.half], shift(p, "code")), x)
        out[pl.ds(0, p.half), :] = x
        packed_lane = lane_of((p.pack, LANES))
        rest = jnp.zeros((p.pack, LANES), jnp.float32)
        for g in range(LANES // p.wide):
            lo = p.half + g * p.pack
            n = min(p.pack, p.rows - lo)
            if n <= 0:
                break
            y = roll(band[lo : lo + n], shift(p, g))
            if n < p.pack:
                y = jnp.concatenate([y, jnp.zeros((p.pack - n, LANES), jnp.float32)], axis=0)
            rest = jnp.where((packed_lane >= g * p.wide) & (packed_lane < (g + 1) * p.wide), y, rest)
        out[pl.ds(p.half, p.pack), :] = rest


def local_kernel(plan, ring_row, ring_col, task, table, hist, address, lane_out, looked, row_hot, col_hot):
    p = plan
    ring_cols = p.tiles * LANES
    row_id = lax.broadcasted_iota(jnp.int32, (p.ring, LANES), 0)
    col_id = lax.broadcasted_iota(jnp.int32, (ring_cols, LANES), 0)
    for i in range(p.agents // LANES):
        here = slice(i * LANES, (i + 1) * LANES)
        row = ring_row[i : i + 1, :]
        col = ring_col[i : i + 1, :]
        row_hot[:, here] = one_hot(row_id, row)
        col_hot[:, here] = one_hot(col_id, col)
        row = jnp.where(row >= p.rows + p.near, row - p.ring, row) + p.wide
        col = jnp.where(col >= p.cols + p.near, col - ring_cols, col) + p.wide
        t = task[i : i + 1, :]
        u = t // PACK
        block = (row * p.magic) >> 16
        lane_out[i : i + 1, :] = (t - u * PACK) * p.blocks + block
        plane = u * p.deep + row - block * p.deep
        address[i : i + 1, :] = plane * p.lines + col
    counts = counted(row_hot, col_hot)
    for t in range(p.tiles):
        hist[t] = counts[:, t * LANES : (t + 1) * LANES]
    looked[...] = jnp.zeros_like(looked)
    looked[pl.ds(0, p.tasks), pl.ds(0, p.codes)] = table[...]


def side_counts(p, message, shift, lo, n):
    parts = []
    for a, b in ((lo, min(lo + n, p.half)), (max(lo, p.half), lo + n)):
        if a < b and a < p.half:
            parts.append(message[pl.ds(a, b - a), :])
        elif a < b:
            parts.append(roll(message[pl.ds(a - p.half, b - a), :], -shift(p, "second")))
    return parts[0] if len(parts) == 1 else jnp.concatenate(parts, axis=0)


def side_codes(p, message, shift, lo, n):
    parts = []
    at = lo
    while at < lo + n:
        if at < p.half:
            end = min(lo + n, p.half)
            parts.append(roll(message[pl.ds(at, end - at), :], -shift(p, "code")))
        else:
            g, r = divmod(at - p.half, p.pack)
            end = min(lo + n, at - r + p.pack)
            parts.append(roll(message[pl.ds(p.half + r, end - at), :], -shift(p, g)))
        at = end
    return parts[0] if len(parts) == 1 else jnp.concatenate(parts, axis=0)


def merged_counts(p, hist, from_left, from_right, row, n):
    last = p.tiles - 1
    lo = row if row < p.rows + p.near else row - p.ring + p.message
    lane = lane_of((n, LANES))
    l = side_counts(p, from_left, right_roll, lo, n)
    r = side_counts(p, from_right, left_roll, lo, n)
    out = []
    for t in range(p.tiles):
        h = hist[t, pl.ds(row, n), :]
        if t == 0:
            h = h + jnp.where(lane < p.near, l, 0.0)
        if t == last - 1:
            h = h + jnp.where(lane >= LANES - p.near, r, 0.0)
        if t == last:
            h = h + jnp.where(lane >= LANES - p.wide, l, jnp.where(lane < p.wide, r, 0.0))
        out.append(h)
    return out


def merged_codes(p, code, from_left, from_right, row, n):
    last = p.tiles - 1
    lane = lane_of((n, LANES))
    out = [code[pl.ds(row, n), pl.ds(t * LANES, LANES)].astype(jnp.float32) for t in range(last)]
    l = side_codes(p, from_left, right_roll, row, n)
    r = side_codes(p, from_right, left_roll, row, n)
    out.append(jnp.where(lane >= LANES - p.wide, l, jnp.where(lane < p.wide, r, 0.0)))
    return out


def across_kernel(plan, hist, code, from_left, from_right, first, second):
    p = plan
    last = p.tiles - 1
    down_cnt = merged_counts(p, hist, from_left, from_right, p.rows - p.wide, p.band)
    up_near = merged_counts(p, hist, from_left, from_right, p.ring - p.near, p.near)
    up_wide = merged_counts(p, hist, from_left, from_right, 0, p.wide)
    down_code = merged_codes(p, code, from_left, from_right, p.rows - p.wide, p.wide)
    up_code = merged_codes(p, code, from_left, from_right, 0, p.wide)
    lane = lane_of((p.wide, LANES))
    inside = (lane >= p.wide) & (lane < LANES - p.wide)
    half = LANES // 2
    odd = lax.axis_index("gy") % 2 == 1

    def put(at, n, down, up):
        first[pl.ds(at, n), :] = jnp.where(odd, up, down)
        second[pl.ds(at, n), :] = jnp.where(odd, down, up)

    for t in range(p.tiles):
        down, up = down_cnt[t], jnp.concatenate([up_near[t], up_wide[t]], axis=0)
        if t < last:
            put(p.tiles * p.band + t * p.wide, p.wide, down_code[t], up_code[t])
        else:
            head = jnp.where(inside, roll(down_code[t], half), down[: p.wide])
            down = jnp.concatenate([head, down[p.wide :]], axis=0)
            tail = jnp.where(inside, roll(up_code[t], half), up[p.near :])
            up = jnp.concatenate([up[: p.near], tail], axis=0)
        put(t * p.band, p.band, down, up)


def look_up(p, looked):
    tables = [jnp.broadcast_to(looked[t : t + 1, :], (SUB, LANES)) for t in range(p.tasks)]

    def put(flat, c, at, code, count):
        crowd = PENALTY * count
        at = pl.ds(at, SUB)
        flat[p.tasks * p.tiles + c, at, :] = jnp.where(code < p.codes - TERMINAL, GAMMA, 0.0)
        for t in range(p.tasks):
            found = jnp.take_along_axis(tables[t], code, axis=1, mode="promise_in_bounds")
            flat[t * p.tiles + c, at, :] = found - crowd

    return put


def rewards_kernel(plan, hist, code, from_left, from_right, looked, flat, near):
    p = plan
    put = look_up(p, looked)
    for row in range(0, p.rows, SUB):
        counts = merged_counts(p, hist, from_left, from_right, row, SUB)
        codes = merged_codes(p, code, from_left, from_right, row, SUB)
        for c in range(p.tiles):
            put(flat, c, row + p.wide, codes[c].astype(jnp.int32), counts[c])
    for at, row in ((0, p.rows), (p.near, p.ring - p.near)):
        counts = merged_counts(p, hist, from_left, from_right, row, p.near)
        for c in range(p.tiles):
            near[c, pl.ds(at, p.near), :] = counts[c]


def sweep_kernel(plan, looked, flat_in, near, first, second, address_in, lane_in, values, answers, flat,
                 turned, reward, gain, value, edge, final, natural, rows_of, address, sems):
    p = plan
    del flat_in
    fetch_address = pltpu.make_async_copy(address_in, address, sems.at[p.tasks * (p.tiles - 1)])
    fetch_address.start()
    last = p.tiles - 1
    odd = lax.axis_index("gy") % 2 == 1
    half = LANES // 2
    w, s = p.wide, p.near

    def above(at, n):
        at = pl.ds(at, n)
        return jnp.where(odd, first[at, :], second[at, :])

    def below(at, n):
        at = pl.ds(at, n)
        return jnp.where(odd, second[at, :], first[at, :])

    put = look_up(p, looked)
    for c in range(p.tiles):
        base = c * p.band
        code_base = p.tiles * p.band + c * w
        for at, extra in ((0, above(base + w, s)), (p.rows - s, below(base, s))):
            at = pl.ds(w + at, s)
            for t in range(p.tasks):
                flat[t * p.tiles + c, at, :] = flat[t * p.tiles + c, at, :] - PENALTY * extra
        for row in range(0, w, SUB):
            count = above(base + row, SUB)
            code = above(code_base + row, SUB) if c < last else roll(count, half)
            if row >= w - s:
                count = count + near[c, pl.ds(s + row - (w - s), SUB), :]
            put(flat, c, row, code.astype(jnp.int32) & (LANES - 1), count)
            count = below(base + s + row, SUB)
            code = below(code_base + row, SUB) if c < last else roll(count, half)
            if row < s:
                count = count + near[c, pl.ds(row, SUB), :]
            put(flat, c, w + p.rows + row, code.astype(jnp.int32) & (LANES - 1), count)

    for u in range(p.groups + 1):
        for i in range(p.deep):
            for c in range(p.tiles):
                parts = []
                for h in range(PACK):
                    t = u * PACK + h if u < p.groups else p.tasks
                    parts.append(flat[t * p.tiles + c, pl.ds(i, p.blocks, stride=p.deep), :])
                x = jnp.transpose(jnp.concatenate(parts, axis=0))
                if c < last:
                    turned[u * p.deep + i, pl.ds(w + c * LANES, LANES), :] = x
                else:
                    turned[u * p.deep + i, pl.ds(w + p.cols, w), :] = x[:w]
                    turned[u * p.deep + i, pl.ds(0, w), :] = x[LANES - w :]

    for q in range(p.span):
        for n in range(p.planes + p.deep):
            x = turned[n, pl.ds(q, SUB, stride=p.span), :]
            if n < p.planes:
                at = pl.ds((q * p.planes + n) * SUB, SUB)
                reward[at, :] = x
            else:
                gain[pl.ds((q * p.deep + n - p.planes) * SUB, SUB), :] = x

    def sweep(held, put):
        load = lambda q: [held[pl.ds((q * p.planes + n) * SUB, SUB), :] for n in range(p.planes)]
        now = load(0)
        before = [pltpu.roll(x, 1, 0) for x in load(p.span - 1)]
        for n in range(p.planes):
            edge[pl.ds(n * SUB, SUB), :] = pltpu.roll(now[n], SUB - 1, 0)
        for q in range(p.span):
            if q + 1 < p.span:
                after = load(q + 1)
            else:
                after = [edge[pl.ds(n * SUB, SUB), :] for n in range(p.planes)]
            for i in range(p.deep):
                g = gain[pl.ds((q * p.deep + i) * SUB, SUB), :]
                for u in range(p.groups):
                    n = u * p.deep + i
                    up = now[n - 1] if i > 0 else pltpu.roll(now[n + p.deep - 1], 1, 1)
                    down = now[n + 1] if i + 1 < p.deep else pltpu.roll(now[n + 1 - p.deep], LANES - 1, 1)
                    best = jnp.maximum(jnp.maximum(up, down), jnp.maximum(before[n], after[n]))
                    put(q, n, reward[pl.ds((q * p.planes + n) * SUB, SUB), :] + g * best)
            before, now = now, after

    def put_value(q, n, x):
        value[pl.ds((q * p.planes + n) * SUB, SUB), :] = x

    def put_final(q, n, x):
        final[pl.ds(n * p.lines + q, SUB, stride=p.span), :] = x

    def sweeps(_, carry):
        for _ in range(UNROLL):
            sweep(value, put_value)
        return carry

    assert (SWEEPS - 2) % UNROLL == 0
    sweep(reward, put_value)
    lax.fori_loop(0, (SWEEPS - 2) // UNROLL, sweeps, 0)
    sweep(value, put_final)
    fetch_address.wait()

    copies = []
    for u in range(p.groups):
        for c in range(last):
            for i in range(p.deep):
                lines = pl.ds((u * p.deep + i) * p.lines + w + c * LANES, LANES)
                x = jnp.transpose(final[lines, :])
                for h in range(PACK):
                    at = pl.ds(i, p.blocks, stride=p.deep)
                    natural[(u * PACK + h) * last + c, at, :] = x[h * p.blocks : (h + 1) * p.blocks]
            for h in range(PACK):
                t = u * PACK + h
                copy = pltpu.make_async_copy(
                    natural.at[t * last + c, pl.ds(w, p.rows), :],
                    values.at[t, :, pl.ds(c * LANES, LANES)],
                    sems.at[t * last + c],
                )
                copy.start()
                copies.append(copy)

    def fetch(i, carry):
        for l in range(LANES):
            rows_of[pl.ds(i * LANES + l, 1), :] = final[pl.ds(address[i, l], 1), :]
        return carry

    lax.fori_loop(0, p.agents // LANES, fetch, 0)
    lane_id = lax.broadcasted_iota(jnp.int32, (LANES, LANES), 0)
    for i in range(p.agents // LANES):
        x = jnp.transpose(rows_of[pl.ds(i * LANES, LANES), :])
        picked = jnp.where(lane_id == lane_in[i : i + 1, :], x, 0.0)
        answers[i : i + 1, :] = jnp.sum(picked, axis=0, keepdims=True)
    for copy in copies:
        copy.wait()


def shift(value, axis, steps):
    count = lax.axis_size(axis)
    return lax.ppermute(value, axis, [(i, (i + steps) % count) for i in range(count)])


def swap(value, axis, parity):
    count = lax.axis_size(axis)
    assert count % 2 == 0
    return lax.ppermute(
        value, axis, [(i, (i + (1 if i % 2 == parity else -1)) % count) for i in range(count)]
    )


def on_device(map_codes, reward_table, start_cell, agent_task, actions):
    rows, cols = map_codes.shape
    tasks, codes = reward_table.shape
    steps, agents = actions.shape
    p = Plan(rows, cols, agents, steps, tasks, codes)
    vmem = pl.BlockSpec(memory_space=pltpu.VMEM)
    smem = pl.BlockSpec(memory_space=pltpu.SMEM)
    f32, i32 = jnp.float32, jnp.int32
    shape = jax.ShapeDtypeStruct
    fast = lambda dims, dtype: pltpu.VMEM(dims, dtype)
    near = lambda x: pltpu.with_memory_space_constraint(x, pltpu.VMEM)
    by_lane = (agents // LANES, LANES)

    def bind(kernel):
        def body(*refs):
            kernel(p, *refs)

        return body

    to_right, to_left, ring_row, ring_col = pl.pallas_call(
        bind(bands_kernel),
        in_specs=[vmem] * 3,
        out_specs=[vmem] * 4,
        out_shape=[
            fast((p.across_rows, LANES), f32),
            fast((p.across_rows, LANES), f32),
            fast(by_lane, i32),
            fast(by_lane, i32),
        ],
        scratch_shapes=[
            pltpu.VMEM((p.message, agents), jnp.bfloat16),
            pltpu.VMEM((2 * LANES, agents), jnp.bfloat16),
        ],
        name="bands",
    )(actions, start_cell.reshape(by_lane), map_codes)
    from_left = shift(to_right, "gx", 1)
    from_right = shift(to_left, "gx", -1)
    hist, address, lane, looked = pl.pallas_call(
        bind(local_kernel),
        in_specs=[vmem] * 4,
        out_specs=[vmem] * 4,
        out_shape=[
            fast((p.tiles, p.ring, LANES), f32),
            fast(by_lane, i32),
            fast(by_lane, i32),
            fast((SUB, LANES), f32),
        ],
        scratch_shapes=[
            pltpu.VMEM((p.ring, agents), jnp.bfloat16),
            pltpu.VMEM((p.tiles * LANES, agents), jnp.bfloat16),
        ],
        name="local",
    )(near(ring_row), near(ring_col), agent_task.reshape(by_lane), reward_table)
    sides = (near(hist), map_codes, near(from_left), near(from_right))
    first, second = pl.pallas_call(
        bind(across_kernel),
        in_specs=[vmem] * 4,
        out_specs=[vmem] * 2,
        out_shape=[fast((p.down_rows, LANES), f32), fast((p.down_rows, LANES), f32)],
        name="across",
    )(*sides)
    first = swap(first, "gy", 0)
    second = swap(second, "gy", 1)
    flats = ((tasks + 1) * p.tiles, p.ring, LANES)
    flat, edges = pl.pallas_call(
        bind(rewards_kernel),
        in_specs=[vmem] * 5,
        out_specs=[vmem] * 2,
        out_shape=[fast(flats, f32), fast((p.tiles, 2 * p.near, LANES), f32)],
        name="rewards",
    )(*sides, near(looked))
    outs = tasks * (p.tiles - 1)
    values, answers, _ = pl.pallas_call(
        bind(sweep_kernel),
        in_specs=[vmem] * 7,
        out_specs=[pl.BlockSpec(memory_space=pl.ANY), vmem, vmem],
        out_shape=[shape((tasks, rows, cols), f32), shape(by_lane, f32), fast(flats, f32)],
        scratch_shapes=[
            pltpu.VMEM((p.planes + p.deep, p.lines, LANES), f32),
            pltpu.VMEM((p.planes * p.lines, LANES), f32),
            pltpu.VMEM((p.deep * p.lines, LANES), f32),
            pltpu.VMEM((p.planes * p.lines, LANES), f32),
            pltpu.VMEM((p.planes * SUB, LANES), f32),
            pltpu.VMEM((p.planes * p.lines, LANES), f32),
            pltpu.VMEM((outs, p.ring, LANES), f32),
            pltpu.VMEM((agents, LANES), f32),
            pltpu.SMEM(by_lane, i32),
            pltpu.SemaphoreType.DMA((outs + 1,)),
        ],
        input_output_aliases={1: 2},
        name="sweep",
    )(near(looked), near(flat), near(edges), near(first), near(second), near(address), near(lane))
    return values, answers.reshape(agents)


def solution(mesh):
    placed = (P("gy", "gx"), P(), P(("gx", "gy")), P(("gx", "gy")), P(None, ("gx", "gy")))
    return jax.shard_map(
        on_device,
        mesh=mesh,
        in_specs=placed,
        out_specs=(P(None, "gy", "gx"), P(("gx", "gy"))),
        check_vma=False,
    )
```

```python
import jax
import jax.numpy as jnp
from jax import lax
from jax.experimental import pallas as pl
from jax.experimental.pallas import tpu as pltpu
from jax.sharding import PartitionSpec as P


SWEEPS = 16
TERMINAL = 2
GAMMA = 0.95
PENALTY = 0.5
LANES = 128
SUB = 8
PACK = 2
UNROLL = 2


class Plan:
    def __init__(self, rows, cols, agents, steps, tasks, codes):
        self.rows, self.cols, self.agents = rows, cols, agents
        self.steps, self.tasks, self.codes = steps, tasks, codes
        self.near = steps
        self.wide = steps + SWEEPS
        self.ring = rows + 2 * self.wide
        self.tiles = cols // LANES + 1
        self.lines = cols + 2 * self.wide
        self.span = self.lines // SUB
        self.blocks = LANES // PACK
        self.deep = self.ring // self.blocks
        self.groups = tasks // PACK
        self.planes = self.groups * self.deep
        self.code_bits = (codes - 1).bit_length()
        self.message = rows + 2 * self.near
        self.half = self.message // 2
        self.band = self.wide + self.near
        self.pack = -(-(rows - self.half) // (LANES // self.wide * SUB)) * SUB
        self.across_rows = self.half + self.pack
        self.down_rows = self.tiles * self.band + (self.tiles - 1) * self.wide
        assert cols % LANES == 0 and rows % SUB == 0 and agents % LANES == 0
        assert 4 * self.wide <= LANES and self.near % SUB == 0 and self.wide % SUB == 0
        assert self.half % SUB == 0 and LANES % self.wide == 0 and self.near % 16 == 0
        assert self.band + self.wide + self.band <= LANES
        assert self.ring % self.blocks == 0 and self.lines % SUB == 0
        assert tasks % PACK == 0 and codes <= LANES
        self.magic = -(-(1 << 16) // self.deep)
        assert all((r * self.magic) >> 16 == r // self.deep for r in range(self.ring))


def lane_of(shape):
    return lax.broadcasted_iota(jnp.int32, shape, len(shape) - 1)


def split_cell(cell, cols):
    if cols & (cols - 1) == 0:
        return cell >> (cols.bit_length() - 1), cell & (cols - 1)
    return lax.div(cell, cols), lax.rem(cell, cols)


def one_hot(ids, positions):
    return jnp.where(ids == positions, 1.0, 0.0).astype(jnp.bfloat16)


def counted(row_hot, col_hot):
    return lax.dot_general(
        row_hot[...], col_hot[...], (((1,), (1,)), ((), ())), preferred_element_type=jnp.float32
    )


def right_roll(p, piece):
    return {"second": p.band, "code": LANES - p.wide}.get(piece, None if isinstance(piece, str) else (piece + 1) * p.wide % LANES)


def left_roll(p, piece):
    return {"second": LANES - p.band, "code": p.wide}.get(piece, None if isinstance(piece, str) else piece * p.wide)


def roll(x, amount):
    amount %= LANES
    return x if amount == 0 else pltpu.roll(x, amount, 1)


def bands_kernel(plan, act, start, code, right, left, ring_row, ring_col, row_hot, col_hot):
    p = plan
    last = p.tiles - 1
    ring_cols = p.tiles * LANES
    row_id = lax.broadcasted_iota(jnp.int32, (p.message, LANES), 0)
    row_id = jnp.where(row_id >= p.rows + p.near, row_id + p.ring - p.message, row_id)
    lines = (
        (0, p.near, last * LANES),
        (LANES - p.wide, p.wide, (last - 1) * LANES + LANES - p.wide),
        (LANES, p.wide, 0),
        (2 * LANES - p.near, p.near, ring_cols - p.near),
    )
    blank = 0
    for at, n, _ in lines + ((2 * LANES, 0, 0),):
        if at > blank:
            col_hot[blank:at, :] = jnp.zeros((at - blank, p.agents), jnp.bfloat16)
        blank = at + n
    for i in range(p.agents // LANES):
        here = slice(i * LANES, (i + 1) * LANES)
        a = act[:, here]
        one = lambda c: jnp.where(a == c, 1, 0)
        row, col = split_cell(start[i : i + 1, :], p.cols)
        row = row + jnp.sum(one(2) - one(1), axis=0, keepdims=True)
        col = col + jnp.sum(one(4) - one(3), axis=0, keepdims=True)
        row = jnp.where(row < 0, row + p.ring, row)
        col = jnp.where(col < 0, col + ring_cols, col)
        ring_row[i : i + 1, :] = row
        ring_col[i : i + 1, :] = col
        row_hot[:, here] = one_hot(row_id, row)
        for at, n, first in lines:
            ids = first + lax.broadcasted_iota(jnp.int32, (n, LANES), 0)
            col_hot[at : at + n, here] = one_hot(ids, col)
    counts = counted(row_hot, col_hot)
    lane = lane_of((p.half, LANES))
    for out, side, spare, shift, band in (
        (right, 0, p.near, right_roll, code[:, (last - 1) * LANES :]),
        (left, 1, LANES - p.near - p.band, left_roll, code[:, :LANES]),
    ):
        own = counts[:, side * LANES : (side + 1) * LANES]
        band = band.astype(jnp.float32)
        x = own[: p.half]
        x = jnp.where((lane >= spare) & (lane < spare + p.band), roll(own[p.half :], shift(p, "second")), x)
        lo = LANES - 2 * p.wide if side == 0 else p.wide
        x = jnp.where((lane >= lo) & (lane < lo + p.wide), roll(band[: p.half], shift(p, "code")), x)
        out[pl.ds(0, p.half), :] = x
        packed_lane = lane_of((p.pack, LANES))
        rest = jnp.zeros((p.pack, LANES), jnp.float32)
        for g in range(LANES // p.wide):
            lo = p.half + g * p.pack
            n = min(p.pack, p.rows - lo)
            if n <= 0:
                break
            y = roll(band[lo : lo + n], shift(p, g))
            if n < p.pack:
                y = jnp.concatenate([y, jnp.zeros((p.pack - n, LANES), jnp.float32)], axis=0)
            rest = jnp.where((packed_lane >= g * p.wide) & (packed_lane < (g + 1) * p.wide), y, rest)
        out[pl.ds(p.half, p.pack), :] = rest


def local_kernel(
    plan, ring_row, ring_col, task, table, code, hist, address, lane_out, looked, code_out, row_hot, col_hot
):
    p = plan
    ring_cols = p.tiles * LANES
    row_id = lax.broadcasted_iota(jnp.int32, (p.ring, LANES), 0)
    col_id = lax.broadcasted_iota(jnp.int32, (ring_cols, LANES), 0)
    for i in range(p.agents // LANES):
        here = slice(i * LANES, (i + 1) * LANES)
        row = ring_row[i : i + 1, :]
        col = ring_col[i : i + 1, :]
        row_hot[:, here] = one_hot(row_id, row)
        col_hot[:, here] = one_hot(col_id, col)
        row = jnp.where(row >= p.rows + p.near, row - p.ring, row) + p.wide
        col = jnp.where(col >= p.cols + p.near, col - ring_cols, col) + p.wide
        t = task[i : i + 1, :]
        u = t // PACK
        block = (row * p.magic) >> 16
        lane_out[i : i + 1, :] = (t - u * PACK) * p.blocks + block
        plane = u * p.deep + row - block * p.deep
        address[i : i + 1, :] = plane * p.lines + col
    counts = counted(row_hot, col_hot)
    for t in range(p.tiles):
        hist[t] = counts[:, t * LANES : (t + 1) * LANES]
    code_out[...] = code[...].astype(jnp.float32)
    looked[...] = jnp.zeros_like(looked)
    looked[pl.ds(0, p.tasks), pl.ds(0, p.codes)] = table[...]


def side_counts(p, message, shift, lo, n):
    parts = []
    for a, b in ((lo, min(lo + n, p.half)), (max(lo, p.half), lo + n)):
        if a < b and a < p.half:
            parts.append(message[pl.ds(a, b - a), :])
        elif a < b:
            parts.append(roll(message[pl.ds(a - p.half, b - a), :], -shift(p, "second")))
    return parts[0] if len(parts) == 1 else jnp.concatenate(parts, axis=0)


def side_codes(p, message, shift, lo, n):
    parts = []
    at = lo
    while at < lo + n:
        if at < p.half:
            end = min(lo + n, p.half)
            parts.append(roll(message[pl.ds(at, end - at), :], -shift(p, "code")))
        else:
            g, r = divmod(at - p.half, p.pack)
            end = min(lo + n, at - r + p.pack)
            parts.append(roll(message[pl.ds(p.half + r, end - at), :], -shift(p, g)))
        at = end
    return parts[0] if len(parts) == 1 else jnp.concatenate(parts, axis=0)


def merged_counts(p, hist, from_left, from_right, row, n):
    last = p.tiles - 1
    lo = row if row < p.rows + p.near else row - p.ring + p.message
    lane = lane_of((n, LANES))
    l = side_counts(p, from_left, right_roll, lo, n)
    r = side_counts(p, from_right, left_roll, lo, n)
    out = []
    for t in range(p.tiles):
        h = hist[t, pl.ds(row, n), :]
        if t == 0:
            h = h + jnp.where(lane < p.near, l, 0.0)
        if t == last - 1:
            h = h + jnp.where(lane >= LANES - p.near, r, 0.0)
        if t == last:
            h = h + jnp.where(lane >= LANES - p.wide, l, jnp.where(lane < p.wide, r, 0.0))
        out.append(h)
    return out


def merged_codes(p, code, from_left, from_right, row, n):
    last = p.tiles - 1
    lane = lane_of((n, LANES))
    out = [code[pl.ds(row, n), pl.ds(t * LANES, LANES)] for t in range(last)]
    l = side_codes(p, from_left, right_roll, row, n)
    r = side_codes(p, from_right, left_roll, row, n)
    out.append(jnp.where(lane >= LANES - p.wide, l, jnp.where(lane < p.wide, r, 0.0)))
    return out


def across_kernel(plan, hist, code, from_left, from_right, first, second):
    p = plan
    last = p.tiles - 1
    down_cnt = merged_counts(p, hist, from_left, from_right, p.rows - p.wide, p.band)
    up_near = merged_counts(p, hist, from_left, from_right, p.ring - p.near, p.near)
    up_wide = merged_counts(p, hist, from_left, from_right, 0, p.wide)
    down_code = merged_codes(p, code, from_left, from_right, p.rows - p.wide, p.wide)
    up_code = merged_codes(p, code, from_left, from_right, 0, p.wide)
    lane = lane_of((p.wide, LANES))
    inside = (lane >= p.wide) & (lane < LANES - p.wide)
    half = LANES // 2
    odd = lax.axis_index("gy") % 2 == 1

    def put(at, n, down, up):
        first[pl.ds(at, n), :] = jnp.where(odd, up, down)
        second[pl.ds(at, n), :] = jnp.where(odd, down, up)

    for t in range(p.tiles):
        down, up = down_cnt[t], jnp.concatenate([up_near[t], up_wide[t]], axis=0)
        if t < last:
            put(p.tiles * p.band + t * p.wide, p.wide, down_code[t], up_code[t])
        else:
            head = jnp.where(inside, roll(down_code[t], half), down[: p.wide])
            down = jnp.concatenate([head, down[p.wide :]], axis=0)
            tail = jnp.where(inside, roll(up_code[t], half), up[p.near :])
            up = jnp.concatenate([up[: p.near], tail], axis=0)
        put(t * p.band, p.band, down, up)


def look_up(p, looked):
    tables = [jnp.broadcast_to(looked[t : t + 1, :], (SUB, LANES)) for t in range(p.tasks)]

    def put(flat, c, at, code, count):
        crowd = PENALTY * count
        at = pl.ds(at, SUB)
        flat[p.tasks * p.tiles + c, at, :] = jnp.where(code < p.codes - TERMINAL, GAMMA, 0.0)
        for t in range(p.tasks):
            found = jnp.take_along_axis(tables[t], code, axis=1, mode="promise_in_bounds")
            flat[t * p.tiles + c, at, :] = found - crowd

    return put


def rewards_kernel(plan, hist, code, from_left, from_right, looked, flat, near):
    p = plan
    put = look_up(p, looked)
    for row in range(0, p.rows, SUB):
        counts = merged_counts(p, hist, from_left, from_right, row, SUB)
        codes = merged_codes(p, code, from_left, from_right, row, SUB)
        for c in range(p.tiles):
            put(flat, c, row + p.wide, codes[c].astype(jnp.int32), counts[c])
    for at, row in ((0, p.rows), (p.near, p.ring - p.near)):
        counts = merged_counts(p, hist, from_left, from_right, row, p.near)
        for c in range(p.tiles):
            near[c, pl.ds(at, p.near), :] = counts[c]


def sweep_kernel(plan, looked, flat_in, near, first, second, address_in, lane_in, values, answers, flat,
                 turned, reward, gain, value, edge, final, natural, rows_of, address, sems):
    p = plan
    del flat_in
    fetch_address = pltpu.make_async_copy(address_in, address, sems.at[p.tasks * (p.tiles - 1)])
    fetch_address.start()
    last = p.tiles - 1
    odd = lax.axis_index("gy") % 2 == 1
    half = LANES // 2
    w, s = p.wide, p.near

    def above(at, n):
        at = pl.ds(at, n)
        return jnp.where(odd, first[at, :], second[at, :])

    def below(at, n):
        at = pl.ds(at, n)
        return jnp.where(odd, second[at, :], first[at, :])

    put = look_up(p, looked)
    for c in range(p.tiles):
        base = c * p.band
        code_base = p.tiles * p.band + c * w
        for at, extra in ((0, above(base + w, s)), (p.rows - s, below(base, s))):
            at = pl.ds(w + at, s)
            for t in range(p.tasks):
                flat[t * p.tiles + c, at, :] = flat[t * p.tiles + c, at, :] - PENALTY * extra
        for row in range(0, w, SUB):
            count = above(base + row, SUB)
            code = above(code_base + row, SUB) if c < last else roll(count, half)
            if row >= w - s:
                count = count + near[c, pl.ds(s + row - (w - s), SUB), :]
            put(flat, c, row, code.astype(jnp.int32) & (LANES - 1), count)
            count = below(base + s + row, SUB)
            code = below(code_base + row, SUB) if c < last else roll(count, half)
            if row < s:
                count = count + near[c, pl.ds(row, SUB), :]
            put(flat, c, w + p.rows + row, code.astype(jnp.int32) & (LANES - 1), count)

    for u in range(p.groups + 1):
        for i in range(p.deep):
            for c in range(p.tiles):
                parts = []
                for h in range(PACK):
                    t = u * PACK + h if u < p.groups else p.tasks
                    parts.append(flat[t * p.tiles + c, pl.ds(i, p.blocks, stride=p.deep), :])
                x = jnp.transpose(jnp.concatenate(parts, axis=0))
                if c < last:
                    turned[u * p.deep + i, pl.ds(w + c * LANES, LANES), :] = x
                else:
                    turned[u * p.deep + i, pl.ds(w + p.cols, w), :] = x[:w]
                    turned[u * p.deep + i, pl.ds(0, w), :] = x[LANES - w :]

    for q in range(p.span):
        for n in range(p.planes + p.deep):
            x = turned[n, pl.ds(q, SUB, stride=p.span), :]
            if n < p.planes:
                at = pl.ds((q * p.planes + n) * SUB, SUB)
                reward[at, :] = x
            else:
                gain[pl.ds((q * p.deep + n - p.planes) * SUB, SUB), :] = x

    def sweep(held, put):
        load = lambda q: [held[pl.ds((q * p.planes + n) * SUB, SUB), :] for n in range(p.planes)]
        now = load(0)
        before = [pltpu.roll(x, 1, 0) for x in load(p.span - 1)]
        for n in range(p.planes):
            edge[pl.ds(n * SUB, SUB), :] = pltpu.roll(now[n], SUB - 1, 0)
        for q in range(p.span):
            if q + 1 < p.span:
                after = load(q + 1)
            else:
                after = [edge[pl.ds(n * SUB, SUB), :] for n in range(p.planes)]
            for i in range(p.deep):
                g = gain[pl.ds((q * p.deep + i) * SUB, SUB), :]
                for u in range(p.groups):
                    n = u * p.deep + i
                    up = now[n - 1] if i > 0 else pltpu.roll(now[n + p.deep - 1], 1, 1)
                    down = now[n + 1] if i + 1 < p.deep else pltpu.roll(now[n + 1 - p.deep], LANES - 1, 1)
                    best = jnp.maximum(jnp.maximum(up, down), jnp.maximum(before[n], after[n]))
                    put(q, n, reward[pl.ds((q * p.planes + n) * SUB, SUB), :] + g * best)
            before, now = now, after

    def put_value(q, n, x):
        value[pl.ds((q * p.planes + n) * SUB, SUB), :] = x

    def put_final(q, n, x):
        final[pl.ds(n * p.lines + q, SUB, stride=p.span), :] = x

    def sweeps(_, carry):
        for _ in range(UNROLL):
            sweep(value, put_value)
        return carry

    assert (SWEEPS - 2) % UNROLL == 0
    sweep(reward, put_value)
    lax.fori_loop(0, (SWEEPS - 2) // UNROLL, sweeps, 0)
    sweep(value, put_final)
    fetch_address.wait()

    copies = []
    for u in range(p.groups):
        for c in range(last):
            for i in range(p.deep):
                lines = pl.ds((u * p.deep + i) * p.lines + w + c * LANES, LANES)
                x = jnp.transpose(final[lines, :])
                for h in range(PACK):
                    at = pl.ds(i, p.blocks, stride=p.deep)
                    natural[(u * PACK + h) * last + c, at, :] = x[h * p.blocks : (h + 1) * p.blocks]
            for h in range(PACK):
                t = u * PACK + h
                copy = pltpu.make_async_copy(
                    natural.at[t * last + c, pl.ds(w, p.rows), :],
                    values.at[t, :, pl.ds(c * LANES, LANES)],
                    sems.at[t * last + c],
                )
                copy.start()
                copies.append(copy)

    def fetch(i, carry):
        for l in range(LANES):
            rows_of[pl.ds(i * LANES + l, 1), :] = final[pl.ds(address[i, l], 1), :]
        return carry

    lax.fori_loop(0, p.agents // LANES, fetch, 0)
    lane_id = lax.broadcasted_iota(jnp.int32, (LANES, LANES), 0)
    for i in range(p.agents // LANES):
        x = jnp.transpose(rows_of[pl.ds(i * LANES, LANES), :])
        picked = jnp.where(lane_id == lane_in[i : i + 1, :], x, 0.0)
        answers[i : i + 1, :] = jnp.sum(picked, axis=0, keepdims=True)
    for copy in copies:
        copy.wait()


def shift(value, axis, steps):
    count = lax.axis_size(axis)
    return lax.ppermute(value, axis, [(i, (i + steps) % count) for i in range(count)])


def swap(value, axis, parity):
    count = lax.axis_size(axis)
    assert count % 2 == 0
    return lax.ppermute(
        value, axis, [(i, (i + (1 if i % 2 == parity else -1)) % count) for i in range(count)]
    )


def on_device(map_codes, reward_table, start_cell, agent_task, actions):
    rows, cols = map_codes.shape
    tasks, codes = reward_table.shape
    steps, agents = actions.shape
    p = Plan(rows, cols, agents, steps, tasks, codes)
    vmem = pl.BlockSpec(memory_space=pltpu.VMEM)
    smem = pl.BlockSpec(memory_space=pltpu.SMEM)
    f32, i32 = jnp.float32, jnp.int32
    shape = jax.ShapeDtypeStruct
    fast = lambda dims, dtype: pltpu.VMEM(dims, dtype)
    near = lambda x: pltpu.with_memory_space_constraint(x, pltpu.VMEM)
    by_lane = (agents // LANES, LANES)

    def bind(kernel):
        def body(*refs):
            kernel(p, *refs)

        return body

    to_right, to_left, ring_row, ring_col = pl.pallas_call(
        bind(bands_kernel),
        in_specs=[vmem] * 3,
        out_specs=[vmem] * 4,
        out_shape=[
            fast((p.across_rows, LANES), f32),
            fast((p.across_rows, LANES), f32),
            fast(by_lane, i32),
            fast(by_lane, i32),
        ],
        scratch_shapes=[
            pltpu.VMEM((p.message, agents), jnp.bfloat16),
            pltpu.VMEM((2 * LANES, agents), jnp.bfloat16),
        ],
        compiler_params=pltpu.CompilerParams(vmem_limit_bytes=12 << 20),
        name="bands",
    )(actions, start_cell.reshape(by_lane), map_codes)
    from_left = shift(to_right, "gx", 1)
    from_right = shift(to_left, "gx", -1)
    hist, address, lane, looked, kept = pl.pallas_call(
        bind(local_kernel),
        in_specs=[vmem] * 5,
        out_specs=[vmem] * 5,
        out_shape=[
            fast((p.tiles, p.ring, LANES), f32),
            fast(by_lane, i32),
            fast(by_lane, i32),
            fast((SUB, LANES), f32),
            fast((rows, cols), f32),
        ],
        scratch_shapes=[
            pltpu.VMEM((p.ring, agents), jnp.bfloat16),
            pltpu.VMEM((p.tiles * LANES, agents), jnp.bfloat16),
        ],
        compiler_params=pltpu.CompilerParams(vmem_limit_bytes=12 << 20),
        name="local",
    )(near(ring_row), near(ring_col), agent_task.reshape(by_lane), reward_table, map_codes)
    sides = (near(hist), near(kept), near(from_left), near(from_right))
    first, second = pl.pallas_call(
        bind(across_kernel),
        in_specs=[vmem] * 4,
        out_specs=[vmem] * 2,
        out_shape=[fast((p.down_rows, LANES), f32), fast((p.down_rows, LANES), f32)],
        compiler_params=pltpu.CompilerParams(vmem_limit_bytes=8 << 20),
        name="across",
    )(*sides)
    first = swap(first, "gy", 0)
    second = swap(second, "gy", 1)
    flats = ((tasks + 1) * p.tiles, p.ring, LANES)
    flat, edges = pl.pallas_call(
        bind(rewards_kernel),
        in_specs=[vmem] * 5,
        out_specs=[vmem] * 2,
        out_shape=[fast(flats, f32), fast((p.tiles, 2 * p.near, LANES), f32)],
        compiler_params=pltpu.CompilerParams(vmem_limit_bytes=12 << 20),
        name="rewards",
    )(*sides, near(looked))
    outs = tasks * (p.tiles - 1)
    values, answers, _ = pl.pallas_call(
        bind(sweep_kernel),
        in_specs=[vmem] * 7,
        out_specs=[pl.BlockSpec(memory_space=pl.ANY), vmem, vmem],
        out_shape=[shape((tasks, rows, cols), f32), shape(by_lane, f32), fast(flats, f32)],
        scratch_shapes=[
            pltpu.VMEM((p.planes + p.deep, p.lines, LANES), f32),
            pltpu.VMEM((p.planes * p.lines, LANES), f32),
            pltpu.VMEM((p.deep * p.lines, LANES), f32),
            pltpu.VMEM((p.planes * p.lines, LANES), f32),
            pltpu.VMEM((p.planes * SUB, LANES), f32),
            pltpu.VMEM((p.planes * p.lines, LANES), f32),
            pltpu.VMEM((outs, p.ring, LANES), f32),
            pltpu.VMEM((agents, LANES), f32),
            pltpu.SMEM(by_lane, i32),
            pltpu.SemaphoreType.DMA((outs + 1,)),
        ],
        input_output_aliases={1: 2},
        compiler_params=pltpu.CompilerParams(vmem_limit_bytes=24 << 20),
        name="sweep",
    )(near(looked), near(flat), near(edges), near(first), near(second), near(address), near(lane))
    return values, answers.reshape(agents)


def solution(mesh):
    placed = (P("gy", "gx"), P(), P(("gx", "gy")), P(("gx", "gy")), P(None, ("gx", "gy")))
    return jax.shard_map(
        on_device,
        mesh=mesh,
        in_specs=placed,
        out_specs=(P(None, "gy", "gx"), P(("gx", "gy"))),
        check_vma=False,
    )
```

```python
import jax
import jax.numpy as jnp
from jax import lax
from jax.experimental import pallas as pl
from jax.experimental.pallas import tpu as pltpu
from jax.sharding import PartitionSpec as P


SWEEPS = 16
TERMINAL = 2
GAMMA = 0.95
PENALTY = 0.5
LANES = 128
SUB = 8
PACK = 2
UNROLL = 2


class Plan:
    def __init__(self, rows, cols, agents, steps, tasks, codes):
        self.rows, self.cols, self.agents = rows, cols, agents
        self.steps, self.tasks, self.codes = steps, tasks, codes
        self.near = steps
        self.wide = steps + SWEEPS
        self.ring = rows + 2 * self.wide
        self.tiles = cols // LANES + 1
        self.lines = cols + 2 * self.wide
        self.span = self.lines // SUB
        self.blocks = LANES // PACK
        self.deep = self.ring // self.blocks
        self.groups = tasks // PACK
        self.planes = self.groups * self.deep
        self.code_bits = (codes - 1).bit_length()
        self.message = rows + 2 * self.near
        self.half = self.message // 2
        self.band = self.wide + self.near
        self.pack = -(-(rows - self.half) // (LANES // self.wide * SUB)) * SUB
        self.across_rows = self.half + self.pack
        self.down_rows = self.tiles * self.band + (self.tiles - 1) * self.wide
        assert cols % LANES == 0 and rows % SUB == 0 and agents % LANES == 0
        assert 4 * self.wide <= LANES and self.near % SUB == 0 and self.wide % SUB == 0
        assert self.half % SUB == 0 and LANES % self.wide == 0 and self.near % 16 == 0
        assert self.band + self.wide + self.band <= LANES
        assert self.ring % self.blocks == 0 and self.lines % SUB == 0
        assert tasks % PACK == 0 and codes <= LANES
        self.magic = -(-(1 << 16) // self.deep)
        assert all((r * self.magic) >> 16 == r // self.deep for r in range(self.ring))


def lane_of(shape):
    return lax.broadcasted_iota(jnp.int32, shape, len(shape) - 1)


def split_cell(cell, cols):
    if cols & (cols - 1) == 0:
        return cell >> (cols.bit_length() - 1), cell & (cols - 1)
    return lax.div(cell, cols), lax.rem(cell, cols)


def one_hot(ids, positions):
    return jnp.where(ids == positions, 1.0, 0.0).astype(jnp.bfloat16)


def counted(row_hot, col_hot):
    return lax.dot_general(
        row_hot[...], col_hot[...], (((1,), (1,)), ((), ())), preferred_element_type=jnp.float32
    )


def right_roll(p, piece):
    return {"second": p.band, "code": LANES - p.wide}.get(piece, None if isinstance(piece, str) else (piece + 1) * p.wide % LANES)


def left_roll(p, piece):
    return {"second": LANES - p.band, "code": p.wide}.get(piece, None if isinstance(piece, str) else piece * p.wide)


def roll(x, amount):
    amount %= LANES
    return x if amount == 0 else pltpu.roll(x, amount, 1)


def bands_kernel(
    plan, act_in, start_in, code_in, task_in, table_in,
    right, left, ring_row, ring_col, code, task, table, act, start, row_hot, col_hot, sems,
):
    p = plan
    pairs = ((act_in, act), (start_in, start), (code_in, code), (task_in, task), (table_in, table))
    copies = [pltpu.make_async_copy(src, dst, sems.at[n]) for n, (src, dst) in enumerate(pairs)]
    for copy in copies:
        copy.start()
    last = p.tiles - 1
    ring_cols = p.tiles * LANES
    row_id = lax.broadcasted_iota(jnp.int32, (p.message, LANES), 0)
    row_id = jnp.where(row_id >= p.rows + p.near, row_id + p.ring - p.message, row_id)
    lines = (
        (0, p.near, last * LANES),
        (LANES - p.wide, p.wide, (last - 1) * LANES + LANES - p.wide),
        (LANES, p.wide, 0),
        (2 * LANES - p.near, p.near, ring_cols - p.near),
    )
    blank = 0
    for at, n, _ in lines + ((2 * LANES, 0, 0),):
        if at > blank:
            col_hot[blank:at, :] = jnp.zeros((at - blank, p.agents), jnp.bfloat16)
        blank = at + n
    copies[0].wait()
    copies[1].wait()
    for i in range(p.agents // LANES):
        here = slice(i * LANES, (i + 1) * LANES)
        a = act[:, here]
        one = lambda c: jnp.where(a == c, 1, 0)
        row, col = split_cell(start[i : i + 1, :], p.cols)
        row = row + jnp.sum(one(2) - one(1), axis=0, keepdims=True)
        col = col + jnp.sum(one(4) - one(3), axis=0, keepdims=True)
        row = jnp.where(row < 0, row + p.ring, row)
        col = jnp.where(col < 0, col + ring_cols, col)
        ring_row[i : i + 1, :] = row
        ring_col[i : i + 1, :] = col
        row_hot[:, here] = one_hot(row_id, row)
        for at, n, first in lines:
            ids = first + lax.broadcasted_iota(jnp.int32, (n, LANES), 0)
            col_hot[at : at + n, here] = one_hot(ids, col)
    counts = counted(row_hot, col_hot)
    for copy in copies[2:]:
        copy.wait()
    lane = lane_of((p.half, LANES))
    for out, side, spare, shift, band in (
        (right, 0, p.near, right_roll, code[:, (last - 1) * LANES :]),
        (left, 1, LANES - p.near - p.band, left_roll, code[:, :LANES]),
    ):
        own = counts[:, side * LANES : (side + 1) * LANES]
        band = band.astype(jnp.float32)
        x = own[: p.half]
        x = jnp.where((lane >= spare) & (lane < spare + p.band), roll(own[p.half :], shift(p, "second")), x)
        lo = LANES - 2 * p.wide if side == 0 else p.wide
        x = jnp.where((lane >= lo) & (lane < lo + p.wide), roll(band[: p.half], shift(p, "code")), x)
        out[pl.ds(0, p.half), :] = x
        packed_lane = lane_of((p.pack, LANES))
        rest = jnp.zeros((p.pack, LANES), jnp.float32)
        for g in range(LANES // p.wide):
            lo = p.half + g * p.pack
            n = min(p.pack, p.rows - lo)
            if n <= 0:
                break
            y = roll(band[lo : lo + n], shift(p, g))
            if n < p.pack:
                y = jnp.concatenate([y, jnp.zeros((p.pack - n, LANES), jnp.float32)], axis=0)
            rest = jnp.where((packed_lane >= g * p.wide) & (packed_lane < (g + 1) * p.wide), y, rest)
        out[pl.ds(p.half, p.pack), :] = rest


def local_kernel(
    plan, ring_row, ring_col, task, table, hist, address, lane_out, looked, row_hot, col_hot
):
    p = plan
    ring_cols = p.tiles * LANES
    row_id = lax.broadcasted_iota(jnp.int32, (p.ring, LANES), 0)
    col_id = lax.broadcasted_iota(jnp.int32, (ring_cols, LANES), 0)
    for i in range(p.agents // LANES):
        here = slice(i * LANES, (i + 1) * LANES)
        row = ring_row[i : i + 1, :]
        col = ring_col[i : i + 1, :]
        row_hot[:, here] = one_hot(row_id, row)
        col_hot[:, here] = one_hot(col_id, col)
        row = jnp.where(row >= p.rows + p.near, row - p.ring, row) + p.wide
        col = jnp.where(col >= p.cols + p.near, col - ring_cols, col) + p.wide
        t = task[i : i + 1, :]
        u = t // PACK
        block = (row * p.magic) >> 16
        lane_out[i : i + 1, :] = (t - u * PACK) * p.blocks + block
        plane = u * p.deep + row - block * p.deep
        address[i : i + 1, :] = plane * p.lines + col
    counts = counted(row_hot, col_hot)
    for t in range(p.tiles):
        hist[t] = counts[:, t * LANES : (t + 1) * LANES]
    looked[...] = jnp.zeros_like(looked)
    looked[pl.ds(0, p.tasks), pl.ds(0, p.codes)] = table[...]


def side_counts(p, message, shift, lo, n):
    parts = []
    for a, b in ((lo, min(lo + n, p.half)), (max(lo, p.half), lo + n)):
        if a < b and a < p.half:
            parts.append(message[pl.ds(a, b - a), :])
        elif a < b:
            parts.append(roll(message[pl.ds(a - p.half, b - a), :], -shift(p, "second")))
    return parts[0] if len(parts) == 1 else jnp.concatenate(parts, axis=0)


def side_codes(p, message, shift, lo, n):
    parts = []
    at = lo
    while at < lo + n:
        if at < p.half:
            end = min(lo + n, p.half)
            parts.append(roll(message[pl.ds(at, end - at), :], -shift(p, "code")))
        else:
            g, r = divmod(at - p.half, p.pack)
            end = min(lo + n, at - r + p.pack)
            parts.append(roll(message[pl.ds(p.half + r, end - at), :], -shift(p, g)))
        at = end
    return parts[0] if len(parts) == 1 else jnp.concatenate(parts, axis=0)


def merged_counts(p, hist, from_left, from_right, row, n):
    last = p.tiles - 1
    lo = row if row < p.rows + p.near else row - p.ring + p.message
    lane = lane_of((n, LANES))
    l = side_counts(p, from_left, right_roll, lo, n)
    r = side_counts(p, from_right, left_roll, lo, n)
    out = []
    for t in range(p.tiles):
        h = hist[t, pl.ds(row, n), :]
        if t == 0:
            h = h + jnp.where(lane < p.near, l, 0.0)
        if t == last - 1:
            h = h + jnp.where(lane >= LANES - p.near, r, 0.0)
        if t == last:
            h = h + jnp.where(lane >= LANES - p.wide, l, jnp.where(lane < p.wide, r, 0.0))
        out.append(h)
    return out


def merged_codes(p, code, from_left, from_right, row, n):
    last = p.tiles - 1
    lane = lane_of((n, LANES))
    out = [code[pl.ds(row, n), pl.ds(t * LANES, LANES)].astype(jnp.float32) for t in range(last)]
    l = side_codes(p, from_left, right_roll, row, n)
    r = side_codes(p, from_right, left_roll, row, n)
    out.append(jnp.where(lane >= LANES - p.wide, l, jnp.where(lane < p.wide, r, 0.0)))
    return out


def across_kernel(plan, hist, code, from_left, from_right, first, second):
    p = plan
    last = p.tiles - 1
    down_cnt = merged_counts(p, hist, from_left, from_right, p.rows - p.wide, p.band)
    up_near = merged_counts(p, hist, from_left, from_right, p.ring - p.near, p.near)
    up_wide = merged_counts(p, hist, from_left, from_right, 0, p.wide)
    down_code = merged_codes(p, code, from_left, from_right, p.rows - p.wide, p.wide)
    up_code = merged_codes(p, code, from_left, from_right, 0, p.wide)
    lane = lane_of((p.wide, LANES))
    inside = (lane >= p.wide) & (lane < LANES - p.wide)
    half = LANES // 2
    odd = lax.axis_index("gy") % 2 == 1

    def put(at, n, down, up):
        first[pl.ds(at, n), :] = jnp.where(odd, up, down)
        second[pl.ds(at, n), :] = jnp.where(odd, down, up)

    for t in range(p.tiles):
        down, up = down_cnt[t], jnp.concatenate([up_near[t], up_wide[t]], axis=0)
        if t < last:
            put(p.tiles * p.band + t * p.wide, p.wide, down_code[t], up_code[t])
        else:
            head = jnp.where(inside, roll(down_code[t], half), down[: p.wide])
            down = jnp.concatenate([head, down[p.wide :]], axis=0)
            tail = jnp.where(inside, roll(up_code[t], half), up[p.near :])
            up = jnp.concatenate([up[: p.near], tail], axis=0)
        put(t * p.band, p.band, down, up)


def look_up(p, looked):
    tables = [jnp.broadcast_to(looked[t : t + 1, :], (SUB, LANES)) for t in range(p.tasks)]

    def put(flat, c, at, code, count):
        crowd = PENALTY * count
        at = pl.ds(at, SUB)
        flat[p.tasks * p.tiles + c, at, :] = jnp.where(code < p.codes - TERMINAL, GAMMA, 0.0)
        for t in range(p.tasks):
            found = jnp.take_along_axis(tables[t], code, axis=1, mode="promise_in_bounds")
            flat[t * p.tiles + c, at, :] = found - crowd

    return put


def rewards_kernel(plan, hist, code, from_left, from_right, looked, flat, near):
    p = plan
    put = look_up(p, looked)
    for row in range(0, p.rows, SUB):
        counts = merged_counts(p, hist, from_left, from_right, row, SUB)
        codes = merged_codes(p, code, from_left, from_right, row, SUB)
        for c in range(p.tiles):
            put(flat, c, row + p.wide, codes[c].astype(jnp.int32), counts[c])
    for at, row in ((0, p.rows), (p.near, p.ring - p.near)):
        counts = merged_counts(p, hist, from_left, from_right, row, p.near)
        for c in range(p.tiles):
            near[c, pl.ds(at, p.near), :] = counts[c]


def sweep_kernel(plan, looked, flat_in, near, first, second, address_in, lane_in, values, answers, flat,
                 turned, reward, gain, value, edge, final, natural, rows_of, address, sems):
    p = plan
    del flat_in
    fetch_address = pltpu.make_async_copy(address_in, address, sems.at[p.tasks * (p.tiles - 1)])
    fetch_address.start()
    last = p.tiles - 1
    odd = lax.axis_index("gy") % 2 == 1
    half = LANES // 2
    w, s = p.wide, p.near

    def above(at, n):
        at = pl.ds(at, n)
        return jnp.where(odd, first[at, :], second[at, :])

    def below(at, n):
        at = pl.ds(at, n)
        return jnp.where(odd, second[at, :], first[at, :])

    put = look_up(p, looked)
    for c in range(p.tiles):
        base = c * p.band
        code_base = p.tiles * p.band + c * w
        for at, extra in ((0, above(base + w, s)), (p.rows - s, below(base, s))):
            at = pl.ds(w + at, s)
            for t in range(p.tasks):
                flat[t * p.tiles + c, at, :] = flat[t * p.tiles + c, at, :] - PENALTY * extra
        for row in range(0, w, SUB):
            count = above(base + row, SUB)
            code = above(code_base + row, SUB) if c < last else roll(count, half)
            if row >= w - s:
                count = count + near[c, pl.ds(s + row - (w - s), SUB), :]
            put(flat, c, row, code.astype(jnp.int32) & (LANES - 1), count)
            count = below(base + s + row, SUB)
            code = below(code_base + row, SUB) if c < last else roll(count, half)
            if row < s:
                count = count + near[c, pl.ds(row, SUB), :]
            put(flat, c, w + p.rows + row, code.astype(jnp.int32) & (LANES - 1), count)

    for u in range(p.groups + 1):
        for i in range(p.deep):
            for c in range(p.tiles):
                parts = []
                for h in range(PACK):
                    t = u * PACK + h if u < p.groups else p.tasks
                    parts.append(flat[t * p.tiles + c, pl.ds(i, p.blocks, stride=p.deep), :])
                x = jnp.transpose(jnp.concatenate(parts, axis=0))
                if c < last:
                    turned[u * p.deep + i, pl.ds(w + c * LANES, LANES), :] = x
                else:
                    turned[u * p.deep + i, pl.ds(w + p.cols, w), :] = x[:w]
                    turned[u * p.deep + i, pl.ds(0, w), :] = x[LANES - w :]

    for q in range(p.span):
        for n in range(p.planes + p.deep):
            x = turned[n, pl.ds(q, SUB, stride=p.span), :]
            if n < p.planes:
                at = pl.ds((q * p.planes + n) * SUB, SUB)
                reward[at, :] = x
            else:
                gain[pl.ds((q * p.deep + n - p.planes) * SUB, SUB), :] = x

    def sweep(held, put):
        load = lambda q: [held[pl.ds((q * p.planes + n) * SUB, SUB), :] for n in range(p.planes)]
        now = load(0)
        before = [pltpu.roll(x, 1, 0) for x in load(p.span - 1)]
        for n in range(p.planes):
            edge[pl.ds(n * SUB, SUB), :] = pltpu.roll(now[n], SUB - 1, 0)
        for q in range(p.span):
            if q + 1 < p.span:
                after = load(q + 1)
            else:
                after = [edge[pl.ds(n * SUB, SUB), :] for n in range(p.planes)]
            for i in range(p.deep):
                g = gain[pl.ds((q * p.deep + i) * SUB, SUB), :]
                for u in range(p.groups):
                    n = u * p.deep + i
                    up = now[n - 1] if i > 0 else pltpu.roll(now[n + p.deep - 1], 1, 1)
                    down = now[n + 1] if i + 1 < p.deep else pltpu.roll(now[n + 1 - p.deep], LANES - 1, 1)
                    best = jnp.maximum(jnp.maximum(up, down), jnp.maximum(before[n], after[n]))
                    put(q, n, reward[pl.ds((q * p.planes + n) * SUB, SUB), :] + g * best)
            before, now = now, after

    def put_value(q, n, x):
        value[pl.ds((q * p.planes + n) * SUB, SUB), :] = x

    def put_final(q, n, x):
        final[pl.ds(n * p.lines + q, SUB, stride=p.span), :] = x

    def sweeps(_, carry):
        for _ in range(UNROLL):
            sweep(value, put_value)
        return carry

    assert (SWEEPS - 2) % UNROLL == 0
    sweep(reward, put_value)
    lax.fori_loop(0, (SWEEPS - 2) // UNROLL, sweeps, 0)
    sweep(value, put_final)
    fetch_address.wait()

    copies = []
    for u in range(p.groups):
        for c in range(last):
            for i in range(p.deep):
                lines = pl.ds((u * p.deep + i) * p.lines + w + c * LANES, LANES)
                x = jnp.transpose(final[lines, :])
                for h in range(PACK):
                    at = pl.ds(i, p.blocks, stride=p.deep)
                    natural[(u * PACK + h) * last + c, at, :] = x[h * p.blocks : (h + 1) * p.blocks]
            for h in range(PACK):
                t = u * PACK + h
                copy = pltpu.make_async_copy(
                    natural.at[t * last + c, pl.ds(w, p.rows), :],
                    values.at[t, :, pl.ds(c * LANES, LANES)],
                    sems.at[t * last + c],
                )
                copy.start()
                copies.append(copy)

    def fetch(i, carry):
        for l in range(LANES):
            rows_of[pl.ds(i * LANES + l, 1), :] = final[pl.ds(address[i, l], 1), :]
        return carry

    lax.fori_loop(0, p.agents // LANES, fetch, 0)
    lane_id = lax.broadcasted_iota(jnp.int32, (LANES, LANES), 0)
    for i in range(p.agents // LANES):
        x = jnp.transpose(rows_of[pl.ds(i * LANES, LANES), :])
        picked = jnp.where(lane_id == lane_in[i : i + 1, :], x, 0.0)
        answers[i : i + 1, :] = jnp.sum(picked, axis=0, keepdims=True)
    for copy in copies:
        copy.wait()


def shift(value, axis, steps):
    count = lax.axis_size(axis)
    return lax.ppermute(value, axis, [(i, (i + steps) % count) for i in range(count)])


def swap(value, axis, parity):
    count = lax.axis_size(axis)
    assert count % 2 == 0
    return lax.ppermute(
        value, axis, [(i, (i + (1 if i % 2 == parity else -1)) % count) for i in range(count)]
    )


def on_device(map_codes, reward_table, start_cell, agent_task, actions):
    rows, cols = map_codes.shape
    tasks, codes = reward_table.shape
    steps, agents = actions.shape
    p = Plan(rows, cols, agents, steps, tasks, codes)
    vmem = pl.BlockSpec(memory_space=pltpu.VMEM)
    smem = pl.BlockSpec(memory_space=pltpu.SMEM)
    f32, i32 = jnp.float32, jnp.int32
    shape = jax.ShapeDtypeStruct
    fast = lambda dims, dtype: pltpu.VMEM(dims, dtype)
    far = lambda x: pltpu.with_memory_space_constraint(x, pltpu.HBM)
    near = lambda x: pltpu.with_memory_space_constraint(x, pltpu.VMEM)
    by_lane = (agents // LANES, LANES)

    def bind(kernel):
        def body(*refs):
            kernel(p, *refs)

        return body

    to_right, to_left, ring_row, ring_col, kept, task, table = pl.pallas_call(
        bind(bands_kernel),
        in_specs=[pl.BlockSpec(memory_space=pl.ANY)] * 5,
        out_specs=[vmem] * 7,
        out_shape=[
            fast((p.across_rows, LANES), f32),
            fast((p.across_rows, LANES), f32),
            fast(by_lane, i32),
            fast(by_lane, i32),
            fast((rows, cols), i32),
            fast(by_lane, i32),
            fast((tasks, codes), f32),
        ],
        scratch_shapes=[
            pltpu.VMEM((steps, agents), i32),
            pltpu.VMEM(by_lane, i32),
            pltpu.VMEM((p.message, agents), jnp.bfloat16),
            pltpu.VMEM((2 * LANES, agents), jnp.bfloat16),
            pltpu.SemaphoreType.DMA((5,)),
        ],
        compiler_params=pltpu.CompilerParams(vmem_limit_bytes=12 << 20),
        name="bands",
    )(*map(far, (actions, start_cell.reshape(by_lane), map_codes, agent_task.reshape(by_lane), reward_table)))
    from_left = shift(to_right, "gx", 1)
    from_right = shift(to_left, "gx", -1)
    hist, address, lane, looked = pl.pallas_call(
        bind(local_kernel),
        in_specs=[vmem] * 4,
        out_specs=[vmem] * 4,
        out_shape=[
            fast((p.tiles, p.ring, LANES), f32),
            fast(by_lane, i32),
            fast(by_lane, i32),
            fast((SUB, LANES), f32),
        ],
        scratch_shapes=[
            pltpu.VMEM((p.ring, agents), jnp.bfloat16),
            pltpu.VMEM((p.tiles * LANES, agents), jnp.bfloat16),
        ],
        compiler_params=pltpu.CompilerParams(vmem_limit_bytes=12 << 20),
        name="local",
    )(near(ring_row), near(ring_col), near(task), near(table))
    sides = (near(hist), near(kept), near(from_left), near(from_right))
    first, second = pl.pallas_call(
        bind(across_kernel),
        in_specs=[vmem] * 4,
        out_specs=[vmem] * 2,
        out_shape=[fast((p.down_rows, LANES), f32), fast((p.down_rows, LANES), f32)],
        compiler_params=pltpu.CompilerParams(vmem_limit_bytes=8 << 20),
        name="across",
    )(*sides)
    first = swap(first, "gy", 0)
    second = swap(second, "gy", 1)
    flats = ((tasks + 1) * p.tiles, p.ring, LANES)
    flat, edges = pl.pallas_call(
        bind(rewards_kernel),
        in_specs=[vmem] * 5,
        out_specs=[vmem] * 2,
        out_shape=[fast(flats, f32), fast((p.tiles, 2 * p.near, LANES), f32)],
        compiler_params=pltpu.CompilerParams(vmem_limit_bytes=12 << 20),
        name="rewards",
    )(*sides, near(looked))
    outs = tasks * (p.tiles - 1)
    values, answers, _ = pl.pallas_call(
        bind(sweep_kernel),
        in_specs=[vmem] * 7,
        out_specs=[pl.BlockSpec(memory_space=pl.ANY), vmem, vmem],
        out_shape=[shape((tasks, rows, cols), f32), shape(by_lane, f32), fast(flats, f32)],
        scratch_shapes=[
            pltpu.VMEM((p.planes + p.deep, p.lines, LANES), f32),
            pltpu.VMEM((p.planes * p.lines, LANES), f32),
            pltpu.VMEM((p.deep * p.lines, LANES), f32),
            pltpu.VMEM((p.planes * p.lines, LANES), f32),
            pltpu.VMEM((p.planes * SUB, LANES), f32),
            pltpu.VMEM((p.planes * p.lines, LANES), f32),
            pltpu.VMEM((outs, p.ring, LANES), f32),
            pltpu.VMEM((agents, LANES), f32),
            pltpu.SMEM(by_lane, i32),
            pltpu.SemaphoreType.DMA((outs + 1,)),
        ],
        input_output_aliases={1: 2},
        compiler_params=pltpu.CompilerParams(vmem_limit_bytes=24 << 20),
        name="sweep",
    )(near(looked), near(flat), near(edges), near(first), near(second), near(address), near(lane))
    return values, answers.reshape(agents)


def solution(mesh):
    placed = (P("gy", "gx"), P(), P(("gx", "gy")), P(("gx", "gy")), P(None, ("gx", "gy")))
    return jax.shard_map(
        on_device,
        mesh=mesh,
        in_specs=placed,
        out_specs=(P(None, "gy", "gx"), P(("gx", "gy"))),
        check_vma=False,
    )
```

```python
import jax
import jax.numpy as jnp
from jax import lax
from jax.experimental import pallas as pl
from jax.experimental.pallas import tpu as pltpu
from jax.sharding import PartitionSpec as P


SWEEPS = 16
TERMINAL = 2
GAMMA = 0.95
PENALTY = 0.5
LANES = 128
SUB = 8
PACK = 2
UNROLL = 2
TAIL = 12


class Plan:
    def __init__(self, rows, cols, agents, steps, tasks, codes):
        self.rows, self.cols, self.agents = rows, cols, agents
        self.steps, self.tasks, self.codes = steps, tasks, codes
        self.near = steps
        self.wide = steps + SWEEPS
        self.ring = rows + 2 * self.wide
        self.tiles = cols // LANES + 1
        self.lines = cols + 2 * self.wide
        self.span = self.lines // SUB
        self.blocks = LANES // PACK
        self.deep = self.ring // self.blocks
        self.groups = tasks // PACK
        self.planes = self.groups * self.deep
        self.code_bits = (codes - 1).bit_length()
        self.message = rows + 2 * self.near
        self.half = self.message // 2
        self.band = self.wide + self.near
        self.pack = -(-(rows - self.half) // (LANES // self.wide * SUB)) * SUB
        self.across_rows = self.half + self.pack
        self.down_rows = self.tiles * self.band + (self.tiles - 1) * self.wide
        assert cols % LANES == 0 and rows % SUB == 0 and agents % LANES == 0
        assert 4 * self.wide <= LANES and self.near % SUB == 0 and self.wide % SUB == 0
        assert self.half % SUB == 0 and LANES % self.wide == 0 and self.near % 16 == 0
        assert self.band + self.wide + self.band <= LANES
        assert self.ring % self.blocks == 0 and self.lines % SUB == 0
        assert tasks % PACK == 0 and codes <= LANES
        self.magic = -(-(1 << 16) // self.deep)
        assert all((r * self.magic) >> 16 == r // self.deep for r in range(self.ring))


def lane_of(shape):
    return lax.broadcasted_iota(jnp.int32, shape, len(shape) - 1)


def split_cell(cell, cols):
    if cols & (cols - 1) == 0:
        return cell >> (cols.bit_length() - 1), cell & (cols - 1)
    return lax.div(cell, cols), lax.rem(cell, cols)


def one_hot(ids, positions):
    return jnp.where(ids == positions, 1.0, 0.0).astype(jnp.bfloat16)


def counted(row_hot, col_hot):
    return lax.dot_general(
        row_hot[...], col_hot[...], (((1,), (1,)), ((), ())), preferred_element_type=jnp.float32
    )


def right_roll(p, piece):
    return {"second": p.band, "code": LANES - p.wide}.get(piece, None if isinstance(piece, str) else (piece + 1) * p.wide % LANES)


def left_roll(p, piece):
    return {"second": LANES - p.band, "code": p.wide}.get(piece, None if isinstance(piece, str) else piece * p.wide)


def roll(x, amount):
    amount %= LANES
    return x if amount == 0 else pltpu.roll(x, amount, 1)


def bands_kernel(
    plan, act_in, start_in, code_in, task_in, table_in,
    right, left, ring_row, ring_col, code, task, table, act, start, row_hot, col_hot, sems,
):
    p = plan
    pairs = ((act_in, act), (start_in, start), (code_in, code), (task_in, task), (table_in, table))
    copies = [pltpu.make_async_copy(src, dst, sems.at[n]) for n, (src, dst) in enumerate(pairs)]
    for copy in copies:
        copy.start()
    last = p.tiles - 1
    ring_cols = p.tiles * LANES
    row_id = lax.broadcasted_iota(jnp.int32, (p.message, LANES), 0)
    row_id = jnp.where(row_id >= p.rows + p.near, row_id + p.ring - p.message, row_id)
    lines = (
        (0, p.near, last * LANES),
        (LANES - p.wide, p.wide, (last - 1) * LANES + LANES - p.wide),
        (LANES, p.wide, 0),
        (2 * LANES - p.near, p.near, ring_cols - p.near),
    )
    blank = 0
    for at, n, _ in lines + ((2 * LANES, 0, 0),):
        if at > blank:
            col_hot[blank:at, :] = jnp.zeros((at - blank, p.agents), jnp.bfloat16)
        blank = at + n
    copies[0].wait()
    copies[1].wait()
    for i in range(p.agents // LANES):
        here = slice(i * LANES, (i + 1) * LANES)
        a = act[:, here]
        one = lambda c: jnp.where(a == c, 1, 0)
        row, col = split_cell(start[i : i + 1, :], p.cols)
        row = row + jnp.sum(one(2) - one(1), axis=0, keepdims=True)
        col = col + jnp.sum(one(4) - one(3), axis=0, keepdims=True)
        row = jnp.where(row < 0, row + p.ring, row)
        col = jnp.where(col < 0, col + ring_cols, col)
        ring_row[i : i + 1, :] = row
        ring_col[i : i + 1, :] = col
        row_hot[:, here] = one_hot(row_id, row)
        for at, n, first in lines:
            ids = first + lax.broadcasted_iota(jnp.int32, (n, LANES), 0)
            col_hot[at : at + n, here] = one_hot(ids, col)
    counts = counted(row_hot, col_hot)
    for copy in copies[2:]:
        copy.wait()
    lane = lane_of((p.half, LANES))
    for out, side, spare, shift, band in (
        (right, 0, p.near, right_roll, code[:, (last - 1) * LANES :]),
        (left, 1, LANES - p.near - p.band, left_roll, code[:, :LANES]),
    ):
        own = counts[:, side * LANES : (side + 1) * LANES]
        band = band.astype(jnp.float32)
        x = own[: p.half]
        x = jnp.where((lane >= spare) & (lane < spare + p.band), roll(own[p.half :], shift(p, "second")), x)
        lo = LANES - 2 * p.wide if side == 0 else p.wide
        x = jnp.where((lane >= lo) & (lane < lo + p.wide), roll(band[: p.half], shift(p, "code")), x)
        out[pl.ds(0, p.half), :] = x
        packed_lane = lane_of((p.pack, LANES))
        rest = jnp.zeros((p.pack, LANES), jnp.float32)
        for g in range(LANES // p.wide):
            lo = p.half + g * p.pack
            n = min(p.pack, p.rows - lo)
            if n <= 0:
                break
            y = roll(band[lo : lo + n], shift(p, g))
            if n < p.pack:
                y = jnp.concatenate([y, jnp.zeros((p.pack - n, LANES), jnp.float32)], axis=0)
            rest = jnp.where((packed_lane >= g * p.wide) & (packed_lane < (g + 1) * p.wide), y, rest)
        out[pl.ds(p.half, p.pack), :] = rest


def local_kernel(
    plan, ring_row, ring_col, task, table, hist, address, lane_out, looked, row_hot, col_hot
):
    p = plan
    ring_cols = p.tiles * LANES
    row_id = lax.broadcasted_iota(jnp.int32, (p.ring, LANES), 0)
    col_id = lax.broadcasted_iota(jnp.int32, (ring_cols, LANES), 0)
    for i in range(p.agents // LANES):
        here = slice(i * LANES, (i + 1) * LANES)
        row = ring_row[i : i + 1, :]
        col = ring_col[i : i + 1, :]
        row_hot[:, here] = one_hot(row_id, row)
        col_hot[:, here] = one_hot(col_id, col)
        row = jnp.where(row >= p.rows + p.near, row - p.ring, row) + p.wide
        col = jnp.where(col >= p.cols + p.near, col - ring_cols, col) + p.wide
        t = task[i : i + 1, :]
        u = t // PACK
        block = (row * p.magic) >> 16
        lane_out[i : i + 1, :] = (t - u * PACK) * p.blocks + block
        plane = u * p.deep + row - block * p.deep
        address[i : i + 1, :] = plane * p.lines + col
    counts = counted(row_hot, col_hot)
    for t in range(p.tiles):
        hist[t] = counts[:, t * LANES : (t + 1) * LANES]
    looked[...] = jnp.zeros_like(looked)
    looked[pl.ds(0, p.tasks), pl.ds(0, p.codes)] = table[...]


def side_counts(p, message, shift, lo, n):
    parts = []
    for a, b in ((lo, min(lo + n, p.half)), (max(lo, p.half), lo + n)):
        if a < b and a < p.half:
            parts.append(message[pl.ds(a, b - a), :])
        elif a < b:
            parts.append(roll(message[pl.ds(a - p.half, b - a), :], -shift(p, "second")))
    return parts[0] if len(parts) == 1 else jnp.concatenate(parts, axis=0)


def side_codes(p, message, shift, lo, n):
    parts = []
    at = lo
    while at < lo + n:
        if at < p.half:
            end = min(lo + n, p.half)
            parts.append(roll(message[pl.ds(at, end - at), :], -shift(p, "code")))
        else:
            g, r = divmod(at - p.half, p.pack)
            end = min(lo + n, at - r + p.pack)
            parts.append(roll(message[pl.ds(p.half + r, end - at), :], -shift(p, g)))
        at = end
    return parts[0] if len(parts) == 1 else jnp.concatenate(parts, axis=0)


def merged_counts(p, hist, from_left, from_right, row, n):
    last = p.tiles - 1
    lo = row if row < p.rows + p.near else row - p.ring + p.message
    lane = lane_of((n, LANES))
    l = side_counts(p, from_left, right_roll, lo, n)
    r = side_counts(p, from_right, left_roll, lo, n)
    out = []
    for t in range(p.tiles):
        h = hist[t, pl.ds(row, n), :]
        if t == 0:
            h = h + jnp.where(lane < p.near, l, 0.0)
        if t == last - 1:
            h = h + jnp.where(lane >= LANES - p.near, r, 0.0)
        if t == last:
            h = h + jnp.where(lane >= LANES - p.wide, l, jnp.where(lane < p.wide, r, 0.0))
        out.append(h)
    return out


def merged_codes(p, code, from_left, from_right, row, n):
    last = p.tiles - 1
    lane = lane_of((n, LANES))
    out = [code[pl.ds(row, n), pl.ds(t * LANES, LANES)].astype(jnp.float32) for t in range(last)]
    l = side_codes(p, from_left, right_roll, row, n)
    r = side_codes(p, from_right, left_roll, row, n)
    out.append(jnp.where(lane >= LANES - p.wide, l, jnp.where(lane < p.wide, r, 0.0)))
    return out


def across_kernel(plan, hist, code, from_left, from_right, first, second):
    p = plan
    last = p.tiles - 1
    down_cnt = merged_counts(p, hist, from_left, from_right, p.rows - p.wide, p.band)
    up_near = merged_counts(p, hist, from_left, from_right, p.ring - p.near, p.near)
    up_wide = merged_counts(p, hist, from_left, from_right, 0, p.wide)
    down_code = merged_codes(p, code, from_left, from_right, p.rows - p.wide, p.wide)
    up_code = merged_codes(p, code, from_left, from_right, 0, p.wide)
    lane = lane_of((p.wide, LANES))
    inside = (lane >= p.wide) & (lane < LANES - p.wide)
    half = LANES // 2
    odd = lax.axis_index("gy") % 2 == 1

    def put(at, n, down, up):
        first[pl.ds(at, n), :] = jnp.where(odd, up, down)
        second[pl.ds(at, n), :] = jnp.where(odd, down, up)

    for t in range(p.tiles):
        down, up = down_cnt[t], jnp.concatenate([up_near[t], up_wide[t]], axis=0)
        if t < last:
            put(p.tiles * p.band + t * p.wide, p.wide, down_code[t], up_code[t])
        else:
            head = jnp.where(inside, roll(down_code[t], half), down[: p.wide])
            down = jnp.concatenate([head, down[p.wide :]], axis=0)
            tail = jnp.where(inside, roll(up_code[t], half), up[p.near :])
            up = jnp.concatenate([up[: p.near], tail], axis=0)
        put(t * p.band, p.band, down, up)


def look_up(p, looked):
    tables = [jnp.broadcast_to(looked[t : t + 1, :], (SUB, LANES)) for t in range(p.tasks)]

    def put(flat, c, at, code, count):
        crowd = PENALTY * count
        at = pl.ds(at, SUB)
        flat[p.tasks * p.tiles + c, at, :] = jnp.where(code < p.codes - TERMINAL, GAMMA, 0.0)
        for t in range(p.tasks):
            found = jnp.take_along_axis(tables[t], code, axis=1, mode="promise_in_bounds")
            flat[t * p.tiles + c, at, :] = found - crowd

    return put


def rewards_kernel(plan, hist, code, from_left, from_right, looked, flat, near):
    p = plan
    put = look_up(p, looked)
    for row in range(0, p.rows, SUB):
        counts = merged_counts(p, hist, from_left, from_right, row, SUB)
        codes = merged_codes(p, code, from_left, from_right, row, SUB)
        for c in range(p.tiles):
            put(flat, c, row + p.wide, codes[c].astype(jnp.int32), counts[c])
    for at, row in ((0, p.rows), (p.near, p.ring - p.near)):
        counts = merged_counts(p, hist, from_left, from_right, row, p.near)
        for c in range(p.tiles):
            near[c, pl.ds(at, p.near), :] = counts[c]


def sweep_kernel(plan, looked, flat_in, near, first, second, address_in, lane_in, values, answers, flat,
                 turned, reward, gain, value, edge, spin, raw, final, natural, rows_of, address, sems):
    p = plan
    del flat_in
    fetch_address = pltpu.make_async_copy(address_in, address, sems.at[p.tasks * (p.tiles - 1)])
    fetch_address.start()
    last = p.tiles - 1
    odd = lax.axis_index("gy") % 2 == 1
    half = LANES // 2
    w, s = p.wide, p.near

    def above(at, n):
        at = pl.ds(at, n)
        return jnp.where(odd, first[at, :], second[at, :])

    def below(at, n):
        at = pl.ds(at, n)
        return jnp.where(odd, second[at, :], first[at, :])

    put = look_up(p, looked)
    for c in range(p.tiles):
        base = c * p.band
        code_base = p.tiles * p.band + c * w
        for at, extra in ((0, above(base + w, s)), (p.rows - s, below(base, s))):
            at = pl.ds(w + at, s)
            for t in range(p.tasks):
                flat[t * p.tiles + c, at, :] = flat[t * p.tiles + c, at, :] - PENALTY * extra
        for row in range(0, w, SUB):
            count = above(base + row, SUB)
            code = above(code_base + row, SUB) if c < last else roll(count, half)
            if row >= w - s:
                count = count + near[c, pl.ds(s + row - (w - s), SUB), :]
            put(flat, c, row, code.astype(jnp.int32) & (LANES - 1), count)
            count = below(base + s + row, SUB)
            code = below(code_base + row, SUB) if c < last else roll(count, half)
            if row < s:
                count = count + near[c, pl.ds(row, SUB), :]
            put(flat, c, w + p.rows + row, code.astype(jnp.int32) & (LANES - 1), count)

    for u in range(p.groups + 1):
        for i in range(p.deep):
            for c in range(p.tiles):
                parts = []
                for h in range(PACK):
                    t = u * PACK + h if u < p.groups else p.tasks
                    parts.append(flat[t * p.tiles + c, pl.ds(i, p.blocks, stride=p.deep), :])
                x = jnp.transpose(jnp.concatenate(parts, axis=0))
                if c < last:
                    turned[u * p.deep + i, pl.ds(w + c * LANES, LANES), :] = x
                else:
                    turned[u * p.deep + i, pl.ds(w + p.cols, w), :] = x[:w]
                    turned[u * p.deep + i, pl.ds(0, w), :] = x[LANES - w :]

    early = p.span - TAIL
    ends = [(u, up) for u in range(p.groups) for up in (True, False)]

    def end_of(line, u, up):
        return line[u * p.deep + (p.deep - 1 if up else 0)]

    def turn(x, up):
        return pltpu.roll(x, 1 if up else LANES - 1, 1)

    def spot(q, e):
        return pl.ds((q * len(ends) + e) * SUB, SUB)

    def put_ends(q, line):
        for e, (u, up) in enumerate(ends):
            x = end_of(line, u, up)
            if q < early:
                spin[spot(q, e), :] = turn(x, up)
            else:
                raw[spot(q - early, e), :] = x

    for q in range(p.span):
        line = []
        for n in range(p.planes + p.deep):
            x = turned[n, pl.ds(q, SUB, stride=p.span), :]
            if n < p.planes:
                reward[pl.ds((q * p.planes + n) * SUB, SUB), :] = x
                line.append(x)
            else:
                gain[pl.ds((q * p.deep + n - p.planes) * SUB, SUB), :] = x
        put_ends(q, line)

    def sweep(held, put, more=True):
        load = lambda q: [held[pl.ds((q * p.planes + n) * SUB, SUB), :] for n in range(p.planes)]
        for q in range(early, p.span):
            for e, (u, up) in enumerate(ends):
                spin[spot(q, e), :] = turn(raw[spot(q - early, e), :], up)
        now = load(0)
        before = [pltpu.roll(x, 1, 0) for x in load(p.span - 1)]
        for n in range(p.planes):
            edge[pl.ds(n * SUB, SUB), :] = pltpu.roll(now[n], SUB - 1, 0)
        passed = [
            jnp.maximum(before[n - 1], now[n]) if n % p.deep else None for n in range(p.planes)
        ]
        for q in range(p.span):
            if q + 1 < p.span:
                after = load(q + 1)
            else:
                after = [edge[pl.ds(n * SUB, SUB), :] for n in range(p.planes)]
            corner = [None] * p.planes
            made = [None] * p.planes
            for n in range(p.planes):
                above_cell = now[n - 1] if n % p.deep else spin[spot(q, 2 * (n // p.deep)), :]
                corner[n] = jnp.maximum(above_cell, after[n])
            for i in range(p.deep):
                g = gain[pl.ds((q * p.deep + i) * SUB, SUB), :]
                for u in range(p.groups):
                    n = u * p.deep + i
                    if i + 1 < p.deep:
                        other = passed[n + 1]
                    else:
                        other = jnp.maximum(before[n], spin[spot(q, 2 * u + 1), :])
                    best = jnp.maximum(corner[n], other)
                    made[n] = reward[pl.ds((q * p.planes + n) * SUB, SUB), :] + g * best
                    put(q, n, made[n])
            if more:
                put_ends(q, made)
            before, now, passed = now, after, corner

    def put_value(q, n, x):
        value[pl.ds((q * p.planes + n) * SUB, SUB), :] = x

    def put_final(q, n, x):
        final[pl.ds(n * p.lines + q, SUB, stride=p.span), :] = x

    def sweeps(_, carry):
        for _ in range(UNROLL):
            sweep(value, put_value)
        return carry

    assert (SWEEPS - 2) % UNROLL == 0
    sweep(reward, put_value)
    lax.fori_loop(0, (SWEEPS - 2) // UNROLL, sweeps, 0)
    sweep(value, put_final, more=False)
    fetch_address.wait()

    copies = []
    for u in range(p.groups):
        for c in range(last):
            for i in range(p.deep):
                lines = pl.ds((u * p.deep + i) * p.lines + w + c * LANES, LANES)
                x = jnp.transpose(final[lines, :])
                for h in range(PACK):
                    at = pl.ds(i, p.blocks, stride=p.deep)
                    natural[(u * PACK + h) * last + c, at, :] = x[h * p.blocks : (h + 1) * p.blocks]
            for h in range(PACK):
                t = u * PACK + h
                copy = pltpu.make_async_copy(
                    natural.at[t * last + c, pl.ds(w, p.rows), :],
                    values.at[t, :, pl.ds(c * LANES, LANES)],
                    sems.at[t * last + c],
                )
                copy.start()
                copies.append(copy)

    def fetch(i, carry):
        for l in range(LANES):
            rows_of[pl.ds(i * LANES + l, 1), :] = final[pl.ds(address[i, l], 1), :]
        return carry

    lax.fori_loop(0, p.agents // LANES, fetch, 0)
    lane_id = lax.broadcasted_iota(jnp.int32, (LANES, LANES), 0)
    for i in range(p.agents // LANES):
        x = jnp.transpose(rows_of[pl.ds(i * LANES, LANES), :])
        picked = jnp.where(lane_id == lane_in[i : i + 1, :], x, 0.0)
        answers[i : i + 1, :] = jnp.sum(picked, axis=0, keepdims=True)
    for copy in copies:
        copy.wait()


def shift(value, axis, steps):
    count = lax.axis_size(axis)
    return lax.ppermute(value, axis, [(i, (i + steps) % count) for i in range(count)])


def swap(value, axis, parity):
    count = lax.axis_size(axis)
    assert count % 2 == 0
    return lax.ppermute(
        value, axis, [(i, (i + (1 if i % 2 == parity else -1)) % count) for i in range(count)]
    )


def on_device(map_codes, reward_table, start_cell, agent_task, actions):
    rows, cols = map_codes.shape
    tasks, codes = reward_table.shape
    steps, agents = actions.shape
    p = Plan(rows, cols, agents, steps, tasks, codes)
    vmem = pl.BlockSpec(memory_space=pltpu.VMEM)
    smem = pl.BlockSpec(memory_space=pltpu.SMEM)
    f32, i32 = jnp.float32, jnp.int32
    shape = jax.ShapeDtypeStruct
    fast = lambda dims, dtype: pltpu.VMEM(dims, dtype)
    far = lambda x: pltpu.with_memory_space_constraint(x, pltpu.HBM)
    near = lambda x: pltpu.with_memory_space_constraint(x, pltpu.VMEM)
    by_lane = (agents // LANES, LANES)

    def bind(kernel):
        def body(*refs):
            kernel(p, *refs)

        return body

    to_right, to_left, ring_row, ring_col, kept, task, table = pl.pallas_call(
        bind(bands_kernel),
        in_specs=[pl.BlockSpec(memory_space=pl.ANY)] * 5,
        out_specs=[vmem] * 7,
        out_shape=[
            fast((p.across_rows, LANES), f32),
            fast((p.across_rows, LANES), f32),
            fast(by_lane, i32),
            fast(by_lane, i32),
            fast((rows, cols), i32),
            fast(by_lane, i32),
            fast((tasks, codes), f32),
        ],
        scratch_shapes=[
            pltpu.VMEM((steps, agents), i32),
            pltpu.VMEM(by_lane, i32),
            pltpu.VMEM((p.message, agents), jnp.bfloat16),
            pltpu.VMEM((2 * LANES, agents), jnp.bfloat16),
            pltpu.SemaphoreType.DMA((5,)),
        ],
        compiler_params=pltpu.CompilerParams(vmem_limit_bytes=12 << 20),
        name="bands",
    )(*map(far, (actions, start_cell.reshape(by_lane), map_codes, agent_task.reshape(by_lane), reward_table)))
    from_left = shift(to_right, "gx", 1)
    from_right = shift(to_left, "gx", -1)
    hist, address, lane, looked = pl.pallas_call(
        bind(local_kernel),
        in_specs=[vmem] * 4,
        out_specs=[vmem] * 4,
        out_shape=[
            fast((p.tiles, p.ring, LANES), f32),
            fast(by_lane, i32),
            fast(by_lane, i32),
            fast((SUB, LANES), f32),
        ],
        scratch_shapes=[
            pltpu.VMEM((p.ring, agents), jnp.bfloat16),
            pltpu.VMEM((p.tiles * LANES, agents), jnp.bfloat16),
        ],
        compiler_params=pltpu.CompilerParams(vmem_limit_bytes=12 << 20),
        name="local",
    )(near(ring_row), near(ring_col), near(task), near(table))
    sides = (near(hist), near(kept), near(from_left), near(from_right))
    first, second = pl.pallas_call(
        bind(across_kernel),
        in_specs=[vmem] * 4,
        out_specs=[vmem] * 2,
        out_shape=[fast((p.down_rows, LANES), f32), fast((p.down_rows, LANES), f32)],
        compiler_params=pltpu.CompilerParams(vmem_limit_bytes=8 << 20),
        name="across",
    )(*sides)
    first = swap(first, "gy", 0)
    second = swap(second, "gy", 1)
    flats = ((tasks + 1) * p.tiles, p.ring, LANES)
    flat, edges = pl.pallas_call(
        bind(rewards_kernel),
        in_specs=[vmem] * 5,
        out_specs=[vmem] * 2,
        out_shape=[fast(flats, f32), fast((p.tiles, 2 * p.near, LANES), f32)],
        compiler_params=pltpu.CompilerParams(vmem_limit_bytes=12 << 20),
        name="rewards",
    )(*sides, near(looked))
    outs = tasks * (p.tiles - 1)
    values, answers, _ = pl.pallas_call(
        bind(sweep_kernel),
        in_specs=[vmem] * 7,
        out_specs=[pl.BlockSpec(memory_space=pl.ANY), vmem, vmem],
        out_shape=[shape((tasks, rows, cols), f32), shape(by_lane, f32), fast(flats, f32)],
        scratch_shapes=[
            pltpu.VMEM((p.planes + p.deep, p.lines, LANES), f32),
            pltpu.VMEM((p.planes * p.lines, LANES), f32),
            pltpu.VMEM((p.deep * p.lines, LANES), f32),
            pltpu.VMEM((p.planes * p.lines, LANES), f32),
            pltpu.VMEM((p.planes * SUB, LANES), f32),
            pltpu.VMEM((2 * p.groups * p.span * SUB, LANES), f32),
            pltpu.VMEM((2 * p.groups * TAIL * SUB, LANES), f32),
            pltpu.VMEM((p.planes * p.lines, LANES), f32),
            pltpu.VMEM((outs, p.ring, LANES), f32),
            pltpu.VMEM((agents, LANES), f32),
            pltpu.SMEM(by_lane, i32),
            pltpu.SemaphoreType.DMA((outs + 1,)),
        ],
        input_output_aliases={1: 2},
        compiler_params=pltpu.CompilerParams(vmem_limit_bytes=24 << 20),
        name="sweep",
    )(near(looked), near(flat), near(edges), near(first), near(second), near(address), near(lane))
    return values, answers.reshape(agents)


def solution(mesh):
    placed = (P("gy", "gx"), P(), P(("gx", "gy")), P(("gx", "gy")), P(None, ("gx", "gy")))
    return jax.shard_map(
        on_device,
        mesh=mesh,
        in_specs=placed,
        out_specs=(P(None, "gy", "gx"), P(("gx", "gy"))),
        check_vma=False,
    )
```

```python
import jax
import jax.numpy as jnp
from jax import lax
from jax.experimental import pallas as pl
from jax.experimental.pallas import tpu as pltpu
from jax.sharding import PartitionSpec as P


SWEEPS = 16
TERMINAL = 2
GAMMA = 0.95
PENALTY = 0.5
LANES = 128
SUB = 8
PACK = 2
UNROLL = 2
TAIL = 12


class Plan:
    def __init__(self, rows, cols, agents, steps, tasks, codes):
        self.rows, self.cols, self.agents = rows, cols, agents
        self.steps, self.tasks, self.codes = steps, tasks, codes
        self.near = steps
        self.wide = steps + SWEEPS
        self.ring = rows + 2 * self.wide
        self.tiles = cols // LANES + 1
        self.lines = cols + 2 * self.wide
        self.span = self.lines // SUB
        self.blocks = LANES // PACK
        self.deep = self.ring // self.blocks
        self.groups = tasks // PACK
        self.planes = self.groups * self.deep
        self.code_bits = max(3, (codes - 1).bit_length())
        self.shelf = 1 << self.code_bits
        self.message = rows + 2 * self.near
        self.half = self.message // 2
        self.band = self.wide + self.near
        self.pack = -(-(rows - self.half) // (LANES // self.wide * SUB)) * SUB
        self.across_rows = self.half + self.pack
        self.down_rows = self.tiles * self.band + (self.tiles - 1) * self.wide
        assert cols % LANES == 0 and rows % SUB == 0 and agents % LANES == 0
        assert 4 * self.wide <= LANES and self.near % SUB == 0 and self.wide % SUB == 0
        assert self.half % SUB == 0 and LANES % self.wide == 0 and self.near % 16 == 0
        assert self.band + self.wide + self.band <= LANES
        assert self.ring % self.blocks == 0 and self.lines % SUB == 0
        assert tasks % PACK == 0 and self.shelf <= LANES and tasks <= LANES
        self.magic = -(-(1 << 16) // self.deep)
        assert all((r * self.magic) >> 16 == r // self.deep for r in range(self.ring))


def lane_of(shape):
    return lax.broadcasted_iota(jnp.int32, shape, len(shape) - 1)


def split_cell(cell, cols):
    if cols & (cols - 1) == 0:
        return cell >> (cols.bit_length() - 1), cell & (cols - 1)
    return lax.div(cell, cols), lax.rem(cell, cols)


def one_hot(ids, positions):
    return jnp.where(ids == positions, 1.0, 0.0).astype(jnp.bfloat16)


def counted(row_hot, col_hot):
    return lax.dot_general(
        row_hot[...], col_hot[...], (((1,), (1,)), ((), ())), preferred_element_type=jnp.float32
    )


def right_roll(p, piece):
    return {"second": p.band, "code": LANES - p.wide}.get(piece, None if isinstance(piece, str) else (piece + 1) * p.wide % LANES)


def left_roll(p, piece):
    return {"second": LANES - p.band, "code": p.wide}.get(piece, None if isinstance(piece, str) else piece * p.wide)


def roll(x, amount):
    amount %= LANES
    return x if amount == 0 else pltpu.roll(x, amount, 1)


def bands_kernel(
    plan, act_in, start_in, code_in, task_in, table_in,
    right, left, ring_row, ring_col, code, task, table, act, start, row_hot, col_hot, sems,
):
    p = plan
    pairs = ((act_in, act), (start_in, start), (code_in, code), (task_in, task), (table_in, table))
    copies = [pltpu.make_async_copy(src, dst, sems.at[n]) for n, (src, dst) in enumerate(pairs)]
    for copy in copies:
        copy.start()
    last = p.tiles - 1
    ring_cols = p.tiles * LANES
    row_id = lax.broadcasted_iota(jnp.int32, (p.message, LANES), 0)
    row_id = jnp.where(row_id >= p.rows + p.near, row_id + p.ring - p.message, row_id)
    lines = (
        (0, p.near, last * LANES),
        (LANES - p.wide, p.wide, (last - 1) * LANES + LANES - p.wide),
        (LANES, p.wide, 0),
        (2 * LANES - p.near, p.near, ring_cols - p.near),
    )
    blank = 0
    for at, n, _ in lines + ((2 * LANES, 0, 0),):
        if at > blank:
            col_hot[blank:at, :] = jnp.zeros((at - blank, p.agents), jnp.bfloat16)
        blank = at + n
    copies[0].wait()
    copies[1].wait()
    for i in range(p.agents // LANES):
        here = slice(i * LANES, (i + 1) * LANES)
        a = act[:, here]
        one = lambda c: jnp.where(a == c, 1, 0)
        row, col = split_cell(start[i : i + 1, :], p.cols)
        row = row + jnp.sum(one(2) - one(1), axis=0, keepdims=True)
        col = col + jnp.sum(one(4) - one(3), axis=0, keepdims=True)
        row = jnp.where(row < 0, row + p.ring, row)
        col = jnp.where(col < 0, col + ring_cols, col)
        ring_row[i : i + 1, :] = row
        ring_col[i : i + 1, :] = col
        row_hot[:, here] = one_hot(row_id, row)
        for at, n, first in lines:
            ids = first + lax.broadcasted_iota(jnp.int32, (n, LANES), 0)
            col_hot[at : at + n, here] = one_hot(ids, col)
    counts = counted(row_hot, col_hot)
    for copy in copies[2:]:
        copy.wait()
    lane = lane_of((p.half, LANES))
    for out, side, spare, shift, band in (
        (right, 0, p.near, right_roll, code[:, (last - 1) * LANES :]),
        (left, 1, LANES - p.near - p.band, left_roll, code[:, :LANES]),
    ):
        own = counts[:, side * LANES : (side + 1) * LANES]
        band = band.astype(jnp.float32)
        x = own[: p.half]
        x = jnp.where((lane >= spare) & (lane < spare + p.band), roll(own[p.half :], shift(p, "second")), x)
        lo = LANES - 2 * p.wide if side == 0 else p.wide
        x = jnp.where((lane >= lo) & (lane < lo + p.wide), roll(band[: p.half], shift(p, "code")), x)
        out[pl.ds(0, p.half), :] = x
        packed_lane = lane_of((p.pack, LANES))
        rest = jnp.zeros((p.pack, LANES), jnp.float32)
        for g in range(LANES // p.wide):
            lo = p.half + g * p.pack
            n = min(p.pack, p.rows - lo)
            if n <= 0:
                break
            y = roll(band[lo : lo + n], shift(p, g))
            if n < p.pack:
                y = jnp.concatenate([y, jnp.zeros((p.pack - n, LANES), jnp.float32)], axis=0)
            rest = jnp.where((packed_lane >= g * p.wide) & (packed_lane < (g + 1) * p.wide), y, rest)
        out[pl.ds(p.half, p.pack), :] = rest


def local_kernel(
    plan, ring_row, ring_col, task, table, hist, address, lane_out, looked, row_hot, col_hot, padded
):
    p = plan
    ring_cols = p.tiles * LANES
    row_id = lax.broadcasted_iota(jnp.int32, (p.ring, LANES), 0)
    col_id = lax.broadcasted_iota(jnp.int32, (ring_cols, LANES), 0)
    for i in range(p.agents // LANES):
        here = slice(i * LANES, (i + 1) * LANES)
        row = ring_row[i : i + 1, :]
        col = ring_col[i : i + 1, :]
        row_hot[:, here] = one_hot(row_id, row)
        col_hot[:, here] = one_hot(col_id, col)
        row = jnp.where(row >= p.rows + p.near, row - p.ring, row) + p.wide
        col = jnp.where(col >= p.cols + p.near, col - ring_cols, col) + p.wide
        t = task[i : i + 1, :]
        u = t // PACK
        block = (row * p.magic) >> 16
        lane_out[i : i + 1, :] = (t - u * PACK) * p.blocks + block
        plane = u * p.deep + row - block * p.deep
        address[i : i + 1, :] = plane * p.lines + col
    counts = counted(row_hot, col_hot)
    for t in range(p.tiles):
        hist[t] = counts[:, t * LANES : (t + 1) * LANES]
    padded[...] = jnp.zeros_like(padded)
    padded[pl.ds(0, p.tasks), pl.ds(0, p.codes)] = table[...]
    upright = jnp.transpose(padded[...])
    for t in range(p.tasks):
        looked[t] = jnp.broadcast_to(upright[: p.shelf, t : t + 1], (p.shelf, LANES))


def side_counts(p, message, shift, lo, n):
    parts = []
    for a, b in ((lo, min(lo + n, p.half)), (max(lo, p.half), lo + n)):
        if a < b and a < p.half:
            parts.append(message[pl.ds(a, b - a), :])
        elif a < b:
            parts.append(roll(message[pl.ds(a - p.half, b - a), :], -shift(p, "second")))
    return parts[0] if len(parts) == 1 else jnp.concatenate(parts, axis=0)


def side_codes(p, message, shift, lo, n):
    parts = []
    at = lo
    while at < lo + n:
        if at < p.half:
            end = min(lo + n, p.half)
            parts.append(roll(message[pl.ds(at, end - at), :], -shift(p, "code")))
        else:
            g, r = divmod(at - p.half, p.pack)
            end = min(lo + n, at - r + p.pack)
            parts.append(roll(message[pl.ds(p.half + r, end - at), :], -shift(p, g)))
        at = end
    return parts[0] if len(parts) == 1 else jnp.concatenate(parts, axis=0)


def merged_counts(p, hist, from_left, from_right, row, n):
    last = p.tiles - 1
    lo = row if row < p.rows + p.near else row - p.ring + p.message
    lane = lane_of((n, LANES))
    l = side_counts(p, from_left, right_roll, lo, n)
    r = side_counts(p, from_right, left_roll, lo, n)
    out = []
    for t in range(p.tiles):
        h = hist[t, pl.ds(row, n), :]
        if t == 0:
            h = h + jnp.where(lane < p.near, l, 0.0)
        if t == last - 1:
            h = h + jnp.where(lane >= LANES - p.near, r, 0.0)
        if t == last:
            h = h + jnp.where(lane >= LANES - p.wide, l, jnp.where(lane < p.wide, r, 0.0))
        out.append(h)
    return out


def merged_codes(p, code, from_left, from_right, row, n):
    last = p.tiles - 1
    lane = lane_of((n, LANES))
    out = [code[pl.ds(row, n), pl.ds(t * LANES, LANES)].astype(jnp.float32) for t in range(last)]
    l = side_codes(p, from_left, right_roll, row, n)
    r = side_codes(p, from_right, left_roll, row, n)
    out.append(jnp.where(lane >= LANES - p.wide, l, jnp.where(lane < p.wide, r, 0.0)))
    return out


def across_kernel(plan, hist, code, from_left, from_right, first, second):
    p = plan
    last = p.tiles - 1
    down_cnt = merged_counts(p, hist, from_left, from_right, p.rows - p.wide, p.band)
    up_near = merged_counts(p, hist, from_left, from_right, p.ring - p.near, p.near)
    up_wide = merged_counts(p, hist, from_left, from_right, 0, p.wide)
    down_code = merged_codes(p, code, from_left, from_right, p.rows - p.wide, p.wide)
    up_code = merged_codes(p, code, from_left, from_right, 0, p.wide)
    lane = lane_of((p.wide, LANES))
    inside = (lane >= p.wide) & (lane < LANES - p.wide)
    half = LANES // 2
    odd = lax.axis_index("gy") % 2 == 1

    def put(at, n, down, up):
        first[pl.ds(at, n), :] = jnp.where(odd, up, down)
        second[pl.ds(at, n), :] = jnp.where(odd, down, up)

    for t in range(p.tiles):
        down, up = down_cnt[t], jnp.concatenate([up_near[t], up_wide[t]], axis=0)
        if t < last:
            put(p.tiles * p.band + t * p.wide, p.wide, down_code[t], up_code[t])
        else:
            head = jnp.where(inside, roll(down_code[t], half), down[: p.wide])
            down = jnp.concatenate([head, down[p.wide :]], axis=0)
            tail = jnp.where(inside, roll(up_code[t], half), up[p.near :])
            up = jnp.concatenate([up[: p.near], tail], axis=0)
        put(t * p.band, p.band, down, up)


def look_up(p, looked):
    def pick(t, low, high):
        found = [
            jnp.take_along_axis(looked[t, pl.ds(g * SUB, SUB), :], low, axis=0, mode="promise_in_bounds")
            for g in range(p.shelf // SUB)
        ]
        for bit in high:
            found = [jnp.where(bit, found[g + 1], found[g]) for g in range(0, len(found), 2)]
        return found[0]

    def put(flat, c, at, code, count):
        crowd = PENALTY * count
        at = pl.ds(at, SUB)
        low = code & (SUB - 1)
        high = [(code & (1 << b)) != 0 for b in range(3, p.code_bits)]
        flat[p.tasks * p.tiles + c, at, :] = jnp.where(code < p.codes - TERMINAL, GAMMA, 0.0)
        for t in range(p.tasks):
            flat[t * p.tiles + c, at, :] = pick(t, low, high) - crowd

    return put


def rewards_kernel(plan, hist, code, from_left, from_right, looked, flat, near):
    p = plan
    put = look_up(p, looked)
    for row in range(0, p.rows, SUB):
        counts = merged_counts(p, hist, from_left, from_right, row, SUB)
        codes = merged_codes(p, code, from_left, from_right, row, SUB)
        for c in range(p.tiles):
            put(flat, c, row + p.wide, codes[c].astype(jnp.int32), counts[c])
    for at, row in ((0, p.rows), (p.near, p.ring - p.near)):
        counts = merged_counts(p, hist, from_left, from_right, row, p.near)
        for c in range(p.tiles):
            near[c, pl.ds(at, p.near), :] = counts[c]


def sweep_kernel(plan, looked, flat_in, near, first, second, address_in, lane_in, values, answers, flat,
                 turned, reward, gain, value, edge, spin, raw, final, natural, rows_of, address, sems):
    p = plan
    del flat_in
    fetch_address = pltpu.make_async_copy(address_in, address, sems.at[p.tasks * (p.tiles - 1)])
    fetch_address.start()
    last = p.tiles - 1
    odd = lax.axis_index("gy") % 2 == 1
    half = LANES // 2
    w, s = p.wide, p.near

    def above(at, n):
        at = pl.ds(at, n)
        return jnp.where(odd, first[at, :], second[at, :])

    def below(at, n):
        at = pl.ds(at, n)
        return jnp.where(odd, second[at, :], first[at, :])

    put = look_up(p, looked)
    for c in range(p.tiles):
        base = c * p.band
        code_base = p.tiles * p.band + c * w
        for at, extra in ((0, above(base + w, s)), (p.rows - s, below(base, s))):
            at = pl.ds(w + at, s)
            for t in range(p.tasks):
                flat[t * p.tiles + c, at, :] = flat[t * p.tiles + c, at, :] - PENALTY * extra
        for row in range(0, w, SUB):
            count = above(base + row, SUB)
            code = above(code_base + row, SUB) if c < last else roll(count, half)
            if row >= w - s:
                count = count + near[c, pl.ds(s + row - (w - s), SUB), :]
            put(flat, c, row, code.astype(jnp.int32) & (p.shelf - 1), count)
            count = below(base + s + row, SUB)
            code = below(code_base + row, SUB) if c < last else roll(count, half)
            if row < s:
                count = count + near[c, pl.ds(row, SUB), :]
            put(flat, c, w + p.rows + row, code.astype(jnp.int32) & (p.shelf - 1), count)

    for u in range(p.groups + 1):
        for i in range(p.deep):
            for c in range(p.tiles):
                parts = []
                for h in range(PACK):
                    t = u * PACK + h if u < p.groups else p.tasks
                    parts.append(flat[t * p.tiles + c, pl.ds(i, p.blocks, stride=p.deep), :])
                x = jnp.transpose(jnp.concatenate(parts, axis=0))
                if c < last:
                    turned[u * p.deep + i, pl.ds(w + c * LANES, LANES), :] = x
                else:
                    turned[u * p.deep + i, pl.ds(w + p.cols, w), :] = x[:w]
                    turned[u * p.deep + i, pl.ds(0, w), :] = x[LANES - w :]

    early = p.span - TAIL
    ends = [(u, up) for u in range(p.groups) for up in (True, False)]

    def end_of(line, u, up):
        return line[u * p.deep + (p.deep - 1 if up else 0)]

    def turn(x, up):
        return pltpu.roll(x, 1 if up else LANES - 1, 1)

    def spot(q, e):
        return pl.ds((q * len(ends) + e) * SUB, SUB)

    def put_ends(q, line):
        for e, (u, up) in enumerate(ends):
            x = end_of(line, u, up)
            if q < early:
                spin[spot(q, e), :] = turn(x, up)
            else:
                raw[spot(q - early, e), :] = x

    for q in range(p.span):
        line = []
        for n in range(p.planes + p.deep):
            x = turned[n, pl.ds(q, SUB, stride=p.span), :]
            if n < p.planes:
                reward[pl.ds((q * p.planes + n) * SUB, SUB), :] = x
                line.append(x)
            else:
                gain[pl.ds((q * p.deep + n - p.planes) * SUB, SUB), :] = x
        put_ends(q, line)

    def sweep(held, put, more=True):
        load = lambda q: [held[pl.ds((q * p.planes + n) * SUB, SUB), :] for n in range(p.planes)]
        for q in range(early, p.span):
            for e, (u, up) in enumerate(ends):
                spin[spot(q, e), :] = turn(raw[spot(q - early, e), :], up)
        now = load(0)
        before = [pltpu.roll(x, 1, 0) for x in load(p.span - 1)]
        for n in range(p.planes):
            edge[pl.ds(n * SUB, SUB), :] = pltpu.roll(now[n], SUB - 1, 0)
        passed = [
            jnp.maximum(before[n - 1], now[n]) if n % p.deep else None for n in range(p.planes)
        ]
        for q in range(p.span):
            if q + 1 < p.span:
                after = load(q + 1)
            else:
                after = [edge[pl.ds(n * SUB, SUB), :] for n in range(p.planes)]
            corner = [None] * p.planes
            made = [None] * p.planes
            for n in range(p.planes):
                above_cell = now[n - 1] if n % p.deep else spin[spot(q, 2 * (n // p.deep)), :]
                corner[n] = jnp.maximum(above_cell, after[n])
            for i in range(p.deep):
                g = gain[pl.ds((q * p.deep + i) * SUB, SUB), :]
                for u in range(p.groups):
                    n = u * p.deep + i
                    if i + 1 < p.deep:
                        other = passed[n + 1]
                    else:
                        other = jnp.maximum(before[n], spin[spot(q, 2 * u + 1), :])
                    best = jnp.maximum(corner[n], other)
                    made[n] = reward[pl.ds((q * p.planes + n) * SUB, SUB), :] + g * best
                    put(q, n, made[n])
            if more:
                put_ends(q, made)
            before, now, passed = now, after, corner

    def put_value(q, n, x):
        value[pl.ds((q * p.planes + n) * SUB, SUB), :] = x

    def put_final(q, n, x):
        final[pl.ds(n * p.lines + q, SUB, stride=p.span), :] = x

    def sweeps(_, carry):
        for _ in range(UNROLL):
            sweep(value, put_value)
        return carry

    assert (SWEEPS - 2) % UNROLL == 0
    sweep(reward, put_value)
    lax.fori_loop(0, (SWEEPS - 2) // UNROLL, sweeps, 0)
    sweep(value, put_final, more=False)
    fetch_address.wait()

    lane_id = lax.broadcasted_iota(jnp.int32, (LANES, LANES), 0)

    def fetch(a):
        rows_of[pl.ds(a, 1), :] = final[pl.ds(address[a // LANES, a % LANES], 1), :]

    def answer(i):
        x = jnp.transpose(rows_of[pl.ds(i * LANES, LANES), :])
        picked = jnp.where(lane_id == lane_in[i : i + 1, :], x, 0.0)
        answers[i : i + 1, :] = jnp.sum(picked, axis=0, keepdims=True)

    copies = []
    fetched = answered = 0
    turns = p.planes * last
    for u in range(p.groups):
        for c in range(last):
            for i in range(p.deep):
                lines = pl.ds((u * p.deep + i) * p.lines + w + c * LANES, LANES)
                x = jnp.transpose(final[lines, :])
                for h in range(PACK):
                    at = pl.ds(i, p.blocks, stride=p.deep)
                    natural[(u * PACK + h) * last + c, at, :] = x[h * p.blocks : (h + 1) * p.blocks]
                until = -(-p.agents * ((u * last + c) * p.deep + i + 1) // turns)
                for a in range(fetched, until):
                    fetch(a)
                fetched = until
                while (answered + 1) * LANES <= fetched:
                    answer(answered)
                    answered += 1
            for h in range(PACK):
                t = u * PACK + h
                copy = pltpu.make_async_copy(
                    natural.at[t * last + c, pl.ds(w, p.rows), :],
                    values.at[t, :, pl.ds(c * LANES, LANES)],
                    sems.at[t * last + c],
                )
                copy.start()
                copies.append(copy)
    for copy in copies:
        copy.wait()


def shift(value, axis, steps):
    count = lax.axis_size(axis)
    return lax.ppermute(value, axis, [(i, (i + steps) % count) for i in range(count)])


def swap(value, axis, parity):
    count = lax.axis_size(axis)
    assert count % 2 == 0
    return lax.ppermute(
        value, axis, [(i, (i + (1 if i % 2 == parity else -1)) % count) for i in range(count)]
    )


def on_device(map_codes, reward_table, start_cell, agent_task, actions):
    rows, cols = map_codes.shape
    tasks, codes = reward_table.shape
    steps, agents = actions.shape
    p = Plan(rows, cols, agents, steps, tasks, codes)
    vmem = pl.BlockSpec(memory_space=pltpu.VMEM)
    smem = pl.BlockSpec(memory_space=pltpu.SMEM)
    f32, i32 = jnp.float32, jnp.int32
    shape = jax.ShapeDtypeStruct
    fast = lambda dims, dtype: pltpu.VMEM(dims, dtype)
    far = lambda x: pltpu.with_memory_space_constraint(x, pltpu.HBM)
    near = lambda x: pltpu.with_memory_space_constraint(x, pltpu.VMEM)
    by_lane = (agents // LANES, LANES)

    def bind(kernel):
        def body(*refs):
            kernel(p, *refs)

        return body

    to_right, to_left, ring_row, ring_col, kept, task, table = pl.pallas_call(
        bind(bands_kernel),
        in_specs=[pl.BlockSpec(memory_space=pl.ANY)] * 5,
        out_specs=[vmem] * 7,
        out_shape=[
            fast((p.across_rows, LANES), f32),
            fast((p.across_rows, LANES), f32),
            fast(by_lane, i32),
            fast(by_lane, i32),
            fast((rows, cols), i32),
            fast(by_lane, i32),
            fast((tasks, codes), f32),
        ],
        scratch_shapes=[
            pltpu.VMEM((steps, agents), i32),
            pltpu.VMEM(by_lane, i32),
            pltpu.VMEM((p.message, agents), jnp.bfloat16),
            pltpu.VMEM((2 * LANES, agents), jnp.bfloat16),
            pltpu.SemaphoreType.DMA((5,)),
        ],
        compiler_params=pltpu.CompilerParams(vmem_limit_bytes=12 << 20),
        name="bands",
    )(*map(far, (actions, start_cell.reshape(by_lane), map_codes, agent_task.reshape(by_lane), reward_table)))
    from_left = shift(to_right, "gx", 1)
    from_right = shift(to_left, "gx", -1)
    hist, address, lane, looked = pl.pallas_call(
        bind(local_kernel),
        in_specs=[vmem] * 4,
        out_specs=[vmem] * 4,
        out_shape=[
            fast((p.tiles, p.ring, LANES), f32),
            fast(by_lane, i32),
            fast(by_lane, i32),
            fast((tasks, p.shelf, LANES), f32),
        ],
        scratch_shapes=[
            pltpu.VMEM((p.ring, agents), jnp.bfloat16),
            pltpu.VMEM((p.tiles * LANES, agents), jnp.bfloat16),
            pltpu.VMEM((LANES, LANES), f32),
        ],
        compiler_params=pltpu.CompilerParams(vmem_limit_bytes=12 << 20),
        name="local",
    )(near(ring_row), near(ring_col), near(task), near(table))
    sides = (near(hist), near(kept), near(from_left), near(from_right))
    first, second = pl.pallas_call(
        bind(across_kernel),
        in_specs=[vmem] * 4,
        out_specs=[vmem] * 2,
        out_shape=[fast((p.down_rows, LANES), f32), fast((p.down_rows, LANES), f32)],
        compiler_params=pltpu.CompilerParams(vmem_limit_bytes=8 << 20),
        name="across",
    )(*sides)
    first = swap(first, "gy", 0)
    second = swap(second, "gy", 1)
    flats = ((tasks + 1) * p.tiles, p.ring, LANES)
    flat, edges = pl.pallas_call(
        bind(rewards_kernel),
        in_specs=[vmem] * 5,
        out_specs=[vmem] * 2,
        out_shape=[fast(flats, f32), fast((p.tiles, 2 * p.near, LANES), f32)],
        compiler_params=pltpu.CompilerParams(vmem_limit_bytes=12 << 20),
        name="rewards",
    )(*sides, near(looked))
    outs = tasks * (p.tiles - 1)
    values, answers, _ = pl.pallas_call(
        bind(sweep_kernel),
        in_specs=[vmem] * 7,
        out_specs=[pl.BlockSpec(memory_space=pl.ANY), vmem, vmem],
        out_shape=[shape((tasks, rows, cols), f32), shape(by_lane, f32), fast(flats, f32)],
        scratch_shapes=[
            pltpu.VMEM((p.planes + p.deep, p.lines, LANES), f32),
            pltpu.VMEM((p.planes * p.lines, LANES), f32),
            pltpu.VMEM((p.deep * p.lines, LANES), f32),
            pltpu.VMEM((p.planes * p.lines, LANES), f32),
            pltpu.VMEM((p.planes * SUB, LANES), f32),
            pltpu.VMEM((2 * p.groups * p.span * SUB, LANES), f32),
            pltpu.VMEM((2 * p.groups * TAIL * SUB, LANES), f32),
            pltpu.VMEM((p.planes * p.lines, LANES), f32),
            pltpu.VMEM((outs, p.ring, LANES), f32),
            pltpu.VMEM((agents, LANES), f32),
            pltpu.SMEM(by_lane, i32),
            pltpu.SemaphoreType.DMA((outs + 1,)),
        ],
        input_output_aliases={1: 2},
        compiler_params=pltpu.CompilerParams(vmem_limit_bytes=24 << 20),
        name="sweep",
    )(near(looked), near(flat), near(edges), near(first), near(second), near(address), near(lane))
    return values, answers.reshape(agents)


def solution(mesh):
    placed = (P("gy", "gx"), P(), P(("gx", "gy")), P(("gx", "gy")), P(None, ("gx", "gy")))
    return jax.shard_map(
        on_device,
        mesh=mesh,
        in_specs=placed,
        out_specs=(P(None, "gy", "gx"), P(("gx", "gy"))),
        check_vma=False,
    )
```

```python
import jax
import jax.numpy as jnp
from jax import lax
from jax.experimental import pallas as pl
from jax.experimental.pallas import tpu as pltpu
from jax.sharding import PartitionSpec as P


SWEEPS = 16
TERMINAL = 2
GAMMA = 0.95
PENALTY = 0.5
LANES = 128
SUB = 8
PACK = 2
UNROLL = 2
TAIL = 12


class Plan:
    def __init__(self, rows, cols, agents, steps, tasks, codes):
        self.rows, self.cols, self.agents = rows, cols, agents
        self.steps, self.tasks, self.codes = steps, tasks, codes
        self.near = steps
        self.wide = steps + SWEEPS
        self.ring = rows + 2 * self.wide
        self.tiles = cols // LANES + 1
        self.span = (cols + 2 * self.wide) // SUB
        self.span += 1 - self.span % 2
        self.lines = self.span * SUB
        self.blocks = LANES // PACK
        self.deep = self.ring // self.blocks
        self.groups = tasks // PACK
        self.planes = self.groups * self.deep
        self.code_bits = max(3, (codes - 1).bit_length())
        self.shelf = 1 << self.code_bits
        self.message = rows + 2 * self.near
        self.half = self.message // 2
        self.band = self.wide + self.near
        self.pack = -(-(rows - self.half) // (LANES // self.wide * SUB)) * SUB
        self.across_rows = self.half + self.pack
        self.down_rows = self.tiles * self.band + (self.tiles - 1) * self.wide
        assert cols % LANES == 0 and rows % SUB == 0 and agents % LANES == 0
        assert 4 * self.wide <= LANES and self.near % SUB == 0 and self.wide % SUB == 0
        assert self.half % SUB == 0 and LANES % self.wide == 0 and self.near % 16 == 0
        assert self.band + self.wide + self.band <= LANES
        assert self.ring % self.blocks == 0
        assert tasks % PACK == 0 and self.shelf <= LANES and tasks <= LANES
        self.magic = -(-(1 << 16) // self.deep)
        assert all((r * self.magic) >> 16 == r // self.deep for r in range(self.ring))


def lane_of(shape):
    return lax.broadcasted_iota(jnp.int32, shape, len(shape) - 1)


def split_cell(cell, cols):
    if cols & (cols - 1) == 0:
        return cell >> (cols.bit_length() - 1), cell & (cols - 1)
    return lax.div(cell, cols), lax.rem(cell, cols)


def one_hot(ids, positions):
    return jnp.where(ids == positions, 1.0, 0.0).astype(jnp.bfloat16)


def counted(row_hot, col_hot):
    return lax.dot_general(
        row_hot[...], col_hot[...], (((1,), (1,)), ((), ())), preferred_element_type=jnp.float32
    )


def right_roll(p, piece):
    return {"second": p.band, "code": LANES - p.wide}.get(piece, None if isinstance(piece, str) else (piece + 1) * p.wide % LANES)


def left_roll(p, piece):
    return {"second": LANES - p.band, "code": p.wide}.get(piece, None if isinstance(piece, str) else piece * p.wide)


def roll(x, amount):
    amount %= LANES
    return x if amount == 0 else pltpu.roll(x, amount, 1)


def bands_kernel(
    plan, act_in, start_in, code_in, task_in, table_in,
    right, left, ring_row, ring_col, code, task, table, act, start, row_hot, col_hot, sems,
):
    p = plan
    pairs = ((act_in, act), (start_in, start), (code_in, code), (task_in, task), (table_in, table))
    copies = [pltpu.make_async_copy(src, dst, sems.at[n]) for n, (src, dst) in enumerate(pairs)]
    for copy in copies:
        copy.start()
    last = p.tiles - 1
    ring_cols = p.tiles * LANES
    row_id = lax.broadcasted_iota(jnp.int32, (p.message, LANES), 0)
    row_id = jnp.where(row_id >= p.rows + p.near, row_id + p.ring - p.message, row_id)
    lines = (
        (0, p.near, last * LANES),
        (LANES - p.wide, p.wide, (last - 1) * LANES + LANES - p.wide),
        (LANES, p.wide, 0),
        (2 * LANES - p.near, p.near, ring_cols - p.near),
    )
    blank = 0
    for at, n, _ in lines + ((2 * LANES, 0, 0),):
        if at > blank:
            col_hot[blank:at, :] = jnp.zeros((at - blank, p.agents), jnp.bfloat16)
        blank = at + n
    copies[0].wait()
    copies[1].wait()
    for i in range(p.agents // LANES):
        here = slice(i * LANES, (i + 1) * LANES)
        a = act[:, here]
        one = lambda c: jnp.where(a == c, 1, 0)
        row, col = split_cell(start[i : i + 1, :], p.cols)
        row = row + jnp.sum(one(2) - one(1), axis=0, keepdims=True)
        col = col + jnp.sum(one(4) - one(3), axis=0, keepdims=True)
        row = jnp.where(row < 0, row + p.ring, row)
        col = jnp.where(col < 0, col + ring_cols, col)
        ring_row[i : i + 1, :] = row
        ring_col[i : i + 1, :] = col
        row_hot[:, here] = one_hot(row_id, row)
        for at, n, first in lines:
            ids = first + lax.broadcasted_iota(jnp.int32, (n, LANES), 0)
            col_hot[at : at + n, here] = one_hot(ids, col)
    counts = counted(row_hot, col_hot)
    for copy in copies[2:]:
        copy.wait()
    lane = lane_of((p.half, LANES))
    for out, side, spare, shift, band in (
        (right, 0, p.near, right_roll, code[:, (last - 1) * LANES :]),
        (left, 1, LANES - p.near - p.band, left_roll, code[:, :LANES]),
    ):
        own = counts[:, side * LANES : (side + 1) * LANES]
        band = band.astype(jnp.float32)
        x = own[: p.half]
        x = jnp.where((lane >= spare) & (lane < spare + p.band), roll(own[p.half :], shift(p, "second")), x)
        lo = LANES - 2 * p.wide if side == 0 else p.wide
        x = jnp.where((lane >= lo) & (lane < lo + p.wide), roll(band[: p.half], shift(p, "code")), x)
        out[pl.ds(0, p.half), :] = x
        packed_lane = lane_of((p.pack, LANES))
        rest = jnp.zeros((p.pack, LANES), jnp.float32)
        for g in range(LANES // p.wide):
            lo = p.half + g * p.pack
            n = min(p.pack, p.rows - lo)
            if n <= 0:
                break
            y = roll(band[lo : lo + n], shift(p, g))
            if n < p.pack:
                y = jnp.concatenate([y, jnp.zeros((p.pack - n, LANES), jnp.float32)], axis=0)
            rest = jnp.where((packed_lane >= g * p.wide) & (packed_lane < (g + 1) * p.wide), y, rest)
        out[pl.ds(p.half, p.pack), :] = rest


def local_kernel(
    plan, ring_row, ring_col, task, table, hist, address, lane_out, looked, row_hot, col_hot, padded
):
    p = plan
    ring_cols = p.tiles * LANES
    row_id = lax.broadcasted_iota(jnp.int32, (p.ring, LANES), 0)
    col_id = lax.broadcasted_iota(jnp.int32, (ring_cols, LANES), 0)
    for i in range(p.agents // LANES):
        here = slice(i * LANES, (i + 1) * LANES)
        row = ring_row[i : i + 1, :]
        col = ring_col[i : i + 1, :]
        row_hot[:, here] = one_hot(row_id, row)
        col_hot[:, here] = one_hot(col_id, col)
        row = jnp.where(row >= p.rows + p.near, row - p.ring, row) + p.wide
        col = jnp.where(col >= p.cols + p.near, col - ring_cols, col) + p.wide
        t = task[i : i + 1, :]
        u = t // PACK
        block = (row * p.magic) >> 16
        lane_out[i : i + 1, :] = (t - u * PACK) * p.blocks + block
        plane = u * p.deep + row - block * p.deep
        address[i : i + 1, :] = plane * p.lines + col
    counts = counted(row_hot, col_hot)
    for t in range(p.tiles):
        hist[t] = counts[:, t * LANES : (t + 1) * LANES]
    padded[...] = jnp.zeros_like(padded)
    padded[pl.ds(0, p.tasks), pl.ds(0, p.codes)] = table[...]
    upright = jnp.transpose(padded[...])
    for t in range(p.tasks):
        looked[t] = jnp.broadcast_to(upright[: p.shelf, t : t + 1], (p.shelf, LANES))


def side_counts(p, message, shift, lo, n):
    parts = []
    for a, b in ((lo, min(lo + n, p.half)), (max(lo, p.half), lo + n)):
        if a < b and a < p.half:
            parts.append(message[pl.ds(a, b - a), :])
        elif a < b:
            parts.append(roll(message[pl.ds(a - p.half, b - a), :], -shift(p, "second")))
    return parts[0] if len(parts) == 1 else jnp.concatenate(parts, axis=0)


def side_codes(p, message, shift, lo, n):
    parts = []
    at = lo
    while at < lo + n:
        if at < p.half:
            end = min(lo + n, p.half)
            parts.append(roll(message[pl.ds(at, end - at), :], -shift(p, "code")))
        else:
            g, r = divmod(at - p.half, p.pack)
            end = min(lo + n, at - r + p.pack)
            parts.append(roll(message[pl.ds(p.half + r, end - at), :], -shift(p, g)))
        at = end
    return parts[0] if len(parts) == 1 else jnp.concatenate(parts, axis=0)


def merged_counts(p, hist, from_left, from_right, row, n):
    last = p.tiles - 1
    lo = row if row < p.rows + p.near else row - p.ring + p.message
    lane = lane_of((n, LANES))
    l = side_counts(p, from_left, right_roll, lo, n)
    r = side_counts(p, from_right, left_roll, lo, n)
    out = []
    for t in range(p.tiles):
        h = hist[t, pl.ds(row, n), :]
        if t == 0:
            h = h + jnp.where(lane < p.near, l, 0.0)
        if t == last - 1:
            h = h + jnp.where(lane >= LANES - p.near, r, 0.0)
        if t == last:
            h = h + jnp.where(lane >= LANES - p.wide, l, jnp.where(lane < p.wide, r, 0.0))
        out.append(h)
    return out


def merged_codes(p, code, from_left, from_right, row, n):
    last = p.tiles - 1
    lane = lane_of((n, LANES))
    out = [code[pl.ds(row, n), pl.ds(t * LANES, LANES)].astype(jnp.float32) for t in range(last)]
    l = side_codes(p, from_left, right_roll, row, n)
    r = side_codes(p, from_right, left_roll, row, n)
    out.append(jnp.where(lane >= LANES - p.wide, l, jnp.where(lane < p.wide, r, 0.0)))
    return out


def across_kernel(plan, hist, code, from_left, from_right, first, second):
    p = plan
    last = p.tiles - 1
    down_cnt = merged_counts(p, hist, from_left, from_right, p.rows - p.wide, p.band)
    up_near = merged_counts(p, hist, from_left, from_right, p.ring - p.near, p.near)
    up_wide = merged_counts(p, hist, from_left, from_right, 0, p.wide)
    down_code = merged_codes(p, code, from_left, from_right, p.rows - p.wide, p.wide)
    up_code = merged_codes(p, code, from_left, from_right, 0, p.wide)
    lane = lane_of((p.wide, LANES))
    inside = (lane >= p.wide) & (lane < LANES - p.wide)
    half = LANES // 2
    odd = lax.axis_index("gy") % 2 == 1

    def put(at, n, down, up):
        first[pl.ds(at, n), :] = jnp.where(odd, up, down)
        second[pl.ds(at, n), :] = jnp.where(odd, down, up)

    for t in range(p.tiles):
        down, up = down_cnt[t], jnp.concatenate([up_near[t], up_wide[t]], axis=0)
        if t < last:
            put(p.tiles * p.band + t * p.wide, p.wide, down_code[t], up_code[t])
        else:
            head = jnp.where(inside, roll(down_code[t], half), down[: p.wide])
            down = jnp.concatenate([head, down[p.wide :]], axis=0)
            tail = jnp.where(inside, roll(up_code[t], half), up[p.near :])
            up = jnp.concatenate([up[: p.near], tail], axis=0)
        put(t * p.band, p.band, down, up)


def look_up(p, looked):
    def pick(t, low, high):
        found = [
            jnp.take_along_axis(looked[t, pl.ds(g * SUB, SUB), :], low, axis=0, mode="promise_in_bounds")
            for g in range(p.shelf // SUB)
        ]
        for bit in high:
            found = [jnp.where(bit, found[g + 1], found[g]) for g in range(0, len(found), 2)]
        return found[0]

    def put(flat, c, at, code, count):
        crowd = PENALTY * count
        at = pl.ds(at, SUB)
        low = code & (SUB - 1)
        high = [(code & (1 << b)) != 0 for b in range(3, p.code_bits)]
        flat[p.tasks * p.tiles + c, at, :] = jnp.where(code < p.codes - TERMINAL, GAMMA, 0.0)
        for t in range(p.tasks):
            flat[t * p.tiles + c, at, :] = pick(t, low, high) - crowd

    return put


def rewards_kernel(plan, hist, code, from_left, from_right, looked, flat, near):
    p = plan
    put = look_up(p, looked)
    for row in range(0, p.rows, SUB):
        counts = merged_counts(p, hist, from_left, from_right, row, SUB)
        codes = merged_codes(p, code, from_left, from_right, row, SUB)
        for c in range(p.tiles):
            put(flat, c, row + p.wide, codes[c].astype(jnp.int32), counts[c])
    for at, row in ((0, p.rows), (p.near, p.ring - p.near)):
        counts = merged_counts(p, hist, from_left, from_right, row, p.near)
        for c in range(p.tiles):
            near[c, pl.ds(at, p.near), :] = counts[c]


def sweep_kernel(plan, looked, flat_in, near, first, second, address_in, lane_in, values, answers, flat,
                 turned, reward, gain, value, edge, spin, raw, final, natural, rows_of, address, sems):
    p = plan
    del flat_in
    fetch_address = pltpu.make_async_copy(address_in, address, sems.at[p.tasks * (p.tiles - 1)])
    fetch_address.start()
    last = p.tiles - 1
    odd = lax.axis_index("gy") % 2 == 1
    half = LANES // 2
    w, s = p.wide, p.near

    def above(at, n):
        at = pl.ds(at, n)
        return jnp.where(odd, first[at, :], second[at, :])

    def below(at, n):
        at = pl.ds(at, n)
        return jnp.where(odd, second[at, :], first[at, :])

    put = look_up(p, looked)
    for c in range(p.tiles):
        base = c * p.band
        code_base = p.tiles * p.band + c * w
        for at, extra in ((0, above(base + w, s)), (p.rows - s, below(base, s))):
            at = pl.ds(w + at, s)
            for t in range(p.tasks):
                flat[t * p.tiles + c, at, :] = flat[t * p.tiles + c, at, :] - PENALTY * extra
        for row in range(0, w, SUB):
            count = above(base + row, SUB)
            code = above(code_base + row, SUB) if c < last else roll(count, half)
            if row >= w - s:
                count = count + near[c, pl.ds(s + row - (w - s), SUB), :]
            put(flat, c, row, code.astype(jnp.int32) & (p.shelf - 1), count)
            count = below(base + s + row, SUB)
            code = below(code_base + row, SUB) if c < last else roll(count, half)
            if row < s:
                count = count + near[c, pl.ds(row, SUB), :]
            put(flat, c, w + p.rows + row, code.astype(jnp.int32) & (p.shelf - 1), count)

    for u in range(p.groups + 1):
        for i in range(p.deep):
            for c in range(p.tiles):
                parts = []
                for h in range(PACK):
                    t = u * PACK + h if u < p.groups else p.tasks
                    parts.append(flat[t * p.tiles + c, pl.ds(i, p.blocks, stride=p.deep), :])
                x = jnp.transpose(jnp.concatenate(parts, axis=0))
                if c < last:
                    turned[u * p.deep + i, pl.ds(w + c * LANES, LANES), :] = x
                else:
                    turned[u * p.deep + i, pl.ds(w + p.cols, w), :] = x[:w]
                    turned[u * p.deep + i, pl.ds(0, w), :] = x[LANES - w :]

    early = p.span - TAIL
    ends = [(u, up) for u in range(p.groups) for up in (True, False)]

    def end_of(line, u, up):
        return line[u * p.deep + (p.deep - 1 if up else 0)]

    def turn(x, up):
        return pltpu.roll(x, 1 if up else LANES - 1, 1)

    def spot(q, e):
        return pl.ds((q * len(ends) + e) * SUB, SUB)

    def put_ends(q, line):
        for e, (u, up) in enumerate(ends):
            x = end_of(line, u, up)
            if q < early:
                spin[spot(q, e), :] = turn(x, up)
            else:
                raw[spot(q - early, e), :] = x

    for q in range(p.span):
        line = []
        for n in range(p.planes + p.deep):
            x = turned[n, pl.ds(q, SUB, stride=p.span), :]
            if n < p.planes:
                reward[pl.ds((q * p.planes + n) * SUB, SUB), :] = x
                line.append(x)
            else:
                gain[pl.ds((q * p.deep + n - p.planes) * SUB, SUB), :] = x
        put_ends(q, line)

    def sweep(held, put, more=True):
        load = lambda q: [held[pl.ds((q * p.planes + n) * SUB, SUB), :] for n in range(p.planes)]
        for q in range(early, p.span):
            for e, (u, up) in enumerate(ends):
                spin[spot(q, e), :] = turn(raw[spot(q - early, e), :], up)
        now = load(0)
        before = [pltpu.roll(x, 1, 0) for x in load(p.span - 1)]
        for n in range(p.planes):
            edge[pl.ds(n * SUB, SUB), :] = pltpu.roll(now[n], SUB - 1, 0)
        passed = [
            jnp.maximum(before[n - 1], now[n]) if n % p.deep else None for n in range(p.planes)
        ]
        for q in range(p.span):
            if q + 1 < p.span:
                after = load(q + 1)
            else:
                after = [edge[pl.ds(n * SUB, SUB), :] for n in range(p.planes)]
            corner = [None] * p.planes
            made = [None] * p.planes
            for n in range(p.planes):
                above_cell = now[n - 1] if n % p.deep else spin[spot(q, 2 * (n // p.deep)), :]
                corner[n] = jnp.maximum(above_cell, after[n])
            for i in range(p.deep):
                g = gain[pl.ds((q * p.deep + i) * SUB, SUB), :]
                for u in range(p.groups):
                    n = u * p.deep + i
                    if i + 1 < p.deep:
                        other = passed[n + 1]
                    else:
                        other = jnp.maximum(before[n], spin[spot(q, 2 * u + 1), :])
                    best = jnp.maximum(corner[n], other)
                    made[n] = reward[pl.ds((q * p.planes + n) * SUB, SUB), :] + g * best
                    put(q, n, made[n])
            if more:
                put_ends(q, made)
            before, now, passed = now, after, corner

    def put_value(q, n, x):
        value[pl.ds((q * p.planes + n) * SUB, SUB), :] = x

    def put_final(q, n, x):
        final[pl.ds(n * p.lines + q, SUB, stride=p.span), :] = x

    def sweeps(_, carry):
        for _ in range(UNROLL):
            sweep(value, put_value)
        return carry

    assert (SWEEPS - 2) % UNROLL == 0
    sweep(reward, put_value)
    lax.fori_loop(0, (SWEEPS - 2) // UNROLL, sweeps, 0)
    sweep(value, put_final, more=False)
    fetch_address.wait()

    lane_id = lax.broadcasted_iota(jnp.int32, (LANES, LANES), 0)

    def fetch(a):
        rows_of[pl.ds(a, 1), :] = final[pl.ds(address[a // LANES, a % LANES], 1), :]

    def answer(i):
        x = jnp.transpose(rows_of[pl.ds(i * LANES, LANES), :])
        picked = jnp.where(lane_id == lane_in[i : i + 1, :], x, 0.0)
        answers[i : i + 1, :] = jnp.sum(picked, axis=0, keepdims=True)

    copies = []
    fetched = answered = 0
    turns = p.planes * last
    for u in range(p.groups):
        for c in range(last):
            for i in range(p.deep):
                lines = pl.ds((u * p.deep + i) * p.lines + w + c * LANES, LANES)
                x = jnp.transpose(final[lines, :])
                for h in range(PACK):
                    at = pl.ds(i, p.blocks, stride=p.deep)
                    natural[(u * PACK + h) * last + c, at, :] = x[h * p.blocks : (h + 1) * p.blocks]
                until = min(p.agents, -(-p.agents * 5 * ((u * last + c) * p.deep + i + 1) // (8 * turns)))
                for a in range(fetched, until):
                    fetch(a)
                fetched = until
                while (answered + 1) * LANES <= fetched:
                    answer(answered)
                    answered += 1
            for h in range(PACK):
                t = u * PACK + h
                copy = pltpu.make_async_copy(
                    natural.at[t * last + c, pl.ds(w, p.rows), :],
                    values.at[t, :, pl.ds(c * LANES, LANES)],
                    sems.at[t * last + c],
                )
                copy.start()
                copies.append(copy)
    for a in range(fetched, p.agents):
        fetch(a)
        if (a + 1) % LANES == 0:
            answer(a // LANES)
    for copy in copies:
        copy.wait()


def shift(value, axis, steps):
    count = lax.axis_size(axis)
    return lax.ppermute(value, axis, [(i, (i + steps) % count) for i in range(count)])


def swap(value, axis, parity):
    count = lax.axis_size(axis)
    assert count % 2 == 0
    return lax.ppermute(
        value, axis, [(i, (i + (1 if i % 2 == parity else -1)) % count) for i in range(count)]
    )


def on_device(map_codes, reward_table, start_cell, agent_task, actions):
    rows, cols = map_codes.shape
    tasks, codes = reward_table.shape
    steps, agents = actions.shape
    p = Plan(rows, cols, agents, steps, tasks, codes)
    vmem = pl.BlockSpec(memory_space=pltpu.VMEM)
    smem = pl.BlockSpec(memory_space=pltpu.SMEM)
    f32, i32 = jnp.float32, jnp.int32
    shape = jax.ShapeDtypeStruct
    fast = lambda dims, dtype: pltpu.VMEM(dims, dtype)
    far = lambda x: pltpu.with_memory_space_constraint(x, pltpu.HBM)
    near = lambda x: pltpu.with_memory_space_constraint(x, pltpu.VMEM)
    by_lane = (agents // LANES, LANES)

    def bind(kernel):
        def body(*refs):
            kernel(p, *refs)

        return body

    to_right, to_left, ring_row, ring_col, kept, task, table = pl.pallas_call(
        bind(bands_kernel),
        in_specs=[pl.BlockSpec(memory_space=pl.ANY)] * 5,
        out_specs=[vmem] * 7,
        out_shape=[
            fast((p.across_rows, LANES), f32),
            fast((p.across_rows, LANES), f32),
            fast(by_lane, i32),
            fast(by_lane, i32),
            fast((rows, cols), i32),
            fast(by_lane, i32),
            fast((tasks, codes), f32),
        ],
        scratch_shapes=[
            pltpu.VMEM((steps, agents), i32),
            pltpu.VMEM(by_lane, i32),
            pltpu.VMEM((p.message, agents), jnp.bfloat16),
            pltpu.VMEM((2 * LANES, agents), jnp.bfloat16),
            pltpu.SemaphoreType.DMA((5,)),
        ],
        compiler_params=pltpu.CompilerParams(vmem_limit_bytes=12 << 20),
        name="bands",
    )(*map(far, (actions, start_cell.reshape(by_lane), map_codes, agent_task.reshape(by_lane), reward_table)))
    from_left = shift(to_right, "gx", 1)
    from_right = shift(to_left, "gx", -1)
    hist, address, lane, looked = pl.pallas_call(
        bind(local_kernel),
        in_specs=[vmem] * 4,
        out_specs=[vmem] * 4,
        out_shape=[
            fast((p.tiles, p.ring, LANES), f32),
            fast(by_lane, i32),
            fast(by_lane, i32),
            fast((tasks, p.shelf, LANES), f32),
        ],
        scratch_shapes=[
            pltpu.VMEM((p.ring, agents), jnp.bfloat16),
            pltpu.VMEM((p.tiles * LANES, agents), jnp.bfloat16),
            pltpu.VMEM((LANES, LANES), f32),
        ],
        compiler_params=pltpu.CompilerParams(vmem_limit_bytes=12 << 20),
        name="local",
    )(near(ring_row), near(ring_col), near(task), near(table))
    sides = (near(hist), near(kept), near(from_left), near(from_right))
    first, second = pl.pallas_call(
        bind(across_kernel),
        in_specs=[vmem] * 4,
        out_specs=[vmem] * 2,
        out_shape=[fast((p.down_rows, LANES), f32), fast((p.down_rows, LANES), f32)],
        compiler_params=pltpu.CompilerParams(vmem_limit_bytes=8 << 20),
        name="across",
    )(*sides)
    first = swap(first, "gy", 0)
    second = swap(second, "gy", 1)
    flats = ((tasks + 1) * p.tiles, p.ring, LANES)
    flat, edges = pl.pallas_call(
        bind(rewards_kernel),
        in_specs=[vmem] * 5,
        out_specs=[vmem] * 2,
        out_shape=[fast(flats, f32), fast((p.tiles, 2 * p.near, LANES), f32)],
        compiler_params=pltpu.CompilerParams(vmem_limit_bytes=12 << 20),
        name="rewards",
    )(*sides, near(looked))
    outs = tasks * (p.tiles - 1)
    values, answers, _ = pl.pallas_call(
        bind(sweep_kernel),
        in_specs=[vmem] * 7,
        out_specs=[pl.BlockSpec(memory_space=pl.ANY), vmem, vmem],
        out_shape=[shape((tasks, rows, cols), f32), shape(by_lane, f32), fast(flats, f32)],
        scratch_shapes=[
            pltpu.VMEM((p.planes + p.deep, p.lines, LANES), f32),
            pltpu.VMEM((p.planes * p.lines, LANES), f32),
            pltpu.VMEM((p.deep * p.lines, LANES), f32),
            pltpu.VMEM((p.planes * p.lines, LANES), f32),
            pltpu.VMEM((p.planes * SUB, LANES), f32),
            pltpu.VMEM((2 * p.groups * p.span * SUB, LANES), f32),
            pltpu.VMEM((2 * p.groups * TAIL * SUB, LANES), f32),
            pltpu.VMEM((p.planes * p.lines, LANES), f32),
            pltpu.VMEM((outs, p.ring, LANES), f32),
            pltpu.VMEM((agents, LANES), f32),
            pltpu.SMEM(by_lane, i32),
            pltpu.SemaphoreType.DMA((outs + 1,)),
        ],
        input_output_aliases={1: 2},
        compiler_params=pltpu.CompilerParams(vmem_limit_bytes=24 << 20),
        name="sweep",
    )(near(looked), near(flat), near(edges), near(first), near(second), near(address), near(lane))
    return values, answers.reshape(agents)


def solution(mesh):
    placed = (P("gy", "gx"), P(), P(("gx", "gy")), P(("gx", "gy")), P(None, ("gx", "gy")))
    return jax.shard_map(
        on_device,
        mesh=mesh,
        in_specs=placed,
        out_specs=(P(None, "gy", "gx"), P(("gx", "gy"))),
        check_vma=False,
    )
```

```python
import jax
import jax.numpy as jnp
from jax import lax
from jax.experimental import pallas as pl
from jax.experimental.pallas import tpu as pltpu
from jax.sharding import PartitionSpec as P


SWEEPS = 16
TERMINAL = 2
GAMMA = 0.95
PENALTY = 0.5
LANES = 128
SUB = 8
PACK = 2
UNROLL = 7
TAIL = 12


class Plan:
    def __init__(self, rows, cols, agents, steps, tasks, codes):
        self.rows, self.cols, self.agents = rows, cols, agents
        self.steps, self.tasks, self.codes = steps, tasks, codes
        self.near = steps
        self.wide = steps + SWEEPS
        self.ring = rows + 2 * self.wide
        self.tiles = cols // LANES + 1
        self.span = (cols + 2 * self.wide) // SUB
        self.span += 1 - self.span % 2
        self.lines = self.span * SUB
        self.blocks = LANES // PACK
        self.deep = self.ring // self.blocks
        self.groups = tasks // PACK
        self.planes = self.groups * self.deep
        self.code_bits = max(3, (codes - 1).bit_length())
        self.shelf = 1 << self.code_bits
        self.message = rows + 2 * self.near
        self.half = self.message // 2
        self.band = self.wide + self.near
        self.pack = -(-(rows - self.half) // (LANES // self.wide * SUB)) * SUB
        self.across_rows = self.half + self.pack
        self.down_rows = self.tiles * self.band + (self.tiles - 1) * self.wide
        assert cols % LANES == 0 and rows % SUB == 0 and agents % LANES == 0
        assert 4 * self.wide <= LANES and self.near % SUB == 0 and self.wide % SUB == 0
        assert self.half % SUB == 0 and LANES % self.wide == 0 and self.near % 16 == 0
        assert self.band + self.wide + self.band <= LANES
        assert self.ring % self.blocks == 0
        assert tasks % PACK == 0 and self.shelf <= LANES and tasks <= LANES
        self.magic = -(-(1 << 16) // self.deep)
        assert all((r * self.magic) >> 16 == r // self.deep for r in range(self.ring))


def lane_of(shape):
    return lax.broadcasted_iota(jnp.int32, shape, len(shape) - 1)


def split_cell(cell, cols):
    if cols & (cols - 1) == 0:
        return cell >> (cols.bit_length() - 1), cell & (cols - 1)
    return lax.div(cell, cols), lax.rem(cell, cols)


def one_hot(ids, positions):
    same = ids.astype(jnp.int16) == positions.astype(jnp.int16)
    return jnp.where(same, jnp.bfloat16(1), jnp.bfloat16(0))


def counted(row_hot, col_hot):
    return lax.dot_general(
        row_hot[...], col_hot[...], (((1,), (1,)), ((), ())), preferred_element_type=jnp.float32
    )


def right_roll(p, piece):
    return {"second": p.band, "code": LANES - p.wide}.get(piece, None if isinstance(piece, str) else (piece + 1) * p.wide % LANES)


def left_roll(p, piece):
    return {"second": LANES - p.band, "code": p.wide}.get(piece, None if isinstance(piece, str) else piece * p.wide)


def roll(x, amount):
    amount %= LANES
    return x if amount == 0 else pltpu.roll(x, amount, 1)


def bands_kernel(
    plan, act_in, start_in, code_in, task_in, table_in,
    right, left, ring_row, ring_col, code, task, table, act, start, row_hot, col_hot, sems,
):
    p = plan
    pairs = ((act_in, act), (start_in, start), (code_in, code), (task_in, task), (table_in, table))
    copies = [pltpu.make_async_copy(src, dst, sems.at[n]) for n, (src, dst) in enumerate(pairs)]
    for copy in copies:
        copy.start()
    last = p.tiles - 1
    ring_cols = p.tiles * LANES
    row_id = lax.broadcasted_iota(jnp.int32, (p.message, LANES), 0)
    row_id = jnp.where(row_id >= p.rows + p.near, row_id + p.ring - p.message, row_id)
    lines = (
        (0, p.near, last * LANES),
        (LANES - p.wide, p.wide, (last - 1) * LANES + LANES - p.wide),
        (LANES, p.wide, 0),
        (2 * LANES - p.near, p.near, ring_cols - p.near),
    )
    blank = 0
    for at, n, _ in lines + ((2 * LANES, 0, 0),):
        if at > blank:
            col_hot[blank:at, :] = jnp.zeros((at - blank, p.agents), jnp.bfloat16)
        blank = at + n
    copies[0].wait()
    copies[1].wait()
    for i in range(p.agents // LANES):
        here = slice(i * LANES, (i + 1) * LANES)
        a = act[:, here]
        one = lambda c: jnp.where(a == c, 1, 0)
        row, col = split_cell(start[i : i + 1, :], p.cols)
        row = row + jnp.sum(one(2) - one(1), axis=0, keepdims=True)
        col = col + jnp.sum(one(4) - one(3), axis=0, keepdims=True)
        row = jnp.where(row < 0, row + p.ring, row)
        col = jnp.where(col < 0, col + ring_cols, col)
        ring_row[i : i + 1, :] = row
        ring_col[i : i + 1, :] = col
        row_hot[:, here] = one_hot(row_id, row)
        for at, n, first in lines:
            ids = first + lax.broadcasted_iota(jnp.int32, (n, LANES), 0)
            col_hot[at : at + n, here] = one_hot(ids, col)
    counts = counted(row_hot, col_hot)
    for copy in copies[2:]:
        copy.wait()
    lane = lane_of((p.half, LANES))
    for out, side, spare, shift, band in (
        (right, 0, p.near, right_roll, code[:, (last - 1) * LANES :]),
        (left, 1, LANES - p.near - p.band, left_roll, code[:, :LANES]),
    ):
        own = counts[:, side * LANES : (side + 1) * LANES]
        band = band.astype(jnp.float32)
        x = own[: p.half]
        x = jnp.where((lane >= spare) & (lane < spare + p.band), roll(own[p.half :], shift(p, "second")), x)
        lo = LANES - 2 * p.wide if side == 0 else p.wide
        x = jnp.where((lane >= lo) & (lane < lo + p.wide), roll(band[: p.half], shift(p, "code")), x)
        out[pl.ds(0, p.half), :] = x
        packed_lane = lane_of((p.pack, LANES))
        rest = jnp.zeros((p.pack, LANES), jnp.float32)
        for g in range(LANES // p.wide):
            lo = p.half + g * p.pack
            n = min(p.pack, p.rows - lo)
            if n <= 0:
                break
            y = roll(band[lo : lo + n], shift(p, g))
            if n < p.pack:
                y = jnp.concatenate([y, jnp.zeros((p.pack - n, LANES), jnp.float32)], axis=0)
            rest = jnp.where((packed_lane >= g * p.wide) & (packed_lane < (g + 1) * p.wide), y, rest)
        out[pl.ds(p.half, p.pack), :] = rest


def local_kernel(
    plan, ring_row, ring_col, task, table, hist, address, lane_out, looked, row_hot, col_hot, padded
):
    p = plan
    ring_cols = p.tiles * LANES
    row_id = lax.broadcasted_iota(jnp.int32, (p.ring, LANES), 0)
    col_id = lax.broadcasted_iota(jnp.int32, (ring_cols, LANES), 0)
    for i in range(p.agents // LANES):
        here = slice(i * LANES, (i + 1) * LANES)
        row = ring_row[i : i + 1, :]
        col = ring_col[i : i + 1, :]
        row_hot[:, here] = one_hot(row_id, row)
        col_hot[:, here] = one_hot(col_id, col)
        row = jnp.where(row >= p.rows + p.near, row - p.ring, row) + p.wide
        col = jnp.where(col >= p.cols + p.near, col - ring_cols, col) + p.wide
        t = task[i : i + 1, :]
        u = t // PACK
        block = (row * p.magic) >> 16
        lane_out[i : i + 1, :] = (t - u * PACK) * p.blocks + block
        plane = u * p.deep + row - block * p.deep
        address[i : i + 1, :] = plane * p.lines + col
    counts = counted(row_hot, col_hot)
    for t in range(p.tiles):
        hist[t] = counts[:, t * LANES : (t + 1) * LANES]
    padded[...] = jnp.zeros_like(padded)
    padded[pl.ds(0, p.tasks), pl.ds(0, p.codes)] = table[...]
    upright = jnp.transpose(padded[...])
    for t in range(p.tasks):
        looked[t] = jnp.broadcast_to(upright[: p.shelf, t : t + 1], (p.shelf, LANES))


def side_counts(p, message, shift, lo, n):
    parts = []
    for a, b in ((lo, min(lo + n, p.half)), (max(lo, p.half), lo + n)):
        if a < b and a < p.half:
            parts.append(message[pl.ds(a, b - a), :])
        elif a < b:
            parts.append(roll(message[pl.ds(a - p.half, b - a), :], -shift(p, "second")))
    return parts[0] if len(parts) == 1 else jnp.concatenate(parts, axis=0)


def side_codes(p, message, shift, lo, n):
    parts = []
    at = lo
    while at < lo + n:
        if at < p.half:
            end = min(lo + n, p.half)
            parts.append(roll(message[pl.ds(at, end - at), :], -shift(p, "code")))
        else:
            g, r = divmod(at - p.half, p.pack)
            end = min(lo + n, at - r + p.pack)
            parts.append(roll(message[pl.ds(p.half + r, end - at), :], -shift(p, g)))
        at = end
    return parts[0] if len(parts) == 1 else jnp.concatenate(parts, axis=0)


def merged_counts(p, hist, from_left, from_right, row, n):
    last = p.tiles - 1
    lo = row if row < p.rows + p.near else row - p.ring + p.message
    lane = lane_of((n, LANES))
    l = side_counts(p, from_left, right_roll, lo, n)
    r = side_counts(p, from_right, left_roll, lo, n)
    out = []
    for t in range(p.tiles):
        h = hist[t, pl.ds(row, n), :]
        if t == 0:
            h = h + jnp.where(lane < p.near, l, 0.0)
        if t == last - 1:
            h = h + jnp.where(lane >= LANES - p.near, r, 0.0)
        if t == last:
            h = h + jnp.where(lane >= LANES - p.wide, l, jnp.where(lane < p.wide, r, 0.0))
        out.append(h)
    return out


def merged_codes(p, code, from_left, from_right, row, n):
    last = p.tiles - 1
    lane = lane_of((n, LANES))
    out = [code[pl.ds(row, n), pl.ds(t * LANES, LANES)].astype(jnp.float32) for t in range(last)]
    l = side_codes(p, from_left, right_roll, row, n)
    r = side_codes(p, from_right, left_roll, row, n)
    out.append(jnp.where(lane >= LANES - p.wide, l, jnp.where(lane < p.wide, r, 0.0)))
    return out


def across_kernel(plan, hist, code, from_left, from_right, first, second):
    p = plan
    last = p.tiles - 1
    down_cnt = merged_counts(p, hist, from_left, from_right, p.rows - p.wide, p.band)
    up_near = merged_counts(p, hist, from_left, from_right, p.ring - p.near, p.near)
    up_wide = merged_counts(p, hist, from_left, from_right, 0, p.wide)
    down_code = merged_codes(p, code, from_left, from_right, p.rows - p.wide, p.wide)
    up_code = merged_codes(p, code, from_left, from_right, 0, p.wide)
    lane = lane_of((p.wide, LANES))
    inside = (lane >= p.wide) & (lane < LANES - p.wide)
    half = LANES // 2
    odd = lax.axis_index("gy") % 2 == 1

    def put(at, n, down, up):
        first[pl.ds(at, n), :] = jnp.where(odd, up, down)
        second[pl.ds(at, n), :] = jnp.where(odd, down, up)

    for t in range(p.tiles):
        down, up = down_cnt[t], jnp.concatenate([up_near[t], up_wide[t]], axis=0)
        if t < last:
            put(p.tiles * p.band + t * p.wide, p.wide, down_code[t], up_code[t])
        else:
            head = jnp.where(inside, roll(down_code[t], half), down[: p.wide])
            down = jnp.concatenate([head, down[p.wide :]], axis=0)
            tail = jnp.where(inside, roll(up_code[t], half), up[p.near :])
            up = jnp.concatenate([up[: p.near], tail], axis=0)
        put(t * p.band, p.band, down, up)


def look_up(p, looked):
    def pick(t, low, high):
        found = [
            jnp.take_along_axis(looked[t, pl.ds(g * SUB, SUB), :], low, axis=0, mode="promise_in_bounds")
            for g in range(p.shelf // SUB)
        ]
        for bit in high:
            found = [jnp.where(bit, found[g + 1], found[g]) for g in range(0, len(found), 2)]
        return found[0]

    def put(flat, c, at, code, count):
        crowd = PENALTY * count
        at = pl.ds(at, SUB)
        low = code & (SUB - 1)
        high = [(code & (1 << b)) != 0 for b in range(3, p.code_bits)]
        flat[p.tasks * p.tiles + c, at, :] = jnp.where(code < p.codes - TERMINAL, GAMMA, 0.0)
        for t in range(p.tasks):
            flat[t * p.tiles + c, at, :] = pick(t, low, high) - crowd

    return put


def rewards_kernel(plan, hist, code, from_left, from_right, looked, flat, near):
    p = plan
    put = look_up(p, looked)
    for row in range(0, p.rows, SUB):
        counts = merged_counts(p, hist, from_left, from_right, row, SUB)
        codes = merged_codes(p, code, from_left, from_right, row, SUB)
        for c in range(p.tiles):
            put(flat, c, row + p.wide, codes[c].astype(jnp.int32), counts[c])
    for at, row in ((0, p.rows), (p.near, p.ring - p.near)):
        counts = merged_counts(p, hist, from_left, from_right, row, p.near)
        for c in range(p.tiles):
            near[c, pl.ds(at, p.near), :] = counts[c]


def sweep_kernel(plan, looked, flat_in, near, first, second, address_in, lane_in, values, answers, flat,
                 turned, reward, gain, value, edge, spin, raw, final, natural, rows_of, address, sems):
    p = plan
    del flat_in
    fetch_address = pltpu.make_async_copy(address_in, address, sems.at[p.tasks * (p.tiles - 1)])
    fetch_address.start()
    last = p.tiles - 1
    odd = lax.axis_index("gy") % 2 == 1
    half = LANES // 2
    w, s = p.wide, p.near

    def above(at, n):
        at = pl.ds(at, n)
        return jnp.where(odd, first[at, :], second[at, :])

    def below(at, n):
        at = pl.ds(at, n)
        return jnp.where(odd, second[at, :], first[at, :])

    put = look_up(p, looked)
    for c in range(p.tiles):
        base = c * p.band
        code_base = p.tiles * p.band + c * w
        for at, extra in ((0, above(base + w, s)), (p.rows - s, below(base, s))):
            at = pl.ds(w + at, s)
            for t in range(p.tasks):
                flat[t * p.tiles + c, at, :] = flat[t * p.tiles + c, at, :] - PENALTY * extra
        for row in range(0, w, SUB):
            count = above(base + row, SUB)
            code = above(code_base + row, SUB) if c < last else roll(count, half)
            if row >= w - s:
                count = count + near[c, pl.ds(s + row - (w - s), SUB), :]
            put(flat, c, row, code.astype(jnp.int32) & (p.shelf - 1), count)
            count = below(base + s + row, SUB)
            code = below(code_base + row, SUB) if c < last else roll(count, half)
            if row < s:
                count = count + near[c, pl.ds(row, SUB), :]
            put(flat, c, w + p.rows + row, code.astype(jnp.int32) & (p.shelf - 1), count)

    for u in range(p.groups + 1):
        for i in range(p.deep):
            for c in range(p.tiles):
                parts = []
                for h in range(PACK):
                    t = u * PACK + h if u < p.groups else p.tasks
                    parts.append(flat[t * p.tiles + c, pl.ds(i, p.blocks, stride=p.deep), :])
                x = jnp.transpose(jnp.concatenate(parts, axis=0))
                if c < last:
                    turned[u * p.deep + i, pl.ds(w + c * LANES, LANES), :] = x
                else:
                    turned[u * p.deep + i, pl.ds(w + p.cols, w), :] = x[:w]
                    turned[u * p.deep + i, pl.ds(0, w), :] = x[LANES - w :]

    early = p.span - TAIL
    ends = [(u, up) for u in range(p.groups) for up in (True, False)]

    def end_of(line, u, up):
        return line[u * p.deep + (p.deep - 1 if up else 0)]

    def turn(x, up):
        return pltpu.roll(x, 1 if up else LANES - 1, 1)

    def spot(q, e):
        return pl.ds((q * len(ends) + e) * SUB, SUB)

    def put_ends(q, line):
        for e, (u, up) in enumerate(ends):
            x = end_of(line, u, up)
            if q < early:
                spin[spot(q, e), :] = turn(x, up)
            else:
                raw[spot(q - early, e), :] = x

    for q in range(p.span):
        line = []
        for n in range(p.planes + p.deep):
            x = turned[n, pl.ds(q, SUB, stride=p.span), :]
            if n < p.planes:
                reward[pl.ds((q * p.planes + n) * SUB, SUB), :] = x
                line.append(x)
            else:
                gain[pl.ds((q * p.deep + n - p.planes) * SUB, SUB), :] = x
        put_ends(q, line)

    def sweep(held, put, more=True):
        load = lambda q: [held[pl.ds((q * p.planes + n) * SUB, SUB), :] for n in range(p.planes)]
        for q in range(early, p.span):
            for e, (u, up) in enumerate(ends):
                spin[spot(q, e), :] = turn(raw[spot(q - early, e), :], up)
        now = load(0)
        before = [pltpu.roll(x, 1, 0) for x in load(p.span - 1)]
        for n in range(p.planes):
            edge[pl.ds(n * SUB, SUB), :] = pltpu.roll(now[n], SUB - 1, 0)
        passed = [
            jnp.maximum(before[n - 1], now[n]) if n % p.deep else None for n in range(p.planes)
        ]
        for q in range(p.span):
            if q + 1 < p.span:
                after = load(q + 1)
            else:
                after = [edge[pl.ds(n * SUB, SUB), :] for n in range(p.planes)]
            corner = [None] * p.planes
            made = [None] * p.planes
            for n in range(p.planes):
                above_cell = now[n - 1] if n % p.deep else spin[spot(q, 2 * (n // p.deep)), :]
                corner[n] = jnp.maximum(above_cell, after[n])
            for i in range(p.deep):
                g = gain[pl.ds((q * p.deep + i) * SUB, SUB), :]
                for u in range(p.groups):
                    n = u * p.deep + i
                    if i + 1 < p.deep:
                        other = passed[n + 1]
                    else:
                        other = jnp.maximum(before[n], spin[spot(q, 2 * u + 1), :])
                    best = jnp.maximum(corner[n], other)
                    made[n] = reward[pl.ds((q * p.planes + n) * SUB, SUB), :] + g * best
                    put(q, n, made[n])
            if more:
                put_ends(q, made)
            before, now, passed = now, after, corner

    def put_value(q, n, x):
        value[pl.ds((q * p.planes + n) * SUB, SUB), :] = x

    def put_final(q, n, x):
        final[pl.ds(n * p.lines + q, SUB, stride=p.span), :] = x

    def sweeps(_, carry):
        for _ in range(UNROLL):
            sweep(value, put_value)
        return carry

    assert (SWEEPS - 2) % UNROLL == 0
    sweep(reward, put_value)
    lax.fori_loop(0, (SWEEPS - 2) // UNROLL, sweeps, 0)
    sweep(value, put_final, more=False)
    fetch_address.wait()

    lane_id = lax.broadcasted_iota(jnp.int32, (LANES, LANES), 0)

    def fetch(a):
        rows_of[pl.ds(a, 1), :] = final[pl.ds(address[a // LANES, a % LANES], 1), :]

    def answer(i):
        x = jnp.transpose(rows_of[pl.ds(i * LANES, LANES), :])
        picked = jnp.where(lane_id == lane_in[i : i + 1, :], x, 0.0)
        answers[i : i + 1, :] = jnp.sum(picked, axis=0, keepdims=True)

    copies = []
    fetched = answered = 0
    turns = p.planes * last
    for u in range(p.groups):
        for c in range(last):
            for i in range(p.deep):
                lines = pl.ds((u * p.deep + i) * p.lines + w + c * LANES, LANES)
                x = jnp.transpose(final[lines, :])
                for h in range(PACK):
                    at = pl.ds(i, p.blocks, stride=p.deep)
                    natural[(u * PACK + h) * last + c, at, :] = x[h * p.blocks : (h + 1) * p.blocks]
                until = min(p.agents, -(-p.agents * 5 * ((u * last + c) * p.deep + i + 1) // (8 * turns)))
                for a in range(fetched, until):
                    fetch(a)
                fetched = until
                while (answered + 1) * LANES <= fetched:
                    answer(answered)
                    answered += 1
            for h in range(PACK):
                t = u * PACK + h
                copy = pltpu.make_async_copy(
                    natural.at[t * last + c, pl.ds(w, p.rows), :],
                    values.at[t, :, pl.ds(c * LANES, LANES)],
                    sems.at[t * last + c],
                )
                copy.start()
                copies.append(copy)
    for a in range(fetched, p.agents):
        fetch(a)
        if (a + 1) % LANES == 0:
            answer(a // LANES)
    for copy in copies:
        copy.wait()


def shift(value, axis, steps):
    count = lax.axis_size(axis)
    return lax.ppermute(value, axis, [(i, (i + steps) % count) for i in range(count)])


def swap(value, axis, parity):
    count = lax.axis_size(axis)
    assert count % 2 == 0
    return lax.ppermute(
        value, axis, [(i, (i + (1 if i % 2 == parity else -1)) % count) for i in range(count)]
    )


def on_device(map_codes, reward_table, start_cell, agent_task, actions):
    rows, cols = map_codes.shape
    tasks, codes = reward_table.shape
    steps, agents = actions.shape
    p = Plan(rows, cols, agents, steps, tasks, codes)
    vmem = pl.BlockSpec(memory_space=pltpu.VMEM)
    smem = pl.BlockSpec(memory_space=pltpu.SMEM)
    f32, i32 = jnp.float32, jnp.int32
    shape = jax.ShapeDtypeStruct
    fast = lambda dims, dtype: pltpu.VMEM(dims, dtype)
    far = lambda x: pltpu.with_memory_space_constraint(x, pltpu.HBM)
    near = lambda x: pltpu.with_memory_space_constraint(x, pltpu.VMEM)
    by_lane = (agents // LANES, LANES)

    def bind(kernel):
        def body(*refs):
            kernel(p, *refs)

        return body

    to_right, to_left, ring_row, ring_col, kept, task, table = pl.pallas_call(
        bind(bands_kernel),
        in_specs=[pl.BlockSpec(memory_space=pl.ANY)] * 5,
        out_specs=[vmem] * 7,
        out_shape=[
            fast((p.across_rows, LANES), f32),
            fast((p.across_rows, LANES), f32),
            fast(by_lane, i32),
            fast(by_lane, i32),
            fast((rows, cols), i32),
            fast(by_lane, i32),
            fast((tasks, codes), f32),
        ],
        scratch_shapes=[
            pltpu.VMEM((steps, agents), i32),
            pltpu.VMEM(by_lane, i32),
            pltpu.VMEM((p.message, agents), jnp.bfloat16),
            pltpu.VMEM((2 * LANES, agents), jnp.bfloat16),
            pltpu.SemaphoreType.DMA((5,)),
        ],
        compiler_params=pltpu.CompilerParams(vmem_limit_bytes=12 << 20),
        name="bands",
    )(*map(far, (actions, start_cell.reshape(by_lane), map_codes, agent_task.reshape(by_lane), reward_table)))
    from_left = shift(to_right, "gx", 1)
    from_right = shift(to_left, "gx", -1)
    hist, address, lane, looked = pl.pallas_call(
        bind(local_kernel),
        in_specs=[vmem] * 4,
        out_specs=[vmem] * 4,
        out_shape=[
            fast((p.tiles, p.ring, LANES), f32),
            fast(by_lane, i32),
            fast(by_lane, i32),
            fast((tasks, p.shelf, LANES), f32),
        ],
        scratch_shapes=[
            pltpu.VMEM((p.ring, agents), jnp.bfloat16),
            pltpu.VMEM((p.tiles * LANES, agents), jnp.bfloat16),
            pltpu.VMEM((LANES, LANES), f32),
        ],
        compiler_params=pltpu.CompilerParams(vmem_limit_bytes=12 << 20),
        name="local",
    )(near(ring_row), near(ring_col), near(task), near(table))
    sides = (near(hist), near(kept), near(from_left), near(from_right))
    first, second = pl.pallas_call(
        bind(across_kernel),
        in_specs=[vmem] * 4,
        out_specs=[vmem] * 2,
        out_shape=[fast((p.down_rows, LANES), f32), fast((p.down_rows, LANES), f32)],
        compiler_params=pltpu.CompilerParams(vmem_limit_bytes=8 << 20),
        name="across",
    )(*sides)
    first = swap(first, "gy", 0)
    second = swap(second, "gy", 1)
    flats = ((tasks + 1) * p.tiles, p.ring, LANES)
    flat, edges = pl.pallas_call(
        bind(rewards_kernel),
        in_specs=[vmem] * 5,
        out_specs=[vmem] * 2,
        out_shape=[fast(flats, f32), fast((p.tiles, 2 * p.near, LANES), f32)],
        compiler_params=pltpu.CompilerParams(vmem_limit_bytes=12 << 20),
        name="rewards",
    )(*sides, near(looked))
    outs = tasks * (p.tiles - 1)
    values, answers, _ = pl.pallas_call(
        bind(sweep_kernel),
        in_specs=[vmem] * 7,
        out_specs=[pl.BlockSpec(memory_space=pl.ANY), vmem, vmem],
        out_shape=[shape((tasks, rows, cols), f32), shape(by_lane, f32), fast(flats, f32)],
        scratch_shapes=[
            pltpu.VMEM((p.planes + p.deep, p.lines, LANES), f32),
            pltpu.VMEM((p.planes * p.lines, LANES), f32),
            pltpu.VMEM((p.deep * p.lines, LANES), f32),
            pltpu.VMEM((p.planes * p.lines, LANES), f32),
            pltpu.VMEM((p.planes * SUB, LANES), f32),
            pltpu.VMEM((2 * p.groups * p.span * SUB, LANES), f32),
            pltpu.VMEM((2 * p.groups * TAIL * SUB, LANES), f32),
            pltpu.VMEM((p.planes * p.lines, LANES), f32),
            pltpu.VMEM((outs, p.ring, LANES), f32),
            pltpu.VMEM((agents, LANES), f32),
            pltpu.SMEM(by_lane, i32),
            pltpu.SemaphoreType.DMA((outs + 1,)),
        ],
        input_output_aliases={1: 2},
        compiler_params=pltpu.CompilerParams(vmem_limit_bytes=24 << 20),
        name="sweep",
    )(near(looked), near(flat), near(edges), near(first), near(second), near(address), near(lane))
    return values, answers.reshape(agents)


def solution(mesh):
    placed = (P("gy", "gx"), P(), P(("gx", "gy")), P(("gx", "gy")), P(None, ("gx", "gy")))
    return jax.shard_map(
        on_device,
        mesh=mesh,
        in_specs=placed,
        out_specs=(P(None, "gy", "gx"), P(("gx", "gy"))),
        check_vma=False,
    )
```
